128 devices in a mesh: dp: 1, sp: 128 (over z, y, x, core).
Axes of the slice: x: 4, y: 4, z: 4, core: 2. Of those that a mesh axis runs over, the one named last changes fastest.
Arguments:
- tokens: bfloat16 [64, 2560], P('dp')
- positions: int32 [64], P('dp')
- k_cache: bfloat16 [64, 2048, 8, 128], P('dp', 'sp')
- v_cache: bfloat16 [64, 2048, 8, 128], P('dp', 'sp')
- w_q: bfloat16 [2560, 4096], replicated
- w_k: bfloat16 [2560, 1024], replicated
- w_v: bfloat16 [2560, 1024], replicated
- w_o: bfloat16 [4096, 2560], replicated
- attn_norm: bfloat16 [2560], replicated
- q_norm: bfloat16 [128], replicated
- k_norm: bfloat16 [128], replicated
Outputs:
- output 1: bfloat16 [64, 2560], P('dp')
- output 2: bfloat16 [64, 2048, 8, 128], P('dp', 'sp')
- output 3: bfloat16 [64, 2048, 8, 128], P('dp', 'sp')
- output 4: bfloat16 [64, 2, 8, 128], P('dp')
All inputs are finite; a program needn't handle non-finite values.
Results may differ from the reference program's by a relative error of at most 0.00652824.
Values sent between devices are 32-bit elements.
A program may use at most 1 GiB of HBM per device.

```python
import jax
import jax.numpy as jnp
from jax import lax

NUM_SEQS = 64
MODEL_DIM = 2560
Q_HEADS = 32
KV_HEADS = 8
HEAD_DIM = 128
CACHE_LEN = 2048

Q_PER_KV = Q_HEADS // KV_HEADS
NORM_EPS = 1e-6
ROPE_THETA = 1000000.0
NEG_FILL = -1e30


def setup_inputs(seed: int = 0, part: int = 0) -> dict:
    part_keys = jax.random.split(jax.random.fold_in(jax.random.key(seed), part), 5)
    shared = jax.random.split(jax.random.key(seed + 1), 7)
    cache_shape = (NUM_SEQS, CACHE_LEN, KV_HEADS, HEAD_DIM)
    tokens = jax.random.normal(part_keys[0], (NUM_SEQS, MODEL_DIM), jnp.float32)
    pos_draw = jax.random.randint(part_keys[1], (NUM_SEQS,), CACHE_LEN // 4, CACHE_LEN, dtype=jnp.int32)
    positions = pos_draw.at[0].set(CACHE_LEN - 1).at[1].set(CACHE_LEN // 4)
    k_cache = jax.random.normal(part_keys[2], cache_shape, jnp.float32)
    coarse = jax.random.normal(part_keys[3], (NUM_SEQS, 16, KV_HEADS, HEAD_DIM), jnp.float32)
    v_noise = jax.random.normal(part_keys[4], cache_shape, jnp.float32)
    v_cache = 1.5 * jnp.repeat(coarse, CACHE_LEN // 16, axis=1) + 0.5 * v_noise
    w_q = jax.random.normal(shared[0], (MODEL_DIM, Q_HEADS * HEAD_DIM), jnp.float32) * MODEL_DIM ** -0.5
    w_k = jax.random.normal(shared[1], (MODEL_DIM, KV_HEADS * HEAD_DIM), jnp.float32) * MODEL_DIM ** -0.5
    w_v = jax.random.normal(shared[2], (MODEL_DIM, KV_HEADS * HEAD_DIM), jnp.float32) * MODEL_DIM ** -0.5
    w_o = jax.random.normal(shared[3], (Q_HEADS * HEAD_DIM, MODEL_DIM), jnp.float32) * (Q_HEADS * HEAD_DIM) ** -0.5
    attn_norm = jax.random.uniform(shared[4], (MODEL_DIM,), jnp.float32, 0.5, 1.5)
    q_norm = jax.random.uniform(shared[5], (HEAD_DIM,), jnp.float32, 0.5, 2.0)
    k_norm = jax.random.uniform(shared[6], (HEAD_DIM,), jnp.float32, 0.5, 2.0)
    return {
        'tokens': tokens.astype(jnp.bfloat16),
        'positions': positions,
        'k_cache': k_cache.astype(jnp.bfloat16),
        'v_cache': v_cache.astype(jnp.bfloat16),
        'w_q': w_q.astype(jnp.bfloat16),
        'w_k': w_k.astype(jnp.bfloat16),
        'w_v': w_v.astype(jnp.bfloat16),
        'w_o': w_o.astype(jnp.bfloat16),
        'attn_norm': attn_norm.astype(jnp.bfloat16),
        'q_norm': q_norm.astype(jnp.bfloat16),
        'k_norm': k_norm.astype(jnp.bfloat16),
    }


def rms_scale(values, gain):
    return values * lax.rsqrt(jnp.mean(values * values, axis=-1, keepdims=True) + NORM_EPS) * gain.astype(jnp.float32)


def rope_table(positions):
    inv_freq = ROPE_THETA ** (-jnp.arange(HEAD_DIM // 2, dtype=jnp.float32) * 2.0 / HEAD_DIM)
    angles = positions.astype(jnp.float32)[:, None] * inv_freq[None, :]
    return jnp.cos(angles)[:, None, :], jnp.sin(angles)[:, None, :]


def norm_rope(proj, gain, cos_table, sin_table):
    normed = rms_scale(proj.astype(jnp.float32), gain)
    first_half = normed[..., :HEAD_DIM // 2]
    second_half = normed[..., HEAD_DIM // 2:]
    rotated = jnp.concatenate([first_half * cos_table - second_half * sin_table, second_half * cos_table + first_half * sin_table], axis=-1)
    return rotated.astype(jnp.bfloat16)


def reference(tokens, positions, k_cache, v_cache, w_q, w_k, w_v, w_o, attn_norm, q_norm, k_norm):
    tokens_f = tokens.astype(jnp.float32)
    hidden = rms_scale(tokens_f, attn_norm).astype(jnp.bfloat16)
    q_proj = jnp.dot(hidden, w_q, preferred_element_type=jnp.float32).astype(jnp.bfloat16).reshape(NUM_SEQS, Q_HEADS, HEAD_DIM)
    k_proj = jnp.dot(hidden, w_k, preferred_element_type=jnp.float32).astype(jnp.bfloat16).reshape(NUM_SEQS, KV_HEADS, HEAD_DIM)
    v_new = jnp.dot(hidden, w_v, preferred_element_type=jnp.float32).astype(jnp.bfloat16).reshape(NUM_SEQS, KV_HEADS, HEAD_DIM)
    cos_table, sin_table = rope_table(positions)
    q_rot = norm_rope(q_proj, q_norm, cos_table, sin_table)
    k_rot = norm_rope(k_proj, k_norm, cos_table, sin_table)
    slot_ids = jnp.arange(CACHE_LEN)
    write_mask = (slot_ids[None, :] == positions[:, None])[:, :, None, None]
    k_out = jnp.where(write_mask, k_rot[:, None], k_cache)
    v_out = jnp.where(write_mask, v_new[:, None], v_cache)
    score_scale = HEAD_DIM ** -0.5

    def one_seq(items):
        q_one, k_one, v_one, pos_one = items
        q_grp = q_one.reshape(KV_HEADS, Q_PER_KV, HEAD_DIM).astype(jnp.float32)
        scores = jnp.einsum('kgd,tkd->kgt', q_grp, k_one.astype(jnp.float32)) * score_scale
        live_mask = (slot_ids <= pos_one)[None, None, :]
        global_peak = jnp.max(jnp.where(live_mask, scores, NEG_FILL), axis=-1, keepdims=True)
        weights = jnp.where(live_mask, jnp.exp(scores - global_peak), 0.0)
        total_sum = jnp.sum(weights, axis=-1, keepdims=True)
        mixed = jnp.einsum('kgt,tkd->kgd', weights.astype(jnp.bfloat16).astype(jnp.float32), v_one.astype(jnp.float32))
        return (mixed / total_sum).astype(jnp.bfloat16).reshape(Q_HEADS * HEAD_DIM)

    attn_out = lax.map(one_seq, (q_rot, k_out, v_out, positions))
    block_out = (tokens_f + jnp.dot(attn_out, w_o, preferred_element_type=jnp.float32)).astype(jnp.bfloat16)
    new_kv = jnp.stack([k_rot, v_new], axis=1)
    return (block_out, k_out, v_out, new_kv)
```

```python
import functools

import jax
import jax.numpy as jnp
import numpy as np
from jax import lax
from jax.experimental import pallas as pl
from jax.experimental.pallas import tpu as pltpu
from jax.sharding import PartitionSpec as P

NORM_EPS = 1e-6
ROPE_THETA = 1000000.0
NEG_FILL = -1e30
SEQS, DIM, HEADS, KV_HEADS, HEAD_DIM, SLOTS = 64, 2560, 32, 8, 128, 16
HALF = HEADS // 2
CHIPS = 64
SCALE = HEAD_DIM ** -0.5
F32, BF16 = jnp.float32, jnp.bfloat16
MESH = pl.DeviceIdType.MESH
DEPTH = 4


def rms(values, gain):
    return values * lax.rsqrt(jnp.mean(values * values, axis=-1, keepdims=True) + NORM_EPS) * gain


def iota(shape, axis):
    return lax.broadcasted_iota(jnp.int32, shape, axis)


def pick(row, lane):
    spread = jnp.broadcast_to(row, (HALF, HEAD_DIM))
    return jnp.sum(jnp.where(lane, spread, 0.0), axis=-1, keepdims=True)


def step_kernel(pos_ref, tok_ref, an_ref, qn_ref, kn_ref, freq_ref, wq_hbm, wk_hbm, wv_hbm, wo_hbm, kc_hbm, vc_hbm,
                out_ref, kv_hbm,
                hid, cosr, sinr, wbuf, wobuf, kbuf, vbuf, gbuf, obuf, oin, st, stin, osend, stsend, rbuf, rst,
                lhs, ypart, yin, ysend, ybuf,
                wsem, wosem, csem, kvsem, gsend, grecv, dsend, drecv, dssend, dsrecv,
                ssend, srecv, tsend, trecv, ysem, bsend, brecv, fsend, frecv):
    me = lax.axis_index("sp")
    chip, core = me // 2, me % 2
    zed = chip // 16
    mate = chip * 2 + (1 - core)
    start = me * SLOTS

    def dev(index):
        return (lax.axis_index("dp"), index)

    barrier = pltpu.get_barrier_semaphore()
    pl.semaphore_signal(barrier, inc=1, device_id=dev(mate), device_id_type=MESH)

    @pl.loop(1, CHIPS)
    def _(off):
        pl.semaphore_signal(barrier, inc=1, device_id=dev(lax.rem(chip + off, CHIPS) * 2 + core), device_id_type=MESH)

    def wcopy(src, col, tile):
        return pltpu.make_async_copy(src.at[:, pl.ds(pl.multiple_of(col, 256), 256)], wbuf.at[tile], wsem.at[tile])

    def kcopy(t):
        return wcopy(wk_hbm, core * 512 + t * 256, t)

    def vcopy(t):
        return wcopy(wv_hbm, core * 512 + t * 256, 2 + t)

    def qcopy(t):
        return wcopy(wq_hbm, core * 2048 + t * 256, 4 + t)

    for t in range(2):
        kcopy(t).start()
    for t in range(2):
        vcopy(t).start()

    tok = tok_ref[...].astype(F32)
    hid[...] = rms(tok, an_ref[...].astype(F32)).astype(BF16)
    row8 = iota((SEQS, HEAD_DIM), 0)
    posv = jnp.zeros((SEQS, HEAD_DIM), jnp.int32)
    for s in range(SEQS):
        posv = jnp.where(row8 == s, pos_ref[s], posv)
    angle = posv.astype(F32) * freq_ref[...]
    cosr[...] = jnp.cos(angle)
    sinr[...] = jnp.where(iota((SEQS, HEAD_DIM), 1) < HEAD_DIM // 2, -1.0, 1.0) * jnp.sin(angle)

    def project(tile):
        return jnp.dot(hid[...], wbuf[tile], preferred_element_type=F32).astype(BF16).astype(F32)

    def rope(head, gain):
        normed = rms(head, gain)
        turned = normed * cosr[...] + pltpu.roll(normed, HEAD_DIM // 2, 1) * sinr[...]
        return turned.astype(BF16).astype(F32)

    for t in range(2):
        kcopy(t).wait()
        qcopy(t).start()
        res = project(t)
        for h in range(2):
            gbuf[4 + core, :, 2 * t + h, :] = rope(res[:, h * 128:(h + 1) * 128], kn_ref[...].astype(F32))
    for t in range(2):
        vcopy(t).wait()
        qcopy(2 + t).start()
        res = project(2 + t)
        for h in range(2):
            gbuf[4 + core, :, 4 + 2 * t + h, :] = res[:, h * 128:(h + 1) * 128]

    pl.semaphore_wait(barrier, CHIPS)

    def gcopy(group, slot):
        return pltpu.make_async_remote_copy(src_ref=gbuf.at[group], dst_ref=gbuf.at[group], send_sem=gsend.at[slot],
                                            recv_sem=grecv.at[slot], device_id=dev(mate), device_id_type=MESH)

    gcopy(4 + core, 2).start()

    def kvload(i):
        rows = pl.ds(i * 16, 16)
        return (pltpu.make_async_copy(kc_hbm.at[rows], kbuf.at[rows], csem.at[0, i]),
                pltpu.make_async_copy(vc_hbm.at[rows], vbuf.at[rows], csem.at[1, i]))

    for g in range(2):
        for t4 in range(4):
            t = g * 4 + t4
            qcopy(t).wait()
            if t + DEPTH < 8:
                qcopy(t + DEPTH).start()
            else:
                for c in kvload(t - 4):
                    c.start()
            res = project(4 + t)
            for h in range(2):
                gbuf[2 * core + g, :, 2 * t4 + h, :] = rope(res[:, h * 128:(h + 1) * 128], qn_ref[...].astype(F32))
        gcopy(2 * core + g, g).start()

    wocopy = pltpu.make_async_copy(wo_hbm.at[pl.ds(pl.multiple_of(core * 2048, 2048), 2048)], wobuf, wosem.at[0])
    wocopy.start()
    for slot in range(3):
        gcopy(4 + core if slot == 2 else 2 * core + slot, slot).wait()
    kvout = pltpu.make_async_copy(gbuf.at[pl.ds(4, 2)], kv_hbm, kvsem.at[0])
    kvout.start()
    for i in range(4):
        for c in kvload(i):
            c.wait()

    def block_of(i):
        return lax.rem(zed + 2 + 3 * (i // 2), 4) * 2 + lax.rem(i, 2)

    row32, col32 = iota((HEADS, HEAD_DIM), 0), iota((HEADS, HEAD_DIM), 1)
    same_head = (col32 % KV_HEADS) == (row32 // 4)
    slot_of = col32 // KV_HEADS + start
    row16, lane16 = iota((HALF, HEAD_DIM), 0), iota((HALF, HEAD_DIM), 1)

    def dcopies(blk, i):
        rows = pl.ds(blk * 8, 8)
        return (pltpu.make_async_remote_copy(src_ref=obuf.at[1 - core, rows], dst_ref=oin.at[rows], send_sem=dsend.at[i],
                                             recv_sem=drecv.at[i], device_id=dev(mate), device_id_type=MESH),
                pltpu.make_async_remote_copy(src_ref=st.at[1 - core, blk], dst_ref=stin.at[blk], send_sem=dssend.at[i],
                                             recv_sem=dsrecv.at[i], device_id=dev(mate), device_id_type=MESH))

    def attend(i):
        blk = block_of(i)
        acc = [[jnp.zeros((HALF, HEAD_DIM), F32) for _ in range(2)] for _ in range(2)]
        for s8 in range(8):
            s = blk * 8 + s8
            q = jnp.concatenate([gbuf[g, s] for g in range(4)], axis=0).astype(BF16)
            scores = lax.dot_general(q, kbuf[s], (((1,), (1,)), ((), ())), preferred_element_type=F32) * SCALE
            live = same_head & (slot_of < pos_ref[s])
            scores = jnp.where(live, scores, NEG_FILL)
            peak = jnp.max(scores, axis=-1, keepdims=True)
            weights = jnp.where(live, jnp.exp(scores - peak), 0.0)
            total = jnp.sum(weights, axis=-1, keepdims=True)
            mixed = jnp.dot(weights.astype(BF16), vbuf[s], preferred_element_type=F32)
            here = lane16 == s8 * HALF + row16
            for half in range(2):
                cut = slice(half * HALF, (half + 1) * HALF)
                obuf[half, s] = mixed[cut]
                acc[half][0] += jnp.where(here, peak[cut], 0.0)
                acc[half][1] += jnp.where(here, total[cut], 0.0)
        for half in range(2):
            for k in range(2):
                st[half, blk, pl.ds(k, 1), :] = jnp.sum(acc[half][k], axis=0, keepdims=True)
        for c in dcopies(blk, i):
            c.start()

    def scatter(blk, s):
        o = pltpu.make_async_remote_copy(src_ref=osend.at[s], dst_ref=rbuf.at[chip], send_sem=ssend.at[0], recv_sem=srecv.at[0],
                                         device_id=dev(s * 2 + core), device_id_type=MESH)
        t = pltpu.make_async_remote_copy(src_ref=stsend.at[blk], dst_ref=rst.at[chip], send_sem=tsend.at[0], recv_sem=trecv.at[0],
                                         device_id=dev(s * 2 + core), device_id_type=MESH)
        return o, t

    def merge(i):
        blk = block_of(i)
        for c in dcopies(blk, i):
            c.wait()
        m0, l0 = st[core, blk, pl.ds(0, 1), :], st[core, blk, pl.ds(1, 1), :]
        m1, l1 = stin[blk, pl.ds(0, 1), :], stin[blk, pl.ds(1, 1), :]
        top = jnp.maximum(m0, m1)
        f0, f1 = jnp.exp(m0 - top), jnp.exp(m1 - top)
        stsend[blk, pl.ds(0, 1), :] = top
        stsend[blk, pl.ds(1, 1), :] = l0 * f0 + l1 * f1
        for s8 in range(8):
            s = blk * 8 + s8
            here = lane16 == s8 * HALF + row16
            osend[s] = obuf[core, s] * pick(f0, here) + oin[s] * pick(f1, here)

        @pl.loop(0, 8)
        def _(s8):
            s = blk * 8 + s8

            @pl.when(s != chip)
            def _():
                for c in scatter(blk, s):
                    c.start()

            @pl.when(s == chip)
            def _():
                pltpu.make_async_copy(osend.at[s], rbuf.at[chip], srecv.at[0]).start()
                pltpu.make_async_copy(stsend.at[blk], rst.at[chip], trecv.at[0]).start()

    LAG = 3

    @pl.loop(0, 8 + LAG)
    def _(i):
        @pl.when(i < 8)
        def _():
            attend(i)

        @pl.when(i >= LAG)
        def _():
            merge(i - LAG)

    def all_of(src, dst, send, recv):
        return pltpu.make_async_remote_copy(src_ref=src, dst_ref=dst, send_sem=send, recv_sem=recv, device_id=dev(mate),
                                            device_id_type=MESH)

    all_of(rst, rst, tsend.at[0], trecv.at[0]).wait_recv()
    all_of(rbuf, rbuf, ssend.at[0], srecv.at[0]).wait_recv()

    here = lane16 == lax.rem(chip, 8) * HALF + row16
    tops = rst[:, 0, :]
    top = jnp.max(tops, axis=0, keepdims=True)
    facs = jnp.exp(tops - top)
    total = pick(jnp.sum(rst[:, 1, :] * facs, axis=0, keepdims=True), here)
    acc = jnp.zeros((HALF, HEAD_DIM), F32)
    for c in range(CHIPS):
        acc += rbuf[c] * pick(facs[c:c + 1], here)
    q_own = jnp.concatenate([gbuf[2 * core, chip], gbuf[2 * core + 1, chip]], axis=0)
    kv_own = gbuf[4 + core, chip]
    k_own = jnp.concatenate([jnp.broadcast_to(kv_own[i:i + 1], (4, HEAD_DIM)) for i in range(4)], axis=0)
    v_own = jnp.concatenate([jnp.broadcast_to(kv_own[4 + i:5 + i], (4, HEAD_DIM)) for i in range(4)], axis=0)
    s_own = jnp.sum(q_own * k_own, axis=-1, keepdims=True) * SCALE
    top = pick(top, here)
    peak = jnp.maximum(top, s_own)
    f_old, f_new = jnp.exp(top - peak), jnp.exp(s_own - peak)
    attn = (acc * f_old + v_own * f_new) / (total * f_old + f_new)
    for h in range(HALF):
        lhs[:, h * 128:(h + 1) * 128] = jnp.where(row16 == h, attn, 0.0).astype(BF16)

    wocopy.wait()

    def out_cols(half, slot):
        for n in range(5):
            cols = pl.ds(pl.multiple_of(half * 1280 + n * 256, 256), 256)
            res = jnp.dot(lhs[...], wobuf[:, cols], preferred_element_type=F32)
            res = jnp.sum(res, axis=0, keepdims=True)
            for k in range(2):
                ypart[slot, pl.ds(2 * n + k, 1), :] = res[:, k * 128:(k + 1) * 128]

    out_cols(1 - core, 0)
    ycopy = pltpu.make_async_remote_copy(src_ref=ypart.at[0], dst_ref=yin, send_sem=ysem.at[0], recv_sem=ysem.at[1],
                                         device_id=dev(mate), device_id_type=MESH)
    ycopy.start()
    out_cols(core, 1)
    ycopy.wait()
    ysend[...] = ypart[1] + yin[...]

    def bcopy(s, group):
        return pltpu.make_async_remote_copy(src_ref=ysend, dst_ref=ybuf.at[core, chip], send_sem=bsend.at[0],
                                            recv_sem=brecv.at[group], device_id=dev(s * 2 + core), device_id_type=MESH)

    @pl.loop(0, CHIPS)
    def _(k):
        s = lax.rem(chip + 32 + k, CHIPS)
        group = lax.rem(zed - s // 16 + 4, 4)

        @pl.when(s != chip)
        def _():
            bcopy(s, group).start()

        @pl.when(s == chip)
        def _():
            pltpu.make_async_copy(ysend, ybuf.at[core, chip], brecv.at[0]).start()

    def slab(half, group):
        return ybuf.at[half, pl.ds(lax.rem(zed + group, 4) * 16, 16)]

    def fcopy(half, group):
        ref = slab(half, group)
        return pltpu.make_async_remote_copy(src_ref=ref, dst_ref=ref, send_sem=fsend.at[group], recv_sem=frecv.at[group],
                                            device_id=dev(mate), device_id_type=MESH)

    for group in (0, 1, 3, 2):
        ref = slab(core, group)
        all_of(ref, ref, bsend.at[0], brecv.at[group]).wait_recv()
        fcopy(core, group).start()
    for group in (0, 1, 3, 2):
        fcopy(1 - core, group).wait_recv()

    for half in range(2):
        for k in range(10):
            cols = slice(half * 1280 + k * 128, half * 1280 + (k + 1) * 128)
            out_ref[:, cols] = (tok_ref[:, cols].astype(F32) + ybuf[half, :, k, :]).astype(BF16)

    for group in range(4):
        fcopy(core, group).wait_send()
    all_of(rst.at[pl.ds(0, CHIPS - 1)], rst.at[pl.ds(0, CHIPS - 1)], tsend.at[0], trecv.at[0]).wait_send()
    all_of(rbuf.at[pl.ds(0, CHIPS - 1)], rbuf.at[pl.ds(0, CHIPS - 1)], ssend.at[0], srecv.at[0]).wait_send()
    rest = ybuf.at[0, pl.ds(0, CHIPS - 1)]
    all_of(rest, rest, bsend.at[0], brecv.at[0]).wait_send()
    kvout.wait()


def step_call(*args):
    dma = pltpu.SemaphoreType.DMA
    vmem = pltpu.VMEM
    blk = pl.BlockSpec(memory_space=pltpu.VMEM)
    hbm = pl.BlockSpec(memory_space=pl.ANY)
    return pl.pallas_call(
        step_kernel,
        name="decode_step",
        out_shape=(jax.ShapeDtypeStruct((SEQS, DIM), BF16), jax.ShapeDtypeStruct((2, SEQS, 8, HEAD_DIM), F32)),
        in_specs=[pl.BlockSpec(memory_space=pltpu.SMEM)] + [blk] * 5 + [hbm] * 6,
        out_specs=(blk, hbm),
        scratch_shapes=[
            vmem((SEQS, DIM), BF16), vmem((SEQS, HEAD_DIM), F32), vmem((SEQS, HEAD_DIM), F32),
            vmem((12, DIM, 256), BF16), vmem((2048, DIM), BF16),
            vmem((SEQS, 128, HEAD_DIM), BF16), vmem((SEQS, 128, HEAD_DIM), BF16),
            vmem((6, SEQS, 8, HEAD_DIM), F32),
            vmem((2, SEQS, HALF, HEAD_DIM), F32), vmem((SEQS, HALF, HEAD_DIM), F32),
            vmem((2, 8, 2, HEAD_DIM), F32), vmem((8, 2, HEAD_DIM), F32),
            vmem((SEQS, HALF, HEAD_DIM), F32), vmem((8, 2, HEAD_DIM), F32),
            vmem((CHIPS, HALF, HEAD_DIM), F32), vmem((CHIPS, 2, HEAD_DIM), F32),
            vmem((HALF, 2048), BF16), vmem((2, 10, HEAD_DIM), F32), vmem((10, HEAD_DIM), F32), vmem((10, HEAD_DIM), F32),
            vmem((2, CHIPS, 10, HEAD_DIM), F32),
            dma((12,)), dma((1,)), dma((2, 4)), dma((1,)), dma((3,)), dma((3,)), dma((8,)), dma((8,)), dma((8,)), dma((8,)),
            dma((1,)), dma((1,)), dma((1,)), dma((1,)), dma((2,)), dma((1,)), dma((4,)), dma((4,)), dma((4,)),
        ],
        compiler_params=pltpu.CompilerParams(collective_id=0, has_side_effects=True, vmem_limit_bytes=60 * 2 ** 20),
    )(*args)


CHUNKS = 8


def cache_kernel(pos_ref, kv_ref, kc_hbm, vc_hbm, ko_hbm, vo_hbm, new_ref, kbuf, vbuf, isem, osem):
    start = lax.axis_index("sp") * SLOTS
    per = SEQS // CHUNKS

    def copies(i, out):
        rows = pl.ds(i * per, per)
        if out:
            return (pltpu.make_async_copy(kbuf.at[rows], ko_hbm.at[rows], osem.at[0, i]),
                    pltpu.make_async_copy(vbuf.at[rows], vo_hbm.at[rows], osem.at[1, i]))
        return (pltpu.make_async_copy(kc_hbm.at[rows], kbuf.at[rows], isem.at[0, i]),
                pltpu.make_async_copy(vc_hbm.at[rows], vbuf.at[rows], isem.at[1, i]))

    for i in range(CHUNKS):
        for c in copies(i, False):
            c.start()
    low = iota((SEQS, 8, HEAD_DIM), 1) < 4
    first, second = kv_ref[0], kv_ref[1]
    new_ref[:, 0] = jnp.where(low, first, pltpu.roll(second, 4, 1)).astype(BF16)
    new_ref[:, 1] = jnp.where(low, pltpu.roll(first, 4, 1), second).astype(BF16)
    for i in range(CHUNKS):
        for c in copies(i, False):
            c.wait()

        @pl.loop(i * per, (i + 1) * per)
        def _(s):
            slot = pos_ref[s] - start

            @pl.when((slot >= 0) & (slot < SLOTS))
            def _():
                kbuf[s, slot] = new_ref[s, 0]
                vbuf[s, slot] = new_ref[s, 1]

        for c in copies(i, True):
            c.start()
    for i in range(CHUNKS):
        for c in copies(i, True):
            c.wait()


def cache_call(*args):
    hbm = pl.BlockSpec(memory_space=pl.ANY)
    blk = pl.BlockSpec(memory_space=pltpu.VMEM)
    shape = (SEQS, SLOTS, KV_HEADS, HEAD_DIM)
    dma = pltpu.SemaphoreType.DMA
    return pl.pallas_call(
        cache_kernel,
        name="cache_write",
        out_shape=(jax.ShapeDtypeStruct(shape, BF16), jax.ShapeDtypeStruct(shape, BF16),
                   jax.ShapeDtypeStruct((SEQS, 2, KV_HEADS, HEAD_DIM), BF16)),
        in_specs=[pl.BlockSpec(memory_space=pltpu.SMEM), blk, hbm, hbm],
        out_specs=(hbm, hbm, blk),
        scratch_shapes=[pltpu.VMEM(shape, BF16), pltpu.VMEM(shape, BF16), dma((2, CHUNKS)), dma((2, CHUNKS))],
    )(*args)


def solution(mesh):
    cache_spec = P('dp', 'sp', None, None)

    def device_step(tokens, positions, k_cache, v_cache, w_q, w_k, w_v, w_o, attn_norm, q_norm, k_norm):
        inv = np.float32(ROPE_THETA) ** (-np.arange(HEAD_DIM // 2, dtype=np.float32) * np.float32(2.0) / np.float32(HEAD_DIM))
        freq = jnp.asarray(np.concatenate([inv, inv])[None, :].astype(np.float32))
        flat = (SEQS, SLOTS * KV_HEADS, HEAD_DIM)
        block_out, kv = step_call(positions, tokens, attn_norm[None, :], q_norm[None, :], k_norm[None, :], freq, w_q, w_k, w_v,
                                  w_o, k_cache.reshape(flat), v_cache.reshape(flat))
        k_out, v_out, new_kv = cache_call(positions, kv, k_cache, v_cache)
        return block_out, k_out, v_out, new_kv

    return jax.shard_map(device_step, mesh=mesh, in_specs=(P('dp', None), P('dp'), cache_spec, cache_spec, P(), P(), P(), P(), P(), P(), P()), out_specs=(P('dp', None), cache_spec, cache_spec, P('dp', None, None, None)), check_vma=False)
```

```python
import functools

import jax
import jax.numpy as jnp
import numpy as np
from jax import lax
from jax.experimental import pallas as pl
from jax.experimental.pallas import tpu as pltpu
from jax.sharding import PartitionSpec as P

NORM_EPS = 1e-6
ROPE_THETA = 1000000.0
NEG_FILL = -1e30
SEQS, DIM, HEADS, KV_HEADS, HEAD_DIM, SLOTS = 64, 2560, 32, 8, 128, 16
HALF = HEADS // 2
CHIPS = 64
SCALE = HEAD_DIM ** -0.5
F32, BF16 = jnp.float32, jnp.bfloat16
MESH = pl.DeviceIdType.MESH
DEPTH = 3
LAG = 5


def rms(values, gain):
    return values * lax.rsqrt(jnp.mean(values * values, axis=-1, keepdims=True) + NORM_EPS) * gain


def iota(shape, axis):
    return lax.broadcasted_iota(jnp.int32, shape, axis)


def pick(row, lane):
    spread = jnp.broadcast_to(row, (HALF, HEAD_DIM))
    return jnp.sum(jnp.where(lane, spread, 0.0), axis=-1, keepdims=True)


def step_kernel(pos_ref, tok_hbm, an_hbm, qn_hbm, kn_hbm, freq_hbm, wq_hbm, wk_hbm, wv_hbm, wo_hbm, kc_hbm, vc_hbm,
                out_hbm, kv_hbm,
                tok_ref, an_ref, qn_ref, kn_ref, freq_ref, isem, outsem, hid, cosr, sinr, wbuf, wobuf, kbuf, vbuf, gbuf, wts, obuf, oin, st, stin, fac, osend, stsend, rbuf, rst, out_ref,
                lhs, ypart, yin, ysend, ybuf,
                wsem, wosem, csem, kvsem, gsend, grecv, dsend, drecv, dssend, dsrecv,
                ssend, srecv, tsend, trecv, ysem, bsend, brecv, fsend, frecv):
    me = lax.axis_index("sp")
    chip, core = me // 2, me % 2
    zed = chip // 16
    mate = chip * 2 + (1 - core)
    start = me * SLOTS

    def dev(index):
        return (lax.axis_index("dp"), index)

    barrier = pltpu.get_barrier_semaphore()
    pl.semaphore_signal(barrier, inc=1, device_id=dev(mate), device_id_type=MESH)

    @pl.loop(1, CHIPS)
    def _(off):
        pl.semaphore_signal(barrier, inc=1, device_id=dev(lax.rem(chip + off, CHIPS) * 2 + core), device_id_type=MESH)

    def wcopy(src, col, tile):
        return pltpu.make_async_copy(src.at[:, pl.ds(pl.multiple_of(col, 256), 256)], wbuf.at[tile], wsem.at[tile])

    def tile_copy(t):
        if t < 2:
            return wcopy(wk_hbm, core * 512 + t * 256, t)
        if t < 4:
            return wcopy(wv_hbm, core * 512 + (t - 2) * 256, t)
        return wcopy(wq_hbm, core * 2048 + (t - 4) * 256, t)

    def kvload(i):
        rows = pl.ds(i * 16, 16)
        return (pltpu.make_async_copy(kc_hbm.at[rows], kbuf.at[rows], csem.at[0, i]),
                pltpu.make_async_copy(vc_hbm.at[rows], vbuf.at[rows], csem.at[1, i]))

    def tile_ready(t):
        tile_copy(t).wait()
        if t + DEPTH < 12:
            tile_copy(t + DEPTH).start()
        elif t + DEPTH < 14:
            for c in kvload(2 * (t + DEPTH - 12)) + kvload(2 * (t + DEPTH - 12) + 1):
                c.start()

    inputs = [pltpu.make_async_copy(a, b, isem.at[i]) for i, (a, b) in enumerate(
        [(tok_hbm, tok_ref), (an_hbm, an_ref), (freq_hbm, freq_ref), (kn_hbm, kn_ref), (qn_hbm, qn_ref)])]
    for c in inputs:
        c.start()
    for t in range(DEPTH):
        tile_copy(t).start()
    for c in inputs:
        c.wait()

    tok = tok_ref[...].astype(F32)
    hid[...] = rms(tok, an_ref[...].astype(F32).reshape(1, DIM)).astype(BF16)
    row8 = iota((SEQS, HEAD_DIM), 0)
    posv = jnp.zeros((SEQS, HEAD_DIM), jnp.int32)
    for s in range(SEQS):
        posv = jnp.where(row8 == s, pos_ref[s], posv)
    angle = posv.astype(F32) * freq_ref[...]
    cosr[...] = jnp.cos(angle)
    sinr[...] = jnp.where(iota((SEQS, HEAD_DIM), 1) < HEAD_DIM // 2, -1.0, 1.0) * jnp.sin(angle)

    def project(tile):
        return jnp.dot(hid[...], wbuf[tile], preferred_element_type=F32).astype(BF16).astype(F32)

    def rope(head, gain):
        normed = rms(head, gain)
        turned = normed * cosr[...] + pltpu.roll(normed, HEAD_DIM // 2, 1) * sinr[...]
        return turned.astype(BF16).astype(F32)

    for t in range(4):
        tile_ready(t)
        res = project(t)
        for h in range(2):
            head = res[:, h * 128:(h + 1) * 128]
            gbuf[4 + core, :, 2 * t + h, :] = rope(head, kn_ref[...].astype(F32)) if t < 2 else head

    def gcopy(group, slot):
        return pltpu.make_async_remote_copy(src_ref=gbuf.at[group], dst_ref=gbuf.at[group], send_sem=gsend.at[slot],
                                            recv_sem=grecv.at[slot], device_id=dev(mate), device_id_type=MESH)

    for g in range(2):
        for t4 in range(4):
            t = 4 + g * 4 + t4
            tile_ready(t)
            res = project(t)
            for h in range(2):
                gbuf[2 * core + g, :, 2 * t4 + h, :] = rope(res[:, h * 128:(h + 1) * 128], qn_ref[...].astype(F32))
        if g == 0:
            pl.semaphore_wait(barrier, CHIPS)
            gcopy(4 + core, 2).start()
        gcopy(2 * core + g, g).start()

    wocopy = pltpu.make_async_copy(wo_hbm.at[pl.ds(pl.multiple_of(core * 2048, 2048), 2048)], wobuf, wosem.at[0])
    wocopy.start()
    for slot in range(3):
        gcopy(4 + core if slot == 2 else 2 * core + slot, slot).wait()
    kvout = pltpu.make_async_copy(gbuf.at[pl.ds(4, 2)], kv_hbm, kvsem.at[0])
    kvout.start()
    for i in range(4):
        for c in kvload(i):
            c.wait()

    def block_of(i):
        return lax.rem(zed + 2 + 3 * (i // 2), 4) * 2 + lax.rem(i, 2)

    row32, col32 = iota((HEADS, HEAD_DIM), 0), iota((HEADS, HEAD_DIM), 1)
    same_head = (col32 % KV_HEADS) == (row32 // 4)
    slot_of = col32 // KV_HEADS + start
    row16, lane16 = iota((HALF, HEAD_DIM), 0), iota((HALF, HEAD_DIM), 1)

    def weigh(blk):
        acc = [[jnp.zeros((HALF, HEAD_DIM), F32) for _ in range(2)] for _ in range(2)]
        for s8 in range(8):
            s = blk * 8 + s8
            q = jnp.concatenate([gbuf[g, s] for g in range(4)], axis=0).astype(BF16)
            scores = lax.dot_general(q, kbuf[s], (((1,), (1,)), ((), ())), preferred_element_type=F32) * SCALE
            live = same_head & (slot_of < pos_ref[s])
            scores = jnp.where(live, scores, NEG_FILL)
            peak = jnp.max(scores, axis=-1, keepdims=True)
            weights = jnp.where(live, jnp.exp(scores - peak), 0.0)
            total = jnp.sum(weights, axis=-1, keepdims=True)
            wts[s] = weights.astype(BF16)
            here = lane16 == s8 * HALF + row16
            for half in range(2):
                cut = slice(half * HALF, (half + 1) * HALF)
                acc[half][0] += jnp.where(here, peak[cut], 0.0)
                acc[half][1] += jnp.where(here, total[cut], 0.0)
        for half in range(2):
            for k in range(2):
                st[half, blk, pl.ds(k, 1), :] = jnp.sum(acc[half][k], axis=0, keepdims=True)

    def mix(i):
        blk = block_of(i)
        for s8 in range(8):
            s = blk * 8 + s8
            mixed = jnp.dot(wts[s], vbuf[s], preferred_element_type=F32)
            for half in range(2):
                obuf[half, s] = mixed[half * HALF:(half + 1) * HALF]
        ocopy(i).start()

    def ocopy(i):
        rows = pl.ds(block_of(i) * 8, 8)
        return pltpu.make_async_remote_copy(src_ref=obuf.at[1 - core, rows], dst_ref=oin.at[rows], send_sem=dsend.at[i],
                                            recv_sem=drecv.at[i], device_id=dev(mate), device_id_type=MESH)

    def merge(i):
        blk = block_of(i)
        ocopy(i).wait()
        f0, f1 = fac[0, pl.ds(blk, 1), :], fac[1, pl.ds(blk, 1), :]
        for s8 in range(8):
            s = blk * 8 + s8
            here = lane16 == s8 * HALF + row16
            osend[s] = obuf[core, s] * pick(f0, here) + oin[s] * pick(f1, here)
        for s8 in range(8):
            s = blk * 8 + s8

            @pl.when(s != chip)
            def _():
                pltpu.make_async_remote_copy(src_ref=osend.at[s], dst_ref=rbuf.at[chip], send_sem=ssend.at[0], recv_sem=srecv.at[0],
                                             device_id=dev(s * 2 + core), device_id_type=MESH).start()

    @pl.loop(0, 8)
    def _(blk):
        weigh(blk)

    stcopy = pltpu.make_async_remote_copy(src_ref=st.at[1 - core], dst_ref=stin, send_sem=dssend.at[0], recv_sem=dsrecv.at[0],
                                          device_id=dev(mate), device_id_type=MESH)
    stcopy.start()

    @pl.loop(0, LAG)
    def _(i):
        mix(i)

    stcopy.wait()
    m0, l0, m1, l1 = st[core, :, 0, :], st[core, :, 1, :], stin[:, 0, :], stin[:, 1, :]
    top = jnp.maximum(m0, m1)
    f0, f1 = jnp.exp(m0 - top), jnp.exp(m1 - top)
    fac[0], fac[1] = f0, f1
    stsend[:, 0, :] = top
    stsend[:, 1, :] = l0 * f0 + l1 * f1

    @pl.loop(1, CHIPS)
    def _(off):
        s = lax.rem(chip + off, CHIPS)
        pltpu.make_async_remote_copy(src_ref=stsend.at[s // 8], dst_ref=rst.at[chip], send_sem=tsend.at[0], recv_sem=trecv.at[0],
                                     device_id=dev(s * 2 + core), device_id_type=MESH).start()

    @pl.loop(LAG, 8 + LAG)
    def _(i):
        @pl.when(i < 8)
        def _():
            mix(i)

        merge(i - LAG)

    rst[chip] = stsend[chip // 8]
    rbuf[chip] = osend[chip]

    def all_of(src, dst, send, recv):
        return pltpu.make_async_remote_copy(src_ref=src, dst_ref=dst, send_sem=send, recv_sem=recv, device_id=dev(mate),
                                            device_id_type=MESH)

    others = pl.ds(0, CHIPS - 1)
    all_of(rst.at[others], rst.at[others], tsend.at[0], trecv.at[0]).wait_recv()
    all_of(rbuf.at[others], rbuf.at[others], ssend.at[0], srecv.at[0]).wait_recv()

    here = lane16 == lax.rem(chip, 8) * HALF + row16
    tops = rst[:, 0, :]
    top = jnp.max(tops, axis=0, keepdims=True)
    facs = jnp.exp(tops - top)
    total = pick(jnp.sum(rst[:, 1, :] * facs, axis=0, keepdims=True), here)
    acc = jnp.zeros((HALF, HEAD_DIM), F32)
    for c in range(CHIPS):
        acc += rbuf[c] * pick(facs[c:c + 1], here)
    q_own = jnp.concatenate([gbuf[2 * core, chip], gbuf[2 * core + 1, chip]], axis=0)
    kv_own = gbuf[4 + core, chip]
    k_own = jnp.concatenate([jnp.broadcast_to(kv_own[i:i + 1], (4, HEAD_DIM)) for i in range(4)], axis=0)
    v_own = jnp.concatenate([jnp.broadcast_to(kv_own[4 + i:5 + i], (4, HEAD_DIM)) for i in range(4)], axis=0)
    s_own = jnp.sum(q_own * k_own, axis=-1, keepdims=True) * SCALE
    top = pick(top, here)
    peak = jnp.maximum(top, s_own)
    f_old, f_new = jnp.exp(top - peak), jnp.exp(s_own - peak)
    attn = (acc * f_old + v_own * f_new) / (total * f_old + f_new)
    for h in range(HALF):
        lhs[:, h * 128:(h + 1) * 128] = jnp.where(row16 == h, attn, 0.0).astype(BF16)

    wocopy.wait()

    def out_cols(half, slot):
        for n in range(5):
            cols = pl.ds(pl.multiple_of(half * 1280 + n * 256, 256), 256)
            res = jnp.dot(lhs[...], wobuf[:, cols], preferred_element_type=F32)
            res = jnp.sum(res, axis=0, keepdims=True)
            for k in range(2):
                ypart[slot, pl.ds(2 * n + k, 1), :] = res[:, k * 128:(k + 1) * 128]

    out_cols(1 - core, 0)
    ycopy = pltpu.make_async_remote_copy(src_ref=ypart.at[0], dst_ref=yin, send_sem=ysem.at[0], recv_sem=ysem.at[1],
                                         device_id=dev(mate), device_id_type=MESH)
    ycopy.start()
    out_cols(core, 1)
    ycopy.wait()
    ysend[...] = ypart[1] + yin[...]

    def bcopy(s, group):
        return pltpu.make_async_remote_copy(src_ref=ysend, dst_ref=ybuf.at[core, chip], send_sem=bsend.at[0],
                                            recv_sem=brecv.at[group], device_id=dev(s * 2 + core), device_id_type=MESH)

    @pl.loop(1, CHIPS)
    def _(k):
        s = lax.rem(chip + 1 + lax.rem(k + 30, CHIPS - 1), CHIPS)
        bcopy(s, lax.rem(zed - s // 16 + 4, 4)).start()

    ybuf[core, chip] = ysend[...]

    def slab(half, group):
        return ybuf.at[half, pl.ds(lax.rem(zed + group, 4) * 16, 16)]

    def fcopy(half, group):
        ref = slab(half, group)
        return pltpu.make_async_remote_copy(src_ref=ref, dst_ref=ref, send_sem=fsend.at[group], recv_sem=frecv.at[group],
                                            device_id=dev(mate), device_id_type=MESH)

    for group in (0, 1, 3, 2):
        ref = ybuf.at[core, pl.ds(0, 15 if group == 0 else 16)]
        all_of(ref, ref, bsend.at[0], brecv.at[group]).wait_recv()
        fcopy(core, group).start()
    for group in (0, 1, 3, 2):
        fcopy(1 - core, group).wait_recv()

    for half in range(2):
        for k in range(10):
            cols = slice(half * 1280 + k * 128, half * 1280 + (k + 1) * 128)
            out_ref[:, cols] = (tok_ref[:, cols].astype(F32) + ybuf[half, :, k, :]).astype(BF16)

    outcopy = pltpu.make_async_copy(out_ref, out_hbm, outsem.at[0])
    outcopy.start()
    for group in range(4):
        fcopy(core, group).wait_send()
    all_of(rst.at[others], rst.at[others], tsend.at[0], trecv.at[0]).wait_send()
    all_of(rbuf.at[others], rbuf.at[others], ssend.at[0], srecv.at[0]).wait_send()
    rest = ybuf.at[0, others]
    all_of(rest, rest, bsend.at[0], brecv.at[0]).wait_send()
    kvout.wait()
    outcopy.wait()


def step_call(*args):
    dma = pltpu.SemaphoreType.DMA
    vmem = pltpu.VMEM
    hbm = pl.BlockSpec(memory_space=pl.ANY)
    return pl.pallas_call(
        step_kernel,
        name="decode_step",
        out_shape=(jax.ShapeDtypeStruct((SEQS, DIM), BF16), jax.ShapeDtypeStruct((2, SEQS, 8, HEAD_DIM), F32)),
        in_specs=[pl.BlockSpec(memory_space=pltpu.SMEM)] + [hbm] * 11,
        out_specs=(hbm, hbm),
        scratch_shapes=[
            vmem((SEQS, DIM), BF16), vmem((DIM,), BF16), vmem((1, HEAD_DIM), BF16), vmem((1, HEAD_DIM), BF16), vmem((1, HEAD_DIM), F32),
            dma((5,)), dma((1,)),
            vmem((SEQS, DIM), BF16), vmem((SEQS, HEAD_DIM), F32), vmem((SEQS, HEAD_DIM), F32),
            vmem((12, DIM, 256), BF16), vmem((2048, DIM), BF16),
            vmem((SEQS, 128, HEAD_DIM), BF16), vmem((SEQS, 128, HEAD_DIM), BF16),
            vmem((6, SEQS, 8, HEAD_DIM), F32),
            vmem((SEQS, HEADS, HEAD_DIM), BF16), vmem((2, SEQS, HALF, HEAD_DIM), F32), vmem((SEQS, HALF, HEAD_DIM), F32),
            vmem((2, 8, 2, HEAD_DIM), F32), vmem((8, 2, HEAD_DIM), F32), vmem((2, 8, HEAD_DIM), F32),
            vmem((SEQS, HALF, HEAD_DIM), F32), vmem((8, 2, HEAD_DIM), F32),
            vmem((CHIPS, HALF, HEAD_DIM), F32), vmem((CHIPS, 2, HEAD_DIM), F32), vmem((SEQS, DIM), BF16),
            vmem((HALF, 2048), BF16), vmem((2, 10, HEAD_DIM), F32), vmem((10, HEAD_DIM), F32), vmem((10, HEAD_DIM), F32),
            vmem((2, CHIPS, 10, HEAD_DIM), F32),
            dma((12,)), dma((1,)), dma((2, 4)), dma((1,)), dma((3,)), dma((3,)), dma((8,)), dma((8,)), dma((1,)), dma((1,)),
            dma((1,)), dma((1,)), dma((1,)), dma((1,)), dma((2,)), dma((1,)), dma((4,)), dma((4,)), dma((4,)),
        ],
        compiler_params=pltpu.CompilerParams(collective_id=0, has_side_effects=True, vmem_limit_bytes=60 * 2 ** 20),
    )(*args)


CHUNKS = 8


def cache_kernel(pos_ref, kv_hbm, row_hbm, kc_hbm, vc_hbm, ko_hbm, vo_hbm, new_hbm, out_hbm,
                 kv, new, row, kbuf, vbuf, isem, osem, ssem):
    start = lax.axis_index("sp") * SLOTS
    per = SEQS // CHUNKS

    def copies(i, out):
        rows = pl.ds(i * per, per)
        if out:
            return (pltpu.make_async_copy(kbuf.at[rows], ko_hbm.at[rows], osem.at[0, i]),
                    pltpu.make_async_copy(vbuf.at[rows], vo_hbm.at[rows], osem.at[1, i]))
        return (pltpu.make_async_copy(kc_hbm.at[rows], kbuf.at[rows], isem.at[0, i]),
                pltpu.make_async_copy(vc_hbm.at[rows], vbuf.at[rows], isem.at[1, i]))

    kvload, rowload = pltpu.make_async_copy(kv_hbm, kv, ssem.at[0]), pltpu.make_async_copy(row_hbm, row, ssem.at[1])
    kvload.start()
    rowload.start()
    for i in range(CHUNKS):
        for c in copies(i, False):
            c.start()
    kvload.wait()
    low = iota((SEQS, 8, HEAD_DIM), 1) < 4
    first, second = kv[0], kv[1]
    new[:, 0] = jnp.where(low, first, pltpu.roll(second, 4, 1)).astype(BF16)
    new[:, 1] = jnp.where(low, pltpu.roll(first, 4, 1), second).astype(BF16)
    small = [pltpu.make_async_copy(new, new_hbm, ssem.at[2]), pltpu.make_async_copy(row, out_hbm, ssem.at[3])]
    small[0].start()
    rowload.wait()
    small[1].start()
    for i in range(CHUNKS):
        for c in copies(i, False):
            c.wait()

        @pl.loop(i * per, (i + 1) * per)
        def _(s):
            slot = pos_ref[s] - start

            @pl.when((slot >= 0) & (slot < SLOTS))
            def _():
                kbuf[s, slot] = new[s, 0]
                vbuf[s, slot] = new[s, 1]

        for c in copies(i, True):
            c.start()
    for c in small:
        c.wait()
    for i in range(CHUNKS):
        for c in copies(i, True):
            c.wait()


def cache_call(*args):
    hbm = pl.BlockSpec(memory_space=pl.ANY)
    shape = (SEQS, SLOTS, KV_HEADS, HEAD_DIM)
    new = (SEQS, 2, KV_HEADS, HEAD_DIM)
    dma = pltpu.SemaphoreType.DMA
    return pl.pallas_call(
        cache_kernel,
        name="cache_write",
        out_shape=(jax.ShapeDtypeStruct(shape, BF16), jax.ShapeDtypeStruct(shape, BF16), jax.ShapeDtypeStruct(new, BF16),
                   jax.ShapeDtypeStruct((SEQS, DIM), BF16)),
        in_specs=[pl.BlockSpec(memory_space=pltpu.SMEM)] + [hbm] * 4,
        out_specs=(hbm,) * 4,
        scratch_shapes=[pltpu.VMEM((2, SEQS, 8, HEAD_DIM), F32), pltpu.VMEM(new, BF16), pltpu.VMEM((SEQS, DIM), BF16),
                        pltpu.VMEM(shape, BF16), pltpu.VMEM(shape, BF16), dma((2, CHUNKS)), dma((2, CHUNKS)), dma((4,))],
    )(*args)


def solution(mesh):
    cache_spec = P('dp', 'sp', None, None)

    def device_step(tokens, positions, k_cache, v_cache, w_q, w_k, w_v, w_o, attn_norm, q_norm, k_norm):
        inv = np.float32(ROPE_THETA) ** (-np.arange(HEAD_DIM // 2, dtype=np.float32) * np.float32(2.0) / np.float32(HEAD_DIM))
        freq = jnp.asarray(np.concatenate([inv, inv])[None, :].astype(np.float32))
        flat = (SEQS, SLOTS * KV_HEADS, HEAD_DIM)
        row, kv = step_call(positions, tokens, attn_norm, q_norm[None, :], k_norm[None, :], freq, w_q, w_k, w_v,
                                  w_o, k_cache.reshape(flat), v_cache.reshape(flat))
        k_out, v_out, new_kv, block_out = cache_call(positions, kv, row, k_cache, v_cache)
        return block_out, k_out, v_out, new_kv

    return jax.shard_map(device_step, mesh=mesh, in_specs=(P('dp', None), P('dp'), cache_spec, cache_spec, P(), P(), P(), P(), P(), P(), P()), out_specs=(P('dp', None), cache_spec, cache_spec, P('dp', None, None, None)), check_vma=False)
```

```python
import functools

import jax
import jax.numpy as jnp
import numpy as np
from jax import lax
from jax.experimental import pallas as pl
from jax.experimental.pallas import tpu as pltpu
from jax.sharding import PartitionSpec as P

NORM_EPS = 1e-6
ROPE_THETA = 1000000.0
NEG_FILL = -1e30
SEQS, DIM, HEADS, KV_HEADS, HEAD_DIM, SLOTS = 64, 2560, 32, 8, 128, 16
HALF = HEADS // 2
CHIPS = 64
SCALE = HEAD_DIM ** -0.5
F32, BF16 = jnp.float32, jnp.bfloat16
MESH = pl.DeviceIdType.MESH
DEPTH = 3
LAG = 5


def rms(values, gain):
    return values * lax.rsqrt(jnp.mean(values * values, axis=-1, keepdims=True) + NORM_EPS) * gain


def iota(shape, axis):
    return lax.broadcasted_iota(jnp.int32, shape, axis)


def pick(row, lane):
    spread = jnp.broadcast_to(row, (HALF, HEAD_DIM))
    return jnp.sum(jnp.where(lane, spread, 0.0), axis=-1, keepdims=True)


def step_kernel(pos_ref, tok_hbm, an_hbm, qn_hbm, kn_hbm, freq_hbm, wq_hbm, wk_hbm, wv_hbm, wo_hbm, kc_hbm, vc_hbm,
                out_hbm, kv_hbm, kbuf, vbuf,
                tok_ref, an_ref, qn_ref, kn_ref, freq_ref, isem, outsem, hid, cosr, sinr, wbuf, wobuf, gbuf, wts, obuf, oin, st, stin, fac, osend, stsend, rbuf, rst, out_ref,
                lhs, ypart, yin, ysend, ybuf,
                wsem, wosem, csem, kvsem, gsend, grecv, dsend, drecv, dssend, dsrecv,
                ssend, srecv, tsend, trecv, ysem, bsend, brecv, fsend, frecv):
    me = lax.axis_index("sp")
    chip, core = me // 2, me % 2
    zed = chip // 16
    mate = chip * 2 + (1 - core)
    start = me * SLOTS

    def dev(index):
        return (lax.axis_index("dp"), index)

    barrier = pltpu.get_barrier_semaphore()
    pl.semaphore_signal(barrier, inc=1, device_id=dev(mate), device_id_type=MESH)

    @pl.loop(1, CHIPS)
    def _(off):
        pl.semaphore_signal(barrier, inc=1, device_id=dev(lax.rem(chip + off, CHIPS) * 2 + core), device_id_type=MESH)

    def wcopy(src, col, tile):
        return pltpu.make_async_copy(src.at[:, pl.ds(pl.multiple_of(col, 256), 256)], wbuf.at[tile], wsem.at[tile])

    def tile_copy(t):
        if t < 2:
            return wcopy(wk_hbm, core * 512 + t * 256, t)
        if t < 4:
            return wcopy(wv_hbm, core * 512 + (t - 2) * 256, t)
        return wcopy(wq_hbm, core * 2048 + (t - 4) * 256, t)

    def kvload(i):
        rows = pl.ds(i * 16, 16)
        return (pltpu.make_async_copy(kc_hbm.at[rows], kbuf.at[rows], csem.at[0, i]),
                pltpu.make_async_copy(vc_hbm.at[rows], vbuf.at[rows], csem.at[1, i]))

    def tile_ready(t):
        tile_copy(t).wait()
        if t + DEPTH < 12:
            tile_copy(t + DEPTH).start()
        elif t + DEPTH < 14:
            for c in kvload(2 * (t + DEPTH - 12)) + kvload(2 * (t + DEPTH - 12) + 1):
                c.start()

    inputs = [pltpu.make_async_copy(a, b, isem.at[i]) for i, (a, b) in enumerate(
        [(tok_hbm, tok_ref), (an_hbm, an_ref), (freq_hbm, freq_ref), (kn_hbm, kn_ref), (qn_hbm, qn_ref)])]
    for c in inputs:
        c.start()
    for t in range(DEPTH):
        tile_copy(t).start()
    for c in inputs:
        c.wait()

    tok = tok_ref[...].astype(F32)
    hid[...] = rms(tok, an_ref[...].astype(F32).reshape(1, DIM)).astype(BF16)
    row8 = iota((SEQS, HEAD_DIM), 0)
    posv = jnp.zeros((SEQS, HEAD_DIM), jnp.int32)
    for s in range(SEQS):
        posv = jnp.where(row8 == s, pos_ref[s], posv)
    angle = posv.astype(F32) * freq_ref[...]
    cosr[...] = jnp.cos(angle)
    sinr[...] = jnp.where(iota((SEQS, HEAD_DIM), 1) < HEAD_DIM // 2, -1.0, 1.0) * jnp.sin(angle)

    def project(tile):
        return jnp.dot(hid[...], wbuf[tile], preferred_element_type=F32).astype(BF16).astype(F32)

    def rope(head, gain):
        normed = rms(head, gain)
        turned = normed * cosr[...] + pltpu.roll(normed, HEAD_DIM // 2, 1) * sinr[...]
        return turned.astype(BF16).astype(F32)

    for t in range(4):
        tile_ready(t)
        res = project(t)
        for h in range(2):
            head = res[:, h * 128:(h + 1) * 128]
            gbuf[4 + core, :, 2 * t + h, :] = rope(head, kn_ref[...].astype(F32)) if t < 2 else head

    def gcopy(group, slot):
        return pltpu.make_async_remote_copy(src_ref=gbuf.at[group], dst_ref=gbuf.at[group], send_sem=gsend.at[slot],
                                            recv_sem=grecv.at[slot], device_id=dev(mate), device_id_type=MESH)

    for g in range(2):
        for t4 in range(4):
            t = 4 + g * 4 + t4
            tile_ready(t)
            res = project(t)
            for h in range(2):
                gbuf[2 * core + g, :, 2 * t4 + h, :] = rope(res[:, h * 128:(h + 1) * 128], qn_ref[...].astype(F32))
        if g == 0:
            pl.semaphore_wait(barrier, CHIPS)
            gcopy(4 + core, 2).start()
        gcopy(2 * core + g, g).start()

    wocopy = pltpu.make_async_copy(wo_hbm.at[pl.ds(pl.multiple_of(core * 2048, 2048), 2048)], wobuf, wosem.at[0])
    wocopy.start()
    for slot in range(3):
        gcopy(4 + core if slot == 2 else 2 * core + slot, slot).wait()
    kvout = pltpu.make_async_copy(gbuf.at[pl.ds(4, 2)], kv_hbm, kvsem.at[0])
    kvout.start()
    for i in range(4):
        for c in kvload(i):
            c.wait()

    def block_of(i):
        return lax.rem(zed + 2 + i // 2 - (i // 4) * (2 * (i // 2) - 1), 4) * 2 + lax.rem(i, 2)

    row32, col32 = iota((HEADS, HEAD_DIM), 0), iota((HEADS, HEAD_DIM), 1)
    same_head = (col32 % KV_HEADS) == (row32 // 4)
    slot_of = col32 // KV_HEADS + start
    row16, lane16 = iota((HALF, HEAD_DIM), 0), iota((HALF, HEAD_DIM), 1)

    def weigh(blk):
        acc = [[jnp.zeros((HALF, HEAD_DIM), F32) for _ in range(2)] for _ in range(2)]
        for s8 in range(8):
            s = blk * 8 + s8
            q = jnp.concatenate([gbuf[g, s] for g in range(4)], axis=0).astype(BF16)
            scores = lax.dot_general(q, kbuf[s], (((1,), (1,)), ((), ())), preferred_element_type=F32) * SCALE
            live = same_head & (slot_of < pos_ref[s])
            scores = jnp.where(live, scores, NEG_FILL)
            peak = jnp.max(scores, axis=-1, keepdims=True)
            weights = jnp.where(live, jnp.exp(scores - peak), 0.0)
            total = jnp.sum(weights, axis=-1, keepdims=True)
            wts[s] = weights.astype(BF16)
            here = lane16 == s8 * HALF + row16
            for half in range(2):
                cut = slice(half * HALF, (half + 1) * HALF)
                acc[half][0] += jnp.where(here, peak[cut], 0.0)
                acc[half][1] += jnp.where(here, total[cut], 0.0)
        for half in range(2):
            for k in range(2):
                st[half, blk, pl.ds(k, 1), :] = jnp.sum(acc[half][k], axis=0, keepdims=True)

    def mix(i):
        blk = block_of(i)
        for s8 in range(8):
            s = blk * 8 + s8
            mixed = jnp.dot(wts[s], vbuf[s], preferred_element_type=F32)
            for half in range(2):
                obuf[half, s] = mixed[half * HALF:(half + 1) * HALF]
        ocopy(i).start()

    def ocopy(i):
        rows = pl.ds(block_of(i) * 8, 8)
        return pltpu.make_async_remote_copy(src_ref=obuf.at[1 - core, rows], dst_ref=oin.at[rows], send_sem=dsend.at[i],
                                            recv_sem=drecv.at[i], device_id=dev(mate), device_id_type=MESH)

    def merge(i):
        blk = block_of(i)
        ocopy(i).wait()
        f0, f1 = fac[0, pl.ds(blk, 1), :], fac[1, pl.ds(blk, 1), :]
        for s8 in range(8):
            s = blk * 8 + s8
            here = lane16 == s8 * HALF + row16
            osend[s] = obuf[core, s] * pick(f0, here) + oin[s] * pick(f1, here)
        for s8 in range(8):
            s = blk * 8 + s8

            @pl.when(s != chip)
            def _():
                pltpu.make_async_remote_copy(src_ref=osend.at[s], dst_ref=rbuf.at[chip], send_sem=ssend.at[0], recv_sem=srecv.at[0],
                                             device_id=dev(s * 2 + core), device_id_type=MESH).start()

    @pl.loop(0, 8)
    def _(blk):
        weigh(blk)

    stcopy = pltpu.make_async_remote_copy(src_ref=st.at[1 - core], dst_ref=stin, send_sem=dssend.at[0], recv_sem=dsrecv.at[0],
                                          device_id=dev(mate), device_id_type=MESH)
    stcopy.start()

    @pl.loop(0, LAG)
    def _(i):
        mix(i)

    stcopy.wait()
    m0, l0, m1, l1 = st[core, :, 0, :], st[core, :, 1, :], stin[:, 0, :], stin[:, 1, :]
    top = jnp.maximum(m0, m1)
    f0, f1 = jnp.exp(m0 - top), jnp.exp(m1 - top)
    fac[0], fac[1] = f0, f1
    stsend[:, 0, :] = top
    stsend[:, 1, :] = l0 * f0 + l1 * f1

    @pl.loop(1, CHIPS)
    def _(off):
        s = lax.rem(chip + off, CHIPS)
        pltpu.make_async_remote_copy(src_ref=stsend.at[s // 8], dst_ref=rst.at[chip], send_sem=tsend.at[0], recv_sem=trecv.at[0],
                                     device_id=dev(s * 2 + core), device_id_type=MESH).start()

    @pl.loop(LAG, 8 + LAG)
    def _(i):
        @pl.when(i < 8)
        def _():
            mix(i)

        merge(i - LAG)

    rst[chip] = stsend[chip // 8]
    rbuf[chip] = osend[chip]

    def all_of(src, dst, send, recv):
        return pltpu.make_async_remote_copy(src_ref=src, dst_ref=dst, send_sem=send, recv_sem=recv, device_id=dev(mate),
                                            device_id_type=MESH)

    others = pl.ds(0, CHIPS - 1)
    all_of(rst.at[others], rst.at[others], tsend.at[0], trecv.at[0]).wait_recv()
    all_of(rbuf.at[others], rbuf.at[others], ssend.at[0], srecv.at[0]).wait_recv()

    here = lane16 == lax.rem(chip, 8) * HALF + row16
    tops = rst[:, 0, :]
    top = jnp.max(tops, axis=0, keepdims=True)
    facs = jnp.exp(tops - top)
    total = pick(jnp.sum(rst[:, 1, :] * facs, axis=0, keepdims=True), here)
    acc = jnp.zeros((HALF, HEAD_DIM), F32)
    for c in range(CHIPS):
        acc += rbuf[c] * pick(facs[c:c + 1], here)
    q_own = jnp.concatenate([gbuf[2 * core, chip], gbuf[2 * core + 1, chip]], axis=0)
    kv_own = gbuf[4 + core, chip]
    k_own = jnp.concatenate([jnp.broadcast_to(kv_own[i:i + 1], (4, HEAD_DIM)) for i in range(4)], axis=0)
    v_own = jnp.concatenate([jnp.broadcast_to(kv_own[4 + i:5 + i], (4, HEAD_DIM)) for i in range(4)], axis=0)
    s_own = jnp.sum(q_own * k_own, axis=-1, keepdims=True) * SCALE
    top = pick(top, here)
    peak = jnp.maximum(top, s_own)
    f_old, f_new = jnp.exp(top - peak), jnp.exp(s_own - peak)
    attn = (acc * f_old + v_own * f_new) / (total * f_old + f_new)
    for h in range(HALF):
        lhs[:, h * 128:(h + 1) * 128] = jnp.where(row16 == h, attn, 0.0).astype(BF16)

    wocopy.wait()

    def out_cols(half, slot):
        for n in range(5):
            cols = pl.ds(pl.multiple_of(half * 1280 + n * 256, 256), 256)
            res = jnp.dot(lhs[...], wobuf[:, cols], preferred_element_type=F32)
            res = jnp.sum(res, axis=0, keepdims=True)
            for k in range(2):
                ypart[slot, pl.ds(2 * n + k, 1), :] = res[:, k * 128:(k + 1) * 128]

    out_cols(1 - core, 0)
    ycopy = pltpu.make_async_remote_copy(src_ref=ypart.at[0], dst_ref=yin, send_sem=ysem.at[0], recv_sem=ysem.at[1],
                                         device_id=dev(mate), device_id_type=MESH)
    ycopy.start()
    out_cols(core, 1)
    ycopy.wait()
    ysend[...] = ypart[1] + yin[...]

    def bcopy(s, group):
        return pltpu.make_async_remote_copy(src_ref=ysend, dst_ref=ybuf.at[core, chip], send_sem=bsend.at[0],
                                            recv_sem=brecv.at[group], device_id=dev(s * 2 + core), device_id_type=MESH)

    @pl.loop(1, CHIPS)
    def _(k):
        s = lax.rem(chip + 1 + lax.rem(k + 30, CHIPS - 1), CHIPS)
        bcopy(s, lax.rem(zed - s // 16 + 4, 4)).start()

    ybuf[core, chip] = ysend[...]

    def slab(half, group):
        return ybuf.at[half, pl.ds(lax.rem(zed + group, 4) * 16, 16)]

    def fcopy(half, group):
        ref = slab(half, group)
        return pltpu.make_async_remote_copy(src_ref=ref, dst_ref=ref, send_sem=fsend.at[group], recv_sem=frecv.at[group],
                                            device_id=dev(mate), device_id_type=MESH)

    for group in (0, 1, 3, 2):
        ref = ybuf.at[core, pl.ds(0, 15 if group == 0 else 16)]
        all_of(ref, ref, bsend.at[0], brecv.at[group]).wait_recv()
        fcopy(core, group).start()
    for group in (0, 1, 3, 2):
        fcopy(1 - core, group).wait_recv()

    for half in range(2):
        for k in range(10):
            cols = slice(half * 1280 + k * 128, half * 1280 + (k + 1) * 128)
            out_ref[:, cols] = (tok_ref[:, cols].astype(F32) + ybuf[half, :, k, :]).astype(BF16)

    outcopy = pltpu.make_async_copy(out_ref, out_hbm, outsem.at[0])
    outcopy.start()
    for group in range(4):
        fcopy(core, group).wait_send()
    all_of(rst.at[others], rst.at[others], tsend.at[0], trecv.at[0]).wait_send()
    all_of(rbuf.at[others], rbuf.at[others], ssend.at[0], srecv.at[0]).wait_send()
    rest = ybuf.at[0, others]
    all_of(rest, rest, bsend.at[0], brecv.at[0]).wait_send()
    kvout.wait()
    outcopy.wait()


def step_call(*args):
    dma = pltpu.SemaphoreType.DMA
    vmem = pltpu.VMEM
    hbm = pl.BlockSpec(memory_space=pl.ANY)
    vm = pl.BlockSpec(memory_space=pltpu.VMEM)
    return pl.pallas_call(
        step_kernel,
        name="decode_step",
        out_shape=(jax.ShapeDtypeStruct((SEQS, DIM), BF16), jax.ShapeDtypeStruct((2, SEQS, 8, HEAD_DIM), F32),
                   jax.ShapeDtypeStruct((SEQS, 128, HEAD_DIM), BF16), jax.ShapeDtypeStruct((SEQS, 128, HEAD_DIM), BF16)),
        in_specs=[pl.BlockSpec(memory_space=pltpu.SMEM)] + [pl.BlockSpec(memory_space=pltpu.HBM)] * 11,
        out_specs=(hbm, hbm, vm, vm),
        scratch_shapes=[
            vmem((SEQS, DIM), BF16), vmem((DIM,), BF16), vmem((1, HEAD_DIM), BF16), vmem((1, HEAD_DIM), BF16), vmem((1, HEAD_DIM), F32),
            dma((5,)), dma((1,)),
            vmem((SEQS, DIM), BF16), vmem((SEQS, HEAD_DIM), F32), vmem((SEQS, HEAD_DIM), F32),
            vmem((12, DIM, 256), BF16), vmem((2048, DIM), BF16),
            vmem((6, SEQS, 8, HEAD_DIM), F32),
            vmem((SEQS, HEADS, HEAD_DIM), BF16), vmem((2, SEQS, HALF, HEAD_DIM), F32), vmem((SEQS, HALF, HEAD_DIM), F32),
            vmem((2, 8, 2, HEAD_DIM), F32), vmem((8, 2, HEAD_DIM), F32), vmem((2, 8, HEAD_DIM), F32),
            vmem((SEQS, HALF, HEAD_DIM), F32), vmem((8, 2, HEAD_DIM), F32),
            vmem((CHIPS, HALF, HEAD_DIM), F32), vmem((CHIPS, 2, HEAD_DIM), F32), vmem((SEQS, DIM), BF16),
            vmem((HALF, 2048), BF16), vmem((2, 10, HEAD_DIM), F32), vmem((10, HEAD_DIM), F32), vmem((10, HEAD_DIM), F32),
            vmem((2, CHIPS, 10, HEAD_DIM), F32),
            dma((12,)), dma((1,)), dma((2, 4)), dma((1,)), dma((3,)), dma((3,)), dma((8,)), dma((8,)), dma((1,)), dma((1,)),
            dma((1,)), dma((1,)), dma((1,)), dma((1,)), dma((2,)), dma((1,)), dma((4,)), dma((4,)), dma((4,)),
        ],
        compiler_params=pltpu.CompilerParams(collective_id=0, has_side_effects=True, vmem_limit_bytes=48 * 2 ** 20),
    )(*args)


CHUNKS = 8


def cache_kernel(pos_ref, kv_hbm, row_hbm, kbuf, vbuf, ko_hbm, vo_hbm, new_hbm, out_hbm,
                 kv, new, row, osem, ssem):
    start = lax.axis_index("sp") * SLOTS
    per = SEQS // CHUNKS

    def copies(i):
        rows = pl.ds(i * per, per)
        return (pltpu.make_async_copy(kbuf.at[rows], ko_hbm.at[rows], osem.at[0, i]),
                pltpu.make_async_copy(vbuf.at[rows], vo_hbm.at[rows], osem.at[1, i]))

    kvload, rowload = pltpu.make_async_copy(kv_hbm, kv, ssem.at[0]), pltpu.make_async_copy(row_hbm, row, ssem.at[1])
    kvload.start()
    rowload.start()
    kvload.wait()
    low = iota((SEQS, 8, HEAD_DIM), 1) < 4
    first, second = kv[0], kv[1]
    new[:, 0] = jnp.where(low, first, pltpu.roll(second, 4, 1)).astype(BF16)
    new[:, 1] = jnp.where(low, pltpu.roll(first, 4, 1), second).astype(BF16)
    small = [pltpu.make_async_copy(new, new_hbm, ssem.at[2]), pltpu.make_async_copy(row, out_hbm, ssem.at[3])]
    small[0].start()
    rowload.wait()
    small[1].start()
    for i in range(CHUNKS):
        @pl.loop(i * per, (i + 1) * per)
        def _(s):
            slot = pos_ref[s] - start

            @pl.when((slot >= 0) & (slot < SLOTS))
            def _():
                kbuf[s, slot] = new[s, 0]
                vbuf[s, slot] = new[s, 1]

        for c in copies(i):
            c.start()
    for c in small:
        c.wait()
    for i in range(CHUNKS):
        for c in copies(i):
            c.wait()


def cache_call(*args):
    hbm = pl.BlockSpec(memory_space=pl.ANY)
    shape = (SEQS, SLOTS, KV_HEADS, HEAD_DIM)
    new = (SEQS, 2, KV_HEADS, HEAD_DIM)
    dma = pltpu.SemaphoreType.DMA
    return pl.pallas_call(
        cache_kernel,
        name="cache_write",
        out_shape=(jax.ShapeDtypeStruct(shape, BF16), jax.ShapeDtypeStruct(shape, BF16), jax.ShapeDtypeStruct(new, BF16),
                   jax.ShapeDtypeStruct((SEQS, DIM), BF16)),
        in_specs=[pl.BlockSpec(memory_space=pltpu.SMEM)] + [hbm] * 2 + [pl.BlockSpec(memory_space=pltpu.VMEM)] * 2,
        compiler_params=pltpu.CompilerParams(vmem_limit_bytes=12 * 2 ** 20),
        out_specs=(hbm,) * 4,
        scratch_shapes=[pltpu.VMEM((2, SEQS, 8, HEAD_DIM), F32), pltpu.VMEM(new, BF16), pltpu.VMEM((SEQS, DIM), BF16),
                        dma((2, CHUNKS)), dma((4,))],
    )(*args)


def solution(mesh):
    cache_spec = P('dp', 'sp', None, None)

    def device_step(tokens, positions, k_cache, v_cache, w_q, w_k, w_v, w_o, attn_norm, q_norm, k_norm):
        inv = np.float32(ROPE_THETA) ** (-np.arange(HEAD_DIM // 2, dtype=np.float32) * np.float32(2.0) / np.float32(HEAD_DIM))
        freq = jnp.asarray(np.concatenate([inv, inv])[None, :].astype(np.float32))
        flat = (SEQS, SLOTS * KV_HEADS, HEAD_DIM)
        row, kv, k_loc, v_loc = step_call(positions, tokens, attn_norm, q_norm[None, :], k_norm[None, :], freq, w_q, w_k, w_v,
                                  w_o, k_cache.reshape(flat), v_cache.reshape(flat))
        k_out, v_out, new_kv, block_out = cache_call(positions, kv, row, k_loc.reshape(k_cache.shape), v_loc.reshape(v_cache.shape))
        return block_out, k_out, v_out, new_kv

    return jax.shard_map(device_step, mesh=mesh, in_specs=(P('dp', None), P('dp'), cache_spec, cache_spec, P(), P(), P(), P(), P(), P(), P()), out_specs=(P('dp', None), cache_spec, cache_spec, P('dp', None, None, None)), check_vma=False)
```

```python
import functools

import jax
import jax.numpy as jnp
import numpy as np
from jax import lax
from jax.experimental import pallas as pl
from jax.experimental.pallas import tpu as pltpu
from jax.sharding import PartitionSpec as P

NORM_EPS = 1e-6
ROPE_THETA = 1000000.0
NEG_FILL = -1e30
SEQS, DIM, HEADS, KV_HEADS, HEAD_DIM, SLOTS = 64, 2560, 32, 8, 128, 16
HALF = HEADS // 2
CHIPS = 64
SCALE = HEAD_DIM ** -0.5
F32, BF16 = jnp.float32, jnp.bfloat16
MESH = pl.DeviceIdType.MESH
DEPTH = 3
LAG = 5


def rms(values, gain):
    return values * lax.rsqrt(jnp.mean(values * values, axis=-1, keepdims=True) + NORM_EPS) * gain


def iota(shape, axis):
    return lax.broadcasted_iota(jnp.int32, shape, axis)


def pick(row, lane):
    spread = jnp.broadcast_to(row, (HALF, HEAD_DIM))
    return jnp.sum(jnp.where(lane, spread, 0.0), axis=-1, keepdims=True)


def step_kernel(pos_hbm, tok_hbm, an_hbm, qn_hbm, kn_hbm, freq_hbm, wq_hbm, wk_hbm, wv_hbm, wo_hbm, kc_hbm, vc_hbm,
                out_ref, new_ref, kbuf, vbuf,
                pos_ref, tok_ref, an_ref, qn_ref, kn_ref, freq_ref, isem, facbuf, hid, cosr, sinr, wbuf, wobuf, gbuf, wts, obuf, oin, st, stin, fac, osend, stsend, rbuf, rst,
                lhs, ypart, yin, ysend, ybuf,
                wsem, wosem, csem, gsend, grecv, dsend, drecv, dssend, dsrecv,
                ssend, srecv, tsend, trecv, ysem, bsend, brecv, fsend, frecv):
    me = lax.axis_index("sp")
    chip, core = me // 2, me % 2
    zed = chip // 16
    mate = chip * 2 + (1 - core)
    start = me * SLOTS

    def dev(index):
        return (lax.axis_index("dp"), index)

    def wcopy(src, col, tile):
        return pltpu.make_async_copy(src.at[:, pl.ds(pl.multiple_of(col, 256), 256)], wbuf.at[tile], wsem.at[tile])

    def tile_copy(t):
        if t < 2:
            return wcopy(wk_hbm, core * 512 + t * 256, t)
        if t < 4:
            return wcopy(wv_hbm, core * 512 + (t - 2) * 256, t)
        return wcopy(wq_hbm, core * 2048 + (t - 4) * 256, t)

    def kvload(i):
        rows = pl.ds(i * 16, 16)
        return (pltpu.make_async_copy(kc_hbm.at[rows], kbuf.at[rows], csem.at[0, i]),
                pltpu.make_async_copy(vc_hbm.at[rows], vbuf.at[rows], csem.at[1, i]))

    def tile_ready(t):
        tile_copy(t).wait()
        if t + DEPTH < 12:
            tile_copy(t + DEPTH).start()
        elif t + DEPTH < 14:
            for c in kvload(2 * (t + DEPTH - 12)) + kvload(2 * (t + DEPTH - 12) + 1):
                c.start()

    inputs = [pltpu.make_async_copy(a, b, isem.at[i]) for i, (a, b) in enumerate(
        [(tok_hbm, tok_ref), (an_hbm, an_ref), (pos_hbm, pos_ref), (freq_hbm, freq_ref), (kn_hbm, kn_ref), (qn_hbm, qn_ref)])]
    for c in inputs:
        c.start()
    for t in range(DEPTH):
        tile_copy(t).start()
    barrier = pltpu.get_barrier_semaphore()
    pl.semaphore_signal(barrier, inc=1, device_id=dev(mate), device_id_type=MESH)

    @pl.loop(1, CHIPS)
    def _(off):
        pl.semaphore_signal(barrier, inc=1, device_id=dev(lax.rem(chip + off, CHIPS) * 2 + core), device_id_type=MESH)

    for c in inputs:
        c.wait()

    tok = tok_ref[...].astype(F32)
    hid[...] = rms(tok, an_ref[...].astype(F32).reshape(1, DIM)).astype(BF16)
    row8 = iota((SEQS, HEAD_DIM), 0)
    posv = jnp.zeros((SEQS, HEAD_DIM), jnp.int32)
    for s in range(SEQS):
        posv = jnp.where(row8 == s, pos_ref[s], posv)
    angle = posv.astype(F32) * freq_ref[...]
    cosr[...] = jnp.cos(angle)
    sinr[...] = jnp.where(iota((SEQS, HEAD_DIM), 1) < HEAD_DIM // 2, -1.0, 1.0) * jnp.sin(angle)

    def project(tile):
        return jnp.dot(hid[...], wbuf[tile], preferred_element_type=F32).astype(BF16).astype(F32)

    def rope(head, gain):
        normed = rms(head, gain)
        turned = normed * cosr[...] + pltpu.roll(normed, HEAD_DIM // 2, 1) * sinr[...]
        return turned.astype(BF16).astype(F32)

    for t in range(4):
        tile_ready(t)
        res = project(t)
        for h in range(2):
            head = res[:, h * 128:(h + 1) * 128]
            gbuf[4 + core, :, 2 * t + h, :] = rope(head, kn_ref[...].astype(F32)) if t < 2 else head

    def gcopy(group, slot):
        return pltpu.make_async_remote_copy(src_ref=gbuf.at[group], dst_ref=gbuf.at[group], send_sem=gsend.at[slot],
                                            recv_sem=grecv.at[slot], device_id=dev(mate), device_id_type=MESH)

    for g in range(2):
        for t4 in range(4):
            t = 4 + g * 4 + t4
            tile_ready(t)
            res = project(t)
            for h in range(2):
                gbuf[2 * core + g, :, 2 * t4 + h, :] = rope(res[:, h * 128:(h + 1) * 128], qn_ref[...].astype(F32))
        if g == 0:
            pl.semaphore_wait(barrier, CHIPS)
            gcopy(4 + core, 2).start()
        gcopy(2 * core + g, g).start()

    wocopy = pltpu.make_async_copy(wo_hbm.at[pl.ds(pl.multiple_of(core * 2048, 2048), 2048)], wobuf, wosem.at[0])
    wocopy.start()
    for slot in range(3):
        gcopy(4 + core if slot == 2 else 2 * core + slot, slot).wait()
    for i in range(4):
        for c in kvload(i):
            c.wait()

    def block_of(i):
        return lax.rem(zed + 2 + i // 2 - (i // 4) * (2 * (i // 2) - 1), 4) * 2 + lax.rem(i, 2)

    row32, col32 = iota((HEADS, HEAD_DIM), 0), iota((HEADS, HEAD_DIM), 1)
    same_head = (col32 % KV_HEADS) == (row32 // 4)
    slot_of = col32 // KV_HEADS + start
    row16, lane16 = iota((HALF, HEAD_DIM), 0), iota((HALF, HEAD_DIM), 1)

    def weigh(blk):
        acc = [[jnp.zeros((HALF, HEAD_DIM), F32) for _ in range(2)] for _ in range(2)]
        for s8 in range(8):
            s = blk * 8 + s8
            q = jnp.concatenate([gbuf[g, s] for g in range(4)], axis=0).astype(BF16)
            scores = lax.dot_general(q, kbuf[s], (((1,), (1,)), ((), ())), preferred_element_type=F32) * SCALE
            live = same_head & (slot_of < pos_ref[s])
            scores = jnp.where(live, scores, NEG_FILL)
            peak = jnp.max(scores, axis=-1, keepdims=True)
            weights = jnp.where(live, jnp.exp(scores - peak), 0.0)
            total = jnp.sum(weights, axis=-1, keepdims=True)
            wts[s] = weights.astype(BF16)
            here = lane16 == s8 * HALF + row16
            for half in range(2):
                cut = slice(half * HALF, (half + 1) * HALF)
                acc[half][0] += jnp.where(here, peak[cut], 0.0)
                acc[half][1] += jnp.where(here, total[cut], 0.0)
        for half in range(2):
            for k in range(2):
                st[half, blk, pl.ds(k, 1), :] = jnp.sum(acc[half][k], axis=0, keepdims=True)

    def mix(i):
        blk = block_of(i)
        for s8 in range(8):
            s = blk * 8 + s8
            mixed = jnp.dot(wts[s], vbuf[s], preferred_element_type=F32)
            for half in range(2):
                obuf[half, s] = mixed[half * HALF:(half + 1) * HALF]
        ocopy(i).start()

    def ocopy(i):
        rows = pl.ds(block_of(i) * 8, 8)
        return pltpu.make_async_remote_copy(src_ref=obuf.at[1 - core, rows], dst_ref=oin.at[rows], send_sem=dsend.at[i],
                                            recv_sem=drecv.at[i], device_id=dev(mate), device_id_type=MESH)

    def merge(i):
        blk = block_of(i)
        ocopy(i).wait()
        f0, f1 = fac[0, pl.ds(blk, 1), :], fac[1, pl.ds(blk, 1), :]
        for s8 in range(8):
            s = blk * 8 + s8
            here = lane16 == s8 * HALF + row16
            osend[s] = obuf[core, s] * pick(f0, here) + oin[s] * pick(f1, here)
        for s8 in range(8):
            s = blk * 8 + s8

            @pl.when(s != chip)
            def _():
                pltpu.make_async_remote_copy(src_ref=osend.at[s], dst_ref=rbuf.at[chip], send_sem=ssend.at[0], recv_sem=srecv.at[lax.rem(zed - s // 16 + 4, 4)],
                                             device_id=dev(s * 2 + core), device_id_type=MESH).start()

    @pl.loop(0, 8)
    def _(blk):
        weigh(blk)

    stcopy = pltpu.make_async_remote_copy(src_ref=st.at[1 - core], dst_ref=stin, send_sem=dssend.at[0], recv_sem=dsrecv.at[0],
                                          device_id=dev(mate), device_id_type=MESH)
    stcopy.start()

    @pl.loop(0, LAG)
    def _(i):
        mix(i)

    stcopy.wait()
    m0, l0, m1, l1 = st[core, :, 0, :], st[core, :, 1, :], stin[:, 0, :], stin[:, 1, :]
    top = jnp.maximum(m0, m1)
    f0, f1 = jnp.exp(m0 - top), jnp.exp(m1 - top)
    fac[0], fac[1] = f0, f1
    stsend[:, 0, :] = top
    stsend[:, 1, :] = l0 * f0 + l1 * f1

    @pl.loop(1, CHIPS)
    def _(off):
        s = lax.rem(chip + off, CHIPS)
        pltpu.make_async_remote_copy(src_ref=stsend.at[s // 8], dst_ref=rst.at[chip], send_sem=tsend.at[0], recv_sem=trecv.at[0],
                                     device_id=dev(s * 2 + core), device_id_type=MESH).start()

    @pl.loop(LAG, 8 + LAG)
    def _(i):
        @pl.when(i < 8)
        def _():
            mix(i)

        merge(i - LAG)

    rst[chip] = stsend[chip // 8]
    rbuf[chip] = osend[chip]

    def all_of(src, dst, send, recv):
        return pltpu.make_async_remote_copy(src_ref=src, dst_ref=dst, send_sem=send, recv_sem=recv, device_id=dev(mate),
                                            device_id_type=MESH)

    low = iota((SEQS, 8, HEAD_DIM), 1) < 4
    new_ref[:, 0] = jnp.where(low, gbuf[4], pltpu.roll(gbuf[5], 4, 1)).astype(BF16)
    new_ref[:, 1] = jnp.where(low, pltpu.roll(gbuf[4], 4, 1), gbuf[5]).astype(BF16)

    others = pl.ds(0, CHIPS - 1)
    all_of(rst.at[others], rst.at[others], tsend.at[0], trecv.at[0]).wait_recv()
    here = lane16 == lax.rem(chip, 8) * HALF + row16
    tops = rst[:, 0, :]
    top = jnp.max(tops, axis=0, keepdims=True)
    facs = jnp.exp(tops - top)
    facbuf[...] = facs
    total = pick(jnp.sum(rst[:, 1, :] * facs, axis=0, keepdims=True), here)
    q_own = jnp.concatenate([gbuf[2 * core, chip], gbuf[2 * core + 1, chip]], axis=0)
    kv_own = gbuf[4 + core, chip]
    k_own = jnp.concatenate([jnp.broadcast_to(kv_own[i:i + 1], (4, HEAD_DIM)) for i in range(4)], axis=0)
    v_own = jnp.concatenate([jnp.broadcast_to(kv_own[4 + i:5 + i], (4, HEAD_DIM)) for i in range(4)], axis=0)
    s_own = jnp.sum(q_own * k_own, axis=-1, keepdims=True) * SCALE
    top = pick(top, here)
    peak = jnp.maximum(top, s_own)
    f_old, f_new = jnp.exp(top - peak), jnp.exp(s_own - peak)
    acc = jnp.zeros((HALF, HEAD_DIM), F32)
    for group in (0, 1, 3, 2):
        part = rbuf.at[pl.ds(0, 15 if group == 0 else 16)]
        all_of(part, part, ssend.at[0], srecv.at[group]).wait_recv()
        base = lax.rem(zed + group, 4) * 16
        for c in range(16):
            acc += rbuf[base + c] * pick(facbuf[pl.ds(base + c, 1), :], here)
    attn = (acc * f_old + v_own * f_new) / (total * f_old + f_new)
    for h in range(HALF):
        lhs[:, h * 128:(h + 1) * 128] = jnp.where(row16 == h, attn, 0.0).astype(BF16)

    wocopy.wait()

    def out_cols(half, slot):
        for n in range(5):
            cols = pl.ds(pl.multiple_of(half * 1280 + n * 256, 256), 256)
            res = jnp.dot(lhs[...], wobuf[:, cols], preferred_element_type=F32)
            res = jnp.sum(res, axis=0, keepdims=True)
            for k in range(2):
                ypart[slot, pl.ds(2 * n + k, 1), :] = res[:, k * 128:(k + 1) * 128]

    out_cols(1 - core, 0)
    ycopy = pltpu.make_async_remote_copy(src_ref=ypart.at[0], dst_ref=yin, send_sem=ysem.at[0], recv_sem=ysem.at[1],
                                         device_id=dev(mate), device_id_type=MESH)
    ycopy.start()
    out_cols(core, 1)
    ycopy.wait()
    ysend[...] = ypart[1] + yin[...]

    def bcopy(s, group):
        return pltpu.make_async_remote_copy(src_ref=ysend, dst_ref=ybuf.at[core, chip], send_sem=bsend.at[0],
                                            recv_sem=brecv.at[group], device_id=dev(s * 2 + core), device_id_type=MESH)

    @pl.loop(1, CHIPS)
    def _(k):
        s = lax.rem(chip + 1 + lax.rem(k + 30, CHIPS - 1), CHIPS)
        bcopy(s, lax.rem(zed - s // 16 + 4, 4)).start()

    ybuf[core, chip] = ysend[...]

    def slab(half, group):
        return ybuf.at[half, pl.ds(lax.rem(zed + group, 4) * 16, 16)]

    def fcopy(half, group):
        ref = slab(half, group)
        return pltpu.make_async_remote_copy(src_ref=ref, dst_ref=ref, send_sem=fsend.at[group], recv_sem=frecv.at[group],
                                            device_id=dev(mate), device_id_type=MESH)

    for group in (0, 1, 3, 2):
        ref = ybuf.at[core, pl.ds(0, 15 if group == 0 else 16)]
        all_of(ref, ref, bsend.at[0], brecv.at[group]).wait_recv()
        fcopy(core, group).start()
    for group in (0, 1, 3, 2):
        fcopy(1 - core, group).wait_recv()

    for half in range(2):
        for k in range(10):
            cols = slice(half * 1280 + k * 128, half * 1280 + (k + 1) * 128)
            out_ref[:, cols] = (tok_ref[:, cols].astype(F32) + ybuf[half, :, k, :]).astype(BF16)

    for group in range(4):
        fcopy(core, group).wait_send()
    all_of(rst.at[others], rst.at[others], tsend.at[0], trecv.at[0]).wait_send()
    all_of(rbuf.at[others], rbuf.at[others], ssend.at[0], srecv.at[0]).wait_send()
    rest = ybuf.at[0, others]
    all_of(rest, rest, bsend.at[0], brecv.at[0]).wait_send()


def step_call(*args):
    dma = pltpu.SemaphoreType.DMA
    vmem = pltpu.VMEM
    vm = pl.BlockSpec(memory_space=pltpu.VMEM)
    return pl.pallas_call(
        step_kernel,
        name="decode_step",
        out_shape=(jax.ShapeDtypeStruct((SEQS, DIM), BF16), jax.ShapeDtypeStruct((SEQS, 2, KV_HEADS, HEAD_DIM), BF16),
                   jax.ShapeDtypeStruct((SEQS, 128, HEAD_DIM), BF16), jax.ShapeDtypeStruct((SEQS, 128, HEAD_DIM), BF16)),
        in_specs=[pl.BlockSpec(memory_space=pltpu.HBM)] * 12,
        out_specs=(vm,) * 4,
        scratch_shapes=[
            pltpu.SMEM((SEQS,), jnp.int32), vmem((SEQS, DIM), BF16), vmem((DIM,), BF16), vmem((1, HEAD_DIM), BF16), vmem((1, HEAD_DIM), BF16), vmem((1, HEAD_DIM), F32),
            dma((6,)), vmem((CHIPS, HEAD_DIM), F32),
            vmem((SEQS, DIM), BF16), vmem((SEQS, HEAD_DIM), F32), vmem((SEQS, HEAD_DIM), F32),
            vmem((12, DIM, 256), BF16), vmem((2048, DIM), BF16),
            vmem((6, SEQS, 8, HEAD_DIM), F32),
            vmem((SEQS, HEADS, HEAD_DIM), BF16), vmem((2, SEQS, HALF, HEAD_DIM), F32), vmem((SEQS, HALF, HEAD_DIM), F32),
            vmem((2, 8, 2, HEAD_DIM), F32), vmem((8, 2, HEAD_DIM), F32), vmem((2, 8, HEAD_DIM), F32),
            vmem((SEQS, HALF, HEAD_DIM), F32), vmem((8, 2, HEAD_DIM), F32),
            vmem((CHIPS, HALF, HEAD_DIM), F32), vmem((CHIPS, 2, HEAD_DIM), F32),
            vmem((HALF, 2048), BF16), vmem((2, 10, HEAD_DIM), F32), vmem((10, HEAD_DIM), F32), vmem((10, HEAD_DIM), F32),
            vmem((2, CHIPS, 10, HEAD_DIM), F32),
            dma((12,)), dma((1,)), dma((2, 4)), dma((3,)), dma((3,)), dma((8,)), dma((8,)), dma((1,)), dma((1,)),
            dma((1,)), dma((4,)), dma((1,)), dma((1,)), dma((2,)), dma((1,)), dma((4,)), dma((4,)), dma((4,)),
        ],
        compiler_params=pltpu.CompilerParams(collective_id=0, has_side_effects=True, vmem_limit_bytes=48 * 2 ** 20),
    )(*args)


CHUNKS = 8


def cache_kernel(pos_ref, new, row, kbuf, vbuf, ko_hbm, vo_hbm, new_hbm, out_hbm, osem, ssem):
    start = lax.axis_index("sp") * SLOTS
    per = SEQS // CHUNKS
    copies = [pltpu.make_async_copy(new, new_hbm, ssem.at[0]), pltpu.make_async_copy(row, out_hbm, ssem.at[1])]
    for c in copies:
        c.start()
    for i in range(CHUNKS):
        @pl.loop(i * per, (i + 1) * per)
        def _(s):
            slot = pos_ref[s] - start

            @pl.when((slot >= 0) & (slot < SLOTS))
            def _():
                kbuf[s, slot] = new[s, 0]
                vbuf[s, slot] = new[s, 1]

        rows = pl.ds(i * per, per)
        both = [pltpu.make_async_copy(kbuf.at[rows], ko_hbm.at[rows], osem.at[0, i]),
                pltpu.make_async_copy(vbuf.at[rows], vo_hbm.at[rows], osem.at[1, i])]
        for c in both:
            c.start()
        copies += both
    for c in copies:
        c.wait()


def cache_call(positions, new, row, k_loc, v_loc):
    hbm = pl.BlockSpec(memory_space=pl.ANY)
    vm = pl.BlockSpec(memory_space=pltpu.VMEM)
    dma = pltpu.SemaphoreType.DMA
    return pl.pallas_call(
        cache_kernel,
        name="cache_write",
        out_shape=tuple(jax.ShapeDtypeStruct(a.shape, a.dtype) for a in (k_loc, v_loc, new, row)),
        in_specs=[pl.BlockSpec(memory_space=pltpu.SMEM)] + [vm] * 4,
        out_specs=(hbm,) * 4,
        scratch_shapes=[dma((2, CHUNKS)), dma((2,))],
        compiler_params=pltpu.CompilerParams(vmem_limit_bytes=12 * 2 ** 20),
    )(positions, new, row, k_loc, v_loc)


def solution(mesh):
    cache_spec = P('dp', 'sp', None, None)

    def device_step(tokens, positions, k_cache, v_cache, w_q, w_k, w_v, w_o, attn_norm, q_norm, k_norm):
        inv = np.float32(ROPE_THETA) ** (-np.arange(HEAD_DIM // 2, dtype=np.float32) * np.float32(2.0) / np.float32(HEAD_DIM))
        freq = jnp.asarray(np.concatenate([inv, inv])[None, :].astype(np.float32))
        flat = (SEQS, SLOTS * KV_HEADS, HEAD_DIM)
        operands = (positions, tokens, attn_norm, q_norm[None, :], k_norm[None, :], freq, w_q, w_k, w_v, w_o, k_cache.reshape(flat), v_cache.reshape(flat))
        row, new, k_loc, v_loc = step_call(*[pltpu.with_memory_space_constraint(a, pltpu.HBM) for a in operands])
        k_out, v_out, new_kv, block_out = cache_call(positions, new, row, k_loc.reshape(k_cache.shape), v_loc.reshape(v_cache.shape))
        return block_out, k_out, v_out, new_kv

    return jax.shard_map(device_step, mesh=mesh, in_specs=(P('dp', None), P('dp'), cache_spec, cache_spec, P(), P(), P(), P(), P(), P(), P()), out_specs=(P('dp', None), cache_spec, cache_spec, P('dp', None, None, None)), check_vma=False)
```

```python
import functools

import jax
import jax.numpy as jnp
import numpy as np
from jax import lax
from jax.experimental import pallas as pl
from jax.experimental.pallas import tpu as pltpu
from jax.sharding import PartitionSpec as P

NORM_EPS = 1e-6
ROPE_THETA = 1000000.0
NEG_FILL = -1e30
SEQS, DIM, HEADS, KV_HEADS, HEAD_DIM, SLOTS = 64, 2560, 32, 8, 128, 16
HALF = HEADS // 2
CHIPS = 64
SCALE = HEAD_DIM ** -0.5
F32, BF16 = jnp.float32, jnp.bfloat16
MESH = pl.DeviceIdType.MESH
DEPTH = 3
FAR_FIRST = sorted(range(16), key=lambda k: -(min(k // 4, 4 - k // 4) + min(k % 4, 4 - k % 4)))
LAG = 5


def rms(values, gain):
    return values * lax.rsqrt(jnp.mean(values * values, axis=-1, keepdims=True) + NORM_EPS) * gain


def iota(shape, axis):
    return lax.broadcasted_iota(jnp.int32, shape, axis)


def pick(row, lane):
    spread = jnp.broadcast_to(row, (HALF, HEAD_DIM))
    return jnp.sum(jnp.where(lane, spread, 0.0), axis=-1, keepdims=True)


def step_kernel(pos_hbm, tok_hbm, an_hbm, qn_hbm, kn_hbm, freq_hbm, wq_hbm, wk_hbm, wv_hbm, wo_hbm, kc_hbm, vc_hbm,
                out_ref, new_ref, kbuf, vbuf,
                pos_ref, tok_ref, an_ref, qn_ref, kn_ref, freq_ref, isem, facbuf, hid, cosr, sinr, wbuf, wobuf, gbuf, wts, obuf, oin, st, stin, fac, osend, stsend, rbuf, rst,
                lhs, ypart, yin, ysend, ybuf,
                wsem, wosem, csem, gsend, grecv, dsend, drecv, dssend, dsrecv,
                ssend, srecv, tsend, trecv, ysem, bsend, brecv, fsend, frecv):
    me = lax.axis_index("sp")
    chip, core = me // 2, me % 2
    zed, low = lax.div(chip, 16), lax.rem(chip, 16)
    mate = chip * 2 + (1 - core)
    start = me * SLOTS

    def dev(index):
        return (lax.axis_index("dp"), index)

    def wcopy(src, col, tile):
        return pltpu.make_async_copy(src.at[:, pl.ds(pl.multiple_of(col, 256), 256)], wbuf.at[tile], wsem.at[tile])

    def tile_copy(t):
        if t < 2:
            return wcopy(wk_hbm, core * 512 + t * 256, t)
        if t < 4:
            return wcopy(wv_hbm, core * 512 + (t - 2) * 256, t)
        return wcopy(wq_hbm, core * 2048 + (t - 4) * 256, t)

    def kvload(i):
        rows = pl.ds(i * 16, 16)
        return (pltpu.make_async_copy(kc_hbm.at[rows], kbuf.at[rows], csem.at[0, i]),
                pltpu.make_async_copy(vc_hbm.at[rows], vbuf.at[rows], csem.at[1, i]))

    def tile_ready(t):
        tile_copy(t).wait()
        if t + DEPTH < 12:
            tile_copy(t + DEPTH).start()
        elif t + DEPTH < 14:
            for c in kvload(2 * (t + DEPTH - 12)) + kvload(2 * (t + DEPTH - 12) + 1):
                c.start()

    inputs = [pltpu.make_async_copy(a, b, isem.at[i]) for i, (a, b) in enumerate(
        [(tok_hbm, tok_ref), (an_hbm, an_ref), (pos_hbm, pos_ref), (freq_hbm, freq_ref), (kn_hbm, kn_ref), (qn_hbm, qn_ref)])]
    for c in inputs:
        c.start()
    for t in range(DEPTH):
        tile_copy(t).start()
    def each_other(send):
        for dz in (2, 1, 3, 0):
            base = lax.rem(zed + dz, 4) * 16
            for k in FAR_FIRST:
                if dz or k:
                    send(base + lax.rem(low + k, 16), (4 - dz) % 4)

    barrier = pltpu.get_barrier_semaphore()
    pl.semaphore_signal(barrier, inc=1, device_id=dev(mate), device_id_type=MESH)

    @pl.loop(1, CHIPS)
    def _(off):
        pl.semaphore_signal(barrier, inc=1, device_id=dev(lax.rem(chip + off, CHIPS) * 2 + core), device_id_type=MESH)

    for c in inputs:
        c.wait()

    tok = tok_ref[...].astype(F32)
    hid[...] = rms(tok, an_ref[...].astype(F32).reshape(1, DIM)).astype(BF16)
    row8 = iota((SEQS, HEAD_DIM), 0)
    posv = jnp.zeros((SEQS, HEAD_DIM), jnp.int32)
    for s in range(SEQS):
        posv = jnp.where(row8 == s, pos_ref[s], posv)
    angle = posv.astype(F32) * freq_ref[...]
    cosr[...] = jnp.cos(angle)
    sinr[...] = jnp.where(iota((SEQS, HEAD_DIM), 1) < HEAD_DIM // 2, -1.0, 1.0) * jnp.sin(angle)

    def project(tile):
        return jnp.dot(hid[...], wbuf[tile], preferred_element_type=F32).astype(BF16).astype(F32)

    def rope(head, gain):
        normed = rms(head, gain)
        turned = normed * cosr[...] + pltpu.roll(normed, HEAD_DIM // 2, 1) * sinr[...]
        return turned.astype(BF16).astype(F32)

    for t in range(4):
        tile_ready(t)
        res = project(t)
        for h in range(2):
            head = res[:, h * 128:(h + 1) * 128]
            gbuf[4 + core, :, 2 * t + h, :] = rope(head, kn_ref[...].astype(F32)) if t < 2 else head

    def gcopy(group, slot):
        return pltpu.make_async_remote_copy(src_ref=gbuf.at[group], dst_ref=gbuf.at[group], send_sem=gsend.at[slot],
                                            recv_sem=grecv.at[slot], device_id=dev(mate), device_id_type=MESH)

    for g in range(2):
        for t4 in range(4):
            t = 4 + g * 4 + t4
            tile_ready(t)
            res = project(t)
            for h in range(2):
                gbuf[2 * core + g, :, 2 * t4 + h, :] = rope(res[:, h * 128:(h + 1) * 128], qn_ref[...].astype(F32))
        if g == 0:
            pl.semaphore_wait(barrier, CHIPS)
            gcopy(4 + core, 2).start()
        gcopy(2 * core + g, g).start()

    wocopy = pltpu.make_async_copy(wo_hbm.at[pl.ds(pl.multiple_of(core * 2048, 2048), 2048)], wobuf, wosem.at[0])
    wocopy.start()
    for slot in range(3):
        gcopy(4 + core if slot == 2 else 2 * core + slot, slot).wait()
    for i in range(4):
        for c in kvload(i):
            c.wait()

    def block_of(i):
        return lax.rem(zed + 2 + i // 2 - (i // 4) * (2 * (i // 2) - 1), 4) * 2 + lax.rem(i, 2)

    row32, col32 = iota((HEADS, HEAD_DIM), 0), iota((HEADS, HEAD_DIM), 1)
    same_head = (col32 % KV_HEADS) == (row32 // 4)
    slot_of = col32 // KV_HEADS + start
    row16, lane16 = iota((HALF, HEAD_DIM), 0), iota((HALF, HEAD_DIM), 1)

    def weigh(blk):
        acc = [[jnp.zeros((HALF, HEAD_DIM), F32) for _ in range(2)] for _ in range(2)]
        for s8 in range(8):
            s = blk * 8 + s8
            q = jnp.concatenate([gbuf[g, s] for g in range(4)], axis=0).astype(BF16)
            scores = lax.dot_general(q, kbuf[s], (((1,), (1,)), ((), ())), preferred_element_type=F32) * SCALE
            live = same_head & (slot_of < pos_ref[s])
            scores = jnp.where(live, scores, NEG_FILL)
            peak = jnp.max(scores, axis=-1, keepdims=True)
            weights = jnp.where(live, jnp.exp(scores - peak), 0.0)
            total = jnp.sum(weights, axis=-1, keepdims=True)
            wts[s] = weights.astype(BF16)
            here = lane16 == s8 * HALF + row16
            for half in range(2):
                cut = slice(half * HALF, (half + 1) * HALF)
                acc[half][0] += jnp.where(here, peak[cut], 0.0)
                acc[half][1] += jnp.where(here, total[cut], 0.0)
        for half in range(2):
            for k in range(2):
                st[half, blk, pl.ds(k, 1), :] = jnp.sum(acc[half][k], axis=0, keepdims=True)

    def mix(i):
        blk = block_of(i)
        for s8 in range(8):
            s = blk * 8 + s8
            mixed = jnp.dot(wts[s], vbuf[s], preferred_element_type=F32)
            for half in range(2):
                obuf[half, s] = mixed[half * HALF:(half + 1) * HALF]
        ocopy(i).start()

    def ocopy(i):
        rows = pl.ds(block_of(i) * 8, 8)
        return pltpu.make_async_remote_copy(src_ref=obuf.at[1 - core, rows], dst_ref=oin.at[rows], send_sem=dsend.at[i],
                                            recv_sem=drecv.at[i], device_id=dev(mate), device_id_type=MESH)

    def merge(i):
        blk = block_of(i)
        ocopy(i).wait()
        f0, f1 = fac[0, pl.ds(blk, 1), :], fac[1, pl.ds(blk, 1), :]
        for s8 in range(8):
            s = blk * 8 + s8
            here = lane16 == s8 * HALF + row16
            osend[s] = obuf[core, s] * pick(f0, here) + oin[s] * pick(f1, here)
        group = lax.rem(zed - lax.div(blk, 2) + 4, 4)
        for s8 in range(8):
            s = blk * 8 + s8

            @pl.when(s != chip)
            def _():
                pltpu.make_async_remote_copy(src_ref=osend.at[s], dst_ref=rbuf.at[chip], send_sem=ssend.at[0], recv_sem=srecv.at[group],
                                             device_id=dev(s * 2 + core), device_id_type=MESH).start()

    @pl.loop(0, 8)
    def _(blk):
        weigh(blk)

    stcopy = pltpu.make_async_remote_copy(src_ref=st.at[1 - core], dst_ref=stin, send_sem=dssend.at[0], recv_sem=dsrecv.at[0],
                                          device_id=dev(mate), device_id_type=MESH)
    stcopy.start()

    @pl.loop(0, LAG)
    def _(i):
        mix(i)

    stcopy.wait()
    m0, l0, m1, l1 = st[core, :, 0, :], st[core, :, 1, :], stin[:, 0, :], stin[:, 1, :]
    top = jnp.maximum(m0, m1)
    f0, f1 = jnp.exp(m0 - top), jnp.exp(m1 - top)
    fac[0], fac[1] = f0, f1
    stsend[:, 0, :] = top
    stsend[:, 1, :] = l0 * f0 + l1 * f1

    def send_stats(s, _):
        pltpu.make_async_remote_copy(src_ref=stsend.at[lax.div(s, 8)], dst_ref=rst.at[chip], send_sem=tsend.at[0], recv_sem=trecv.at[0],
                                     device_id=dev(s * 2 + core), device_id_type=MESH).start()

    each_other(send_stats)

    @pl.loop(LAG, 8 + LAG)
    def _(i):
        @pl.when(i < 8)
        def _():
            mix(i)

        merge(i - LAG)

    rst[chip] = stsend[chip // 8]
    rbuf[chip] = osend[chip]

    def all_of(src, dst, send, recv):
        return pltpu.make_async_remote_copy(src_ref=src, dst_ref=dst, send_sem=send, recv_sem=recv, device_id=dev(mate),
                                            device_id_type=MESH)

    upper = iota((SEQS, 8, HEAD_DIM), 1) < 4
    new_ref[:, 0] = jnp.where(upper, gbuf[4], pltpu.roll(gbuf[5], 4, 1)).astype(BF16)
    new_ref[:, 1] = jnp.where(upper, pltpu.roll(gbuf[4], 4, 1), gbuf[5]).astype(BF16)

    slot_row = iota((128, HEAD_DIM), 0) // KV_HEADS + start

    @pl.loop(0, 16)
    def _(i):
        for s4 in range(4):
            s = i * 4 + s4
            first, second = gbuf[4, s], gbuf[5, s]
            mine = slot_row == pos_ref[s]
            k_new = jnp.where(upper[0], first, pltpu.roll(second, 4, 0))
            v_new = jnp.where(upper[0], pltpu.roll(first, 4, 0), second)
            kbuf[s] = jnp.where(mine, jnp.concatenate([k_new] * SLOTS, axis=0).astype(BF16), kbuf[s])
            vbuf[s] = jnp.where(mine, jnp.concatenate([v_new] * SLOTS, axis=0).astype(BF16), vbuf[s])

    others = pl.ds(0, CHIPS - 1)
    all_of(rst.at[others], rst.at[others], tsend.at[0], trecv.at[0]).wait_recv()
    here = lane16 == lax.rem(chip, 8) * HALF + row16
    tops = rst[:, 0, :]
    top = jnp.max(tops, axis=0, keepdims=True)
    facs = jnp.exp(tops - top)
    facbuf[...] = facs
    total = pick(jnp.sum(rst[:, 1, :] * facs, axis=0, keepdims=True), here)
    q_own = jnp.concatenate([gbuf[2 * core, chip], gbuf[2 * core + 1, chip]], axis=0)
    kv_own = gbuf[4 + core, chip]
    k_own = jnp.concatenate([jnp.broadcast_to(kv_own[i:i + 1], (4, HEAD_DIM)) for i in range(4)], axis=0)
    v_own = jnp.concatenate([jnp.broadcast_to(kv_own[4 + i:5 + i], (4, HEAD_DIM)) for i in range(4)], axis=0)
    s_own = jnp.sum(q_own * k_own, axis=-1, keepdims=True) * SCALE
    top = pick(top, here)
    peak = jnp.maximum(top, s_own)
    f_old, f_new = jnp.exp(top - peak), jnp.exp(s_own - peak)
    acc = jnp.zeros((HALF, HEAD_DIM), F32)
    for group in (0, 1, 3, 2):
        part = rbuf.at[pl.ds(0, 15 if group == 0 else 16)]
        all_of(part, part, ssend.at[0], srecv.at[group]).wait_recv()
        base = lax.rem(zed + group, 4) * 16
        for c in range(16):
            acc += rbuf[base + c] * pick(facbuf[pl.ds(base + c, 1), :], here)
    attn = (acc * f_old + v_own * f_new) / (total * f_old + f_new)
    for h in range(HALF):
        lhs[:, h * 128:(h + 1) * 128] = jnp.where(row16 == h, attn, 0.0).astype(BF16)

    wocopy.wait()

    def out_cols(half, slot):
        for n in range(5):
            cols = pl.ds(pl.multiple_of(half * 1280 + n * 256, 256), 256)
            res = jnp.dot(lhs[...], wobuf[:, cols], preferred_element_type=F32)
            res = jnp.sum(res, axis=0, keepdims=True)
            for k in range(2):
                ypart[slot, pl.ds(2 * n + k, 1), :] = res[:, k * 128:(k + 1) * 128]

    out_cols(1 - core, 0)
    ycopy = pltpu.make_async_remote_copy(src_ref=ypart.at[0], dst_ref=yin, send_sem=ysem.at[0], recv_sem=ysem.at[1],
                                         device_id=dev(mate), device_id_type=MESH)
    ycopy.start()
    out_cols(core, 1)
    ycopy.wait()
    ysend[...] = ypart[1] + yin[...]

    def bcopy(s, group):
        return pltpu.make_async_remote_copy(src_ref=ysend, dst_ref=ybuf.at[core, chip], send_sem=bsend.at[0],
                                            recv_sem=brecv.at[group], device_id=dev(s * 2 + core), device_id_type=MESH)

    each_other(lambda s, group: bcopy(s, group).start())

    ybuf[core, chip] = ysend[...]

    def slab(half, group):
        return ybuf.at[half, pl.ds(lax.rem(zed + group, 4) * 16, 16)]

    def fcopy(half, group):
        ref = slab(half, group)
        return pltpu.make_async_remote_copy(src_ref=ref, dst_ref=ref, send_sem=fsend.at[group], recv_sem=frecv.at[group],
                                            device_id=dev(mate), device_id_type=MESH)

    def finish(half, group):
        rows = pl.ds(pl.multiple_of(lax.rem(zed + group, 4) * 16, 16), 16)
        for k in range(10):
            cols = pl.ds(pl.multiple_of(half * 1280 + k * 128, 128), 128)
            out_ref[rows, cols] = (tok_ref[rows, cols].astype(F32) + ybuf[half, rows, k, :]).astype(BF16)

    for group in (0, 1, 3, 2):
        ref = ybuf.at[core, pl.ds(0, 15 if group == 0 else 16)]
        all_of(ref, ref, bsend.at[0], brecv.at[group]).wait_recv()
        fcopy(core, group).start()
        finish(core, group)
    for group in (0, 1, 3, 2):
        fcopy(1 - core, group).wait_recv()
        finish(1 - core, group)

    for group in range(4):
        fcopy(core, group).wait_send()
    all_of(rst.at[others], rst.at[others], tsend.at[0], trecv.at[0]).wait_send()
    all_of(rbuf.at[others], rbuf.at[others], ssend.at[0], srecv.at[0]).wait_send()
    rest = ybuf.at[0, others]
    all_of(rest, rest, bsend.at[0], brecv.at[0]).wait_send()


def step_call(*args):
    dma = pltpu.SemaphoreType.DMA
    vmem = pltpu.VMEM
    vm = pl.BlockSpec(memory_space=pltpu.VMEM)
    return pl.pallas_call(
        step_kernel,
        name="decode_step",
        out_shape=(jax.ShapeDtypeStruct((SEQS, DIM), BF16), jax.ShapeDtypeStruct((SEQS, 2, KV_HEADS, HEAD_DIM), BF16),
                   jax.ShapeDtypeStruct((SEQS, 128, HEAD_DIM), BF16), jax.ShapeDtypeStruct((SEQS, 128, HEAD_DIM), BF16)),
        in_specs=[pl.BlockSpec(memory_space=pltpu.HBM)] * 12,
        out_specs=(vm,) * 4,
        scratch_shapes=[
            pltpu.SMEM((SEQS,), jnp.int32), vmem((SEQS, DIM), BF16), vmem((DIM,), BF16), vmem((1, HEAD_DIM), BF16), vmem((1, HEAD_DIM), BF16), vmem((1, HEAD_DIM), F32),
            dma((6,)), vmem((CHIPS, HEAD_DIM), F32),
            vmem((SEQS, DIM), BF16), vmem((SEQS, HEAD_DIM), F32), vmem((SEQS, HEAD_DIM), F32),
            vmem((12, DIM, 256), BF16), vmem((2048, DIM), BF16),
            vmem((6, SEQS, 8, HEAD_DIM), F32),
            vmem((SEQS, HEADS, HEAD_DIM), BF16), vmem((2, SEQS, HALF, HEAD_DIM), F32), vmem((SEQS, HALF, HEAD_DIM), F32),
            vmem((2, 8, 2, HEAD_DIM), F32), vmem((8, 2, HEAD_DIM), F32), vmem((2, 8, HEAD_DIM), F32),
            vmem((SEQS, HALF, HEAD_DIM), F32), vmem((8, 2, HEAD_DIM), F32),
            vmem((CHIPS, HALF, HEAD_DIM), F32), vmem((CHIPS, 2, HEAD_DIM), F32),
            vmem((HALF, 2048), BF16), vmem((2, 10, HEAD_DIM), F32), vmem((10, HEAD_DIM), F32), vmem((10, HEAD_DIM), F32),
            vmem((2, CHIPS, 10, HEAD_DIM), F32),
            dma((12,)), dma((1,)), dma((2, 4)), dma((3,)), dma((3,)), dma((8,)), dma((8,)), dma((1,)), dma((1,)),
            dma((1,)), dma((4,)), dma((1,)), dma((1,)), dma((2,)), dma((1,)), dma((4,)), dma((4,)), dma((4,)),
        ],
        compiler_params=pltpu.CompilerParams(collective_id=0, has_side_effects=True, vmem_limit_bytes=48 * 2 ** 20),
    )(*args)


def store_kernel(*refs):
    sem = refs[-1]
    count = (len(refs) - 1) // 2
    copies = [pltpu.make_async_copy(refs[i], refs[count + i], sem.at[i]) for i in range(count)]
    for c in copies:
        c.start()
    for c in copies:
        c.wait()


def store_call(*arrays):
    return pl.pallas_call(
        store_kernel,
        name="store",
        out_shape=tuple(jax.ShapeDtypeStruct(a.shape, a.dtype) for a in arrays),
        in_specs=[pl.BlockSpec(memory_space=pltpu.VMEM)] * len(arrays),
        out_specs=(pl.BlockSpec(memory_space=pl.ANY),) * len(arrays),
        scratch_shapes=[pltpu.SemaphoreType.DMA((len(arrays),))],
        compiler_params=pltpu.CompilerParams(vmem_limit_bytes=12 * 2 ** 20),
    )(*arrays)


def solution(mesh):
    cache_spec = P('dp', 'sp', None, None)

    def device_step(tokens, positions, k_cache, v_cache, w_q, w_k, w_v, w_o, attn_norm, q_norm, k_norm):
        inv = np.float32(ROPE_THETA) ** (-np.arange(HEAD_DIM // 2, dtype=np.float32) * np.float32(2.0) / np.float32(HEAD_DIM))
        freq = jnp.asarray(np.concatenate([inv, inv])[None, :].astype(np.float32))
        flat = (SEQS, SLOTS * KV_HEADS, HEAD_DIM)
        operands = (positions, tokens, attn_norm, q_norm[None, :], k_norm[None, :], freq, w_q, w_k, w_v, w_o, k_cache.reshape(flat), v_cache.reshape(flat))
        row, new, k_loc, v_loc = step_call(*[pltpu.with_memory_space_constraint(a, pltpu.HBM) for a in operands])
        k_out, v_out, new_kv, block_out = store_call(k_loc.reshape(k_cache.shape), v_loc.reshape(v_cache.shape), new, row)
        return block_out, k_out, v_out, new_kv

    return jax.shard_map(device_step, mesh=mesh, in_specs=(P('dp', None), P('dp'), cache_spec, cache_spec, P(), P(), P(), P(), P(), P(), P()), out_specs=(P('dp', None), cache_spec, cache_spec, P('dp', None, None, None)), check_vma=False)
```

```python
import functools

import jax
import jax.numpy as jnp
import numpy as np
from jax import lax
from jax.experimental import pallas as pl
from jax.experimental.pallas import tpu as pltpu
from jax.sharding import PartitionSpec as P

NORM_EPS = 1e-6
ROPE_THETA = 1000000.0
NEG_FILL = -1e30
SEQS, DIM, HEADS, KV_HEADS, HEAD_DIM, SLOTS = 64, 2560, 32, 8, 128, 16
HALF = HEADS // 2
CHIPS = 64
SCALE = HEAD_DIM ** -0.5
F32, BF16 = jnp.float32, jnp.bfloat16
MESH = pl.DeviceIdType.MESH
DEPTH = 2
TILES = 6
FAR_FIRST = sorted(range(16), key=lambda k: -(min(k // 4, 4 - k // 4) + min(k % 4, 4 - k % 4)))
LAG = 5


def rms(values, gain):
    return values * lax.rsqrt(jnp.mean(values * values, axis=-1, keepdims=True) + NORM_EPS) * gain


def iota(shape, axis):
    return lax.broadcasted_iota(jnp.int32, shape, axis)


def pick(row, lane):
    spread = jnp.broadcast_to(row, (HALF, HEAD_DIM))
    return jnp.sum(jnp.where(lane, spread, 0.0), axis=-1, keepdims=True)


def step_kernel(pos_hbm, tok_hbm, an_hbm, qn_hbm, kn_hbm, freq_hbm, wq_hbm, wk_hbm, wv_hbm, wo_hbm, kc_hbm, vc_hbm,
                out_ref, new_ref, kbuf, vbuf,
                pos_ref, tok_ref, an_ref, qn_ref, kn_ref, freq_ref, isem, facbuf, hid, cosr, sinr, wbuf, wobuf, gbuf, wts, obuf, oin, st, stin, fac, osend, stsend, rbuf, rst,
                lhs, ypart, yin, ysend, ybuf,
                wsem, wosem, csem, gsend, grecv, dsend, drecv, dssend, dsrecv,
                ssend, srecv, tsend, trecv, ysem, bsend, brecv, fsend, frecv):
    me = lax.axis_index("sp")
    chip, core = me // 2, me % 2
    zed, low = lax.div(chip, 16), lax.rem(chip, 16)
    mate = chip * 2 + (1 - core)
    start = me * SLOTS

    def dev(index):
        return (lax.axis_index("dp"), index)

    def tile_copy(t):
        src, col = ((wk_hbm, 0), (wv_hbm, 0))[t] if t < 2 else (wq_hbm, (t - 2) * 512)
        col = pl.multiple_of(core * (512 if t < 2 else 2048) + col, 512)
        return pltpu.make_async_copy(src.at[:, pl.ds(col, 512)], wbuf.at[t], wsem.at[t])

    def kvload(i):
        rows = pl.ds(i * 16, 16)
        return (pltpu.make_async_copy(kc_hbm.at[rows], kbuf.at[rows], csem.at[0, i]),
                pltpu.make_async_copy(vc_hbm.at[rows], vbuf.at[rows], csem.at[1, i]))

    def tile_ready(t):
        tile_copy(t).wait()
        if t + DEPTH < TILES:
            tile_copy(t + DEPTH).start()
        else:
            for i in (2 * (t + DEPTH - TILES), 2 * (t + DEPTH - TILES) + 1):
                for c in kvload(i):
                    c.start()

    inputs = [pltpu.make_async_copy(a, b, isem.at[i]) for i, (a, b) in enumerate(
        [(tok_hbm, tok_ref), (an_hbm, an_ref), (pos_hbm, pos_ref), (freq_hbm, freq_ref), (kn_hbm, kn_ref), (qn_hbm, qn_ref)])]
    for c in inputs:
        c.start()
    for t in range(DEPTH):
        tile_copy(t).start()
    def each_other(send):
        for dz in (2, 1, 3, 0):
            base = lax.rem(zed + dz, 4) * 16
            for k in FAR_FIRST:
                if dz or k:
                    send(base + lax.rem(low + k, 16), (4 - dz) % 4)

    barrier = pltpu.get_barrier_semaphore()
    pl.semaphore_signal(barrier, inc=1, device_id=dev(mate), device_id_type=MESH)

    @pl.loop(1, CHIPS)
    def _(off):
        pl.semaphore_signal(barrier, inc=1, device_id=dev(lax.rem(chip + off, CHIPS) * 2 + core), device_id_type=MESH)

    for c in inputs:
        c.wait()

    tok = tok_ref[...].astype(F32)
    hid[...] = rms(tok, an_ref[...].astype(F32).reshape(1, DIM)).astype(BF16)
    row8 = iota((SEQS, HEAD_DIM), 0)
    posv = jnp.zeros((SEQS, HEAD_DIM), jnp.int32)
    for s in range(SEQS):
        posv = jnp.where(row8 == s, pos_ref[s], posv)
    angle = posv.astype(F32) * freq_ref[...]
    cosr[...] = jnp.cos(angle)
    sinr[...] = jnp.where(iota((SEQS, HEAD_DIM), 1) < HEAD_DIM // 2, -1.0, 1.0) * jnp.sin(angle)

    def project(tile):
        return jnp.dot(hid[...], wbuf[tile], preferred_element_type=F32).astype(BF16).astype(F32)

    def rope(head, gain):
        normed = rms(head, gain)
        turned = normed * cosr[...] + pltpu.roll(normed, HEAD_DIM // 2, 1) * sinr[...]
        return turned.astype(BF16).astype(F32)

    for t in range(2):
        tile_ready(t)
        res = project(t)
        for h in range(4):
            head = res[:, h * 128:(h + 1) * 128]
            gbuf[4 + core, :, 4 * t + h, :] = head if t else rope(head, kn_ref[...].astype(F32))

    def gcopy(group, slot):
        return pltpu.make_async_remote_copy(src_ref=gbuf.at[group], dst_ref=gbuf.at[group], send_sem=gsend.at[slot],
                                            recv_sem=grecv.at[slot], device_id=dev(mate), device_id_type=MESH)

    for g in range(2):
        for t2 in range(2):
            t = 2 + g * 2 + t2
            tile_ready(t)
            res = project(t)
            for h in range(4):
                gbuf[2 * core + g, :, 4 * t2 + h, :] = rope(res[:, h * 128:(h + 1) * 128], qn_ref[...].astype(F32))
        if g == 0:
            pl.semaphore_wait(barrier, CHIPS)
            gcopy(4 + core, 2).start()
        gcopy(2 * core + g, g).start()

    wocopy = pltpu.make_async_copy(wo_hbm.at[pl.ds(pl.multiple_of(core * 2048, 2048), 2048)], wobuf, wosem.at[0])
    wocopy.start()
    for slot in range(3):
        gcopy(4 + core if slot == 2 else 2 * core + slot, slot).wait()
    for i in range(4):
        for c in kvload(i):
            c.wait()

    def block_of(i):
        return lax.rem(zed + 2 + i // 2 - (i // 4) * (2 * (i // 2) - 1), 4) * 2 + lax.rem(i, 2)

    row32, col32 = iota((HEADS, HEAD_DIM), 0), iota((HEADS, HEAD_DIM), 1)
    same_head = (col32 % KV_HEADS) == (row32 // 4)
    slot_of = col32 // KV_HEADS + start
    row16, lane16 = iota((HALF, HEAD_DIM), 0), iota((HALF, HEAD_DIM), 1)

    def weigh(blk):
        acc = [[jnp.zeros((HALF, HEAD_DIM), F32) for _ in range(2)] for _ in range(2)]
        for s8 in range(8):
            s = blk * 8 + s8
            q = jnp.concatenate([gbuf[g, s] for g in range(4)], axis=0).astype(BF16)
            scores = lax.dot_general(q, kbuf[s], (((1,), (1,)), ((), ())), preferred_element_type=F32) * SCALE
            live = same_head & (slot_of < pos_ref[s])
            scores = jnp.where(live, scores, NEG_FILL)
            peak = jnp.max(scores, axis=-1, keepdims=True)
            weights = jnp.where(live, jnp.exp(scores - peak), 0.0)
            total = jnp.sum(weights, axis=-1, keepdims=True)
            wts[s] = weights.astype(BF16)
            here = lane16 == s8 * HALF + row16
            for half in range(2):
                cut = slice(half * HALF, (half + 1) * HALF)
                acc[half][0] += jnp.where(here, peak[cut], 0.0)
                acc[half][1] += jnp.where(here, total[cut], 0.0)
        for half in range(2):
            for k in range(2):
                st[half, blk, pl.ds(k, 1), :] = jnp.sum(acc[half][k], axis=0, keepdims=True)

    def mix(i):
        blk = block_of(i)
        for s8 in range(8):
            s = blk * 8 + s8
            mixed = jnp.dot(wts[s], vbuf[s], preferred_element_type=F32)
            for half in range(2):
                obuf[half, s] = mixed[half * HALF:(half + 1) * HALF]
        ocopy(i).start()

    def ocopy(i):
        rows = pl.ds(block_of(i) * 8, 8)
        return pltpu.make_async_remote_copy(src_ref=obuf.at[1 - core, rows], dst_ref=oin.at[rows], send_sem=dsend.at[i],
                                            recv_sem=drecv.at[i], device_id=dev(mate), device_id_type=MESH)

    def merge(i):
        blk = block_of(i)
        ocopy(i).wait()
        f0, f1 = fac[0, pl.ds(blk, 1), :], fac[1, pl.ds(blk, 1), :]
        for s8 in range(8):
            s = blk * 8 + s8
            here = lane16 == s8 * HALF + row16
            osend[s] = obuf[core, s] * pick(f0, here) + oin[s] * pick(f1, here)
        group = lax.rem(zed - lax.div(blk, 2) + 4, 4)
        for s8 in range(8):
            s = blk * 8 + s8

            @pl.when(s != chip)
            def _():
                pltpu.make_async_remote_copy(src_ref=osend.at[s], dst_ref=rbuf.at[chip], send_sem=ssend.at[0], recv_sem=srecv.at[group],
                                             device_id=dev(s * 2 + core), device_id_type=MESH).start()

    @pl.loop(0, 8)
    def _(blk):
        weigh(blk)

    stcopy = pltpu.make_async_remote_copy(src_ref=st.at[1 - core], dst_ref=stin, send_sem=dssend.at[0], recv_sem=dsrecv.at[0],
                                          device_id=dev(mate), device_id_type=MESH)
    stcopy.start()

    @pl.loop(0, LAG)
    def _(i):
        mix(i)

    stcopy.wait()
    m0, l0, m1, l1 = st[core, :, 0, :], st[core, :, 1, :], stin[:, 0, :], stin[:, 1, :]
    top = jnp.maximum(m0, m1)
    f0, f1 = jnp.exp(m0 - top), jnp.exp(m1 - top)
    fac[0], fac[1] = f0, f1
    stsend[:, 0, :] = top
    stsend[:, 1, :] = l0 * f0 + l1 * f1

    def send_stats(s, _):
        pltpu.make_async_remote_copy(src_ref=stsend.at[lax.div(s, 8)], dst_ref=rst.at[chip], send_sem=tsend.at[0], recv_sem=trecv.at[0],
                                     device_id=dev(s * 2 + core), device_id_type=MESH).start()

    each_other(send_stats)

    @pl.loop(LAG, 8 + LAG)
    def _(i):
        @pl.when(i < 8)
        def _():
            mix(i)

        merge(i - LAG)

    rst[chip] = stsend[chip // 8]
    rbuf[chip] = osend[chip]

    def all_of(src, dst, send, recv):
        return pltpu.make_async_remote_copy(src_ref=src, dst_ref=dst, send_sem=send, recv_sem=recv, device_id=dev(mate),
                                            device_id_type=MESH)

    upper = iota((SEQS, 8, HEAD_DIM), 1) < 4
    new_ref[:, 0] = jnp.where(upper, gbuf[4], pltpu.roll(gbuf[5], 4, 1)).astype(BF16)
    new_ref[:, 1] = jnp.where(upper, pltpu.roll(gbuf[4], 4, 1), gbuf[5]).astype(BF16)

    slot_row = iota((128, HEAD_DIM), 0) // KV_HEADS + start

    @pl.loop(0, 16)
    def _(i):
        for s4 in range(4):
            s = i * 4 + s4
            first, second = gbuf[4, s], gbuf[5, s]
            mine = slot_row == pos_ref[s]
            k_new = jnp.where(upper[0], first, pltpu.roll(second, 4, 0))
            v_new = jnp.where(upper[0], pltpu.roll(first, 4, 0), second)
            kbuf[s] = jnp.where(mine, jnp.concatenate([k_new] * SLOTS, axis=0).astype(BF16), kbuf[s])
            vbuf[s] = jnp.where(mine, jnp.concatenate([v_new] * SLOTS, axis=0).astype(BF16), vbuf[s])

    others = pl.ds(0, CHIPS - 1)
    all_of(rst.at[others], rst.at[others], tsend.at[0], trecv.at[0]).wait_recv()
    here = lane16 == lax.rem(chip, 8) * HALF + row16
    tops = rst[:, 0, :]
    top = jnp.max(tops, axis=0, keepdims=True)
    facs = jnp.exp(tops - top)
    facbuf[...] = facs
    total = pick(jnp.sum(rst[:, 1, :] * facs, axis=0, keepdims=True), here)
    q_own = jnp.concatenate([gbuf[2 * core, chip], gbuf[2 * core + 1, chip]], axis=0)
    kv_own = gbuf[4 + core, chip]
    k_own = jnp.concatenate([jnp.broadcast_to(kv_own[i:i + 1], (4, HEAD_DIM)) for i in range(4)], axis=0)
    v_own = jnp.concatenate([jnp.broadcast_to(kv_own[4 + i:5 + i], (4, HEAD_DIM)) for i in range(4)], axis=0)
    s_own = jnp.sum(q_own * k_own, axis=-1, keepdims=True) * SCALE
    top = pick(top, here)
    peak = jnp.maximum(top, s_own)
    f_old, f_new = jnp.exp(top - peak), jnp.exp(s_own - peak)
    acc = jnp.zeros((HALF, HEAD_DIM), F32)
    for group in (0, 1, 3, 2):
        part = rbuf.at[pl.ds(0, 15 if group == 0 else 16)]
        all_of(part, part, ssend.at[0], srecv.at[group]).wait_recv()
        base = lax.rem(zed + group, 4) * 16
        for c in range(16):
            acc += rbuf[base + c] * pick(facbuf[pl.ds(base + c, 1), :], here)
    attn = (acc * f_old + v_own * f_new) / (total * f_old + f_new)
    for h in range(HALF):
        lhs[:, h * 128:(h + 1) * 128] = jnp.where(row16 == h, attn, 0.0).astype(BF16)

    wocopy.wait()

    def out_cols(half, slot):
        cols = pl.ds(pl.multiple_of(half * 1280, 1280), 1280)
        res = jnp.sum(jnp.dot(lhs[...], wobuf[:, cols], preferred_element_type=F32), axis=0, keepdims=True)
        for k in range(10):
            ypart[slot, pl.ds(k, 1), :] = res[:, k * 128:(k + 1) * 128]

    out_cols(1 - core, 0)
    ycopy = pltpu.make_async_remote_copy(src_ref=ypart.at[0], dst_ref=yin, send_sem=ysem.at[0], recv_sem=ysem.at[1],
                                         device_id=dev(mate), device_id_type=MESH)
    ycopy.start()
    out_cols(core, 1)
    ycopy.wait()
    ysend[...] = ypart[1] + yin[...]

    def bcopy(s, group):
        return pltpu.make_async_remote_copy(src_ref=ysend, dst_ref=ybuf.at[core, chip], send_sem=bsend.at[0],
                                            recv_sem=brecv.at[group], device_id=dev(s * 2 + core), device_id_type=MESH)

    each_other(lambda s, group: bcopy(s, group).start())

    ybuf[core, chip] = ysend[...]

    def slab(half, group):
        return ybuf.at[half, pl.ds(lax.rem(zed + group, 4) * 16, 16)]

    def fcopy(half, group):
        ref = slab(half, group)
        return pltpu.make_async_remote_copy(src_ref=ref, dst_ref=ref, send_sem=fsend.at[group], recv_sem=frecv.at[group],
                                            device_id=dev(mate), device_id_type=MESH)

    def finish(half, group):
        rows = pl.ds(pl.multiple_of(lax.rem(zed + group, 4) * 16, 16), 16)
        for k in range(10):
            cols = pl.ds(pl.multiple_of(half * 1280 + k * 128, 128), 128)
            out_ref[rows, cols] = (tok_ref[rows, cols].astype(F32) + ybuf[half, rows, k, :]).astype(BF16)

    for group in (0, 1, 3, 2):
        ref = ybuf.at[core, pl.ds(0, 15 if group == 0 else 16)]
        all_of(ref, ref, bsend.at[0], brecv.at[group]).wait_recv()
        fcopy(core, group).start()
        finish(core, group)
    for group in (0, 1, 3, 2):
        fcopy(1 - core, group).wait_recv()
        finish(1 - core, group)

    for group in range(4):
        fcopy(core, group).wait_send()
    all_of(rst.at[others], rst.at[others], tsend.at[0], trecv.at[0]).wait_send()
    all_of(rbuf.at[others], rbuf.at[others], ssend.at[0], srecv.at[0]).wait_send()
    rest = ybuf.at[0, others]
    all_of(rest, rest, bsend.at[0], brecv.at[0]).wait_send()


def step_call(*args):
    dma = pltpu.SemaphoreType.DMA
    vmem = pltpu.VMEM
    vm = pl.BlockSpec(memory_space=pltpu.VMEM)
    return pl.pallas_call(
        step_kernel,
        name="decode_step",
        out_shape=(jax.ShapeDtypeStruct((SEQS, DIM), BF16), jax.ShapeDtypeStruct((SEQS, 2, KV_HEADS, HEAD_DIM), BF16),
                   jax.ShapeDtypeStruct((SEQS, 128, HEAD_DIM), BF16), jax.ShapeDtypeStruct((SEQS, 128, HEAD_DIM), BF16)),
        in_specs=[pl.BlockSpec(memory_space=pltpu.HBM)] * 12,
        out_specs=(vm,) * 4,
        scratch_shapes=[
            pltpu.SMEM((SEQS,), jnp.int32), vmem((SEQS, DIM), BF16), vmem((DIM,), BF16), vmem((1, HEAD_DIM), BF16), vmem((1, HEAD_DIM), BF16), vmem((1, HEAD_DIM), F32),
            dma((6,)), vmem((CHIPS, HEAD_DIM), F32),
            vmem((SEQS, DIM), BF16), vmem((SEQS, HEAD_DIM), F32), vmem((SEQS, HEAD_DIM), F32),
            vmem((TILES, DIM, 512), BF16), vmem((2048, DIM), BF16),
            vmem((6, SEQS, 8, HEAD_DIM), F32),
            vmem((SEQS, HEADS, HEAD_DIM), BF16), vmem((2, SEQS, HALF, HEAD_DIM), F32), vmem((SEQS, HALF, HEAD_DIM), F32),
            vmem((2, 8, 2, HEAD_DIM), F32), vmem((8, 2, HEAD_DIM), F32), vmem((2, 8, HEAD_DIM), F32),
            vmem((SEQS, HALF, HEAD_DIM), F32), vmem((8, 2, HEAD_DIM), F32),
            vmem((CHIPS, HALF, HEAD_DIM), F32), vmem((CHIPS, 2, HEAD_DIM), F32),
            vmem((HALF, 2048), BF16), vmem((2, 10, HEAD_DIM), F32), vmem((10, HEAD_DIM), F32), vmem((10, HEAD_DIM), F32),
            vmem((2, CHIPS, 10, HEAD_DIM), F32),
            dma((TILES,)), dma((1,)), dma((2, 4)), dma((3,)), dma((3,)), dma((8,)), dma((8,)), dma((1,)), dma((1,)),
            dma((1,)), dma((4,)), dma((1,)), dma((1,)), dma((2,)), dma((1,)), dma((4,)), dma((4,)), dma((4,)),
        ],
        compiler_params=pltpu.CompilerParams(collective_id=0, has_side_effects=True, vmem_limit_bytes=48 * 2 ** 20),
    )(*args)


def store_kernel(*refs):
    sem = refs[-1]
    count = (len(refs) - 1) // 2
    copies = [pltpu.make_async_copy(refs[i], refs[count + i], sem.at[i]) for i in range(count)]
    for c in copies:
        c.start()
    for c in copies:
        c.wait()


def store_call(*arrays):
    return pl.pallas_call(
        store_kernel,
        name="store",
        out_shape=tuple(jax.ShapeDtypeStruct(a.shape, a.dtype) for a in arrays),
        in_specs=[pl.BlockSpec(memory_space=pltpu.VMEM)] * len(arrays),
        out_specs=(pl.BlockSpec(memory_space=pl.ANY),) * len(arrays),
        scratch_shapes=[pltpu.SemaphoreType.DMA((len(arrays),))],
        compiler_params=pltpu.CompilerParams(vmem_limit_bytes=12 * 2 ** 20),
    )(*arrays)


def solution(mesh):
    cache_spec = P('dp', 'sp', None, None)

    def device_step(tokens, positions, k_cache, v_cache, w_q, w_k, w_v, w_o, attn_norm, q_norm, k_norm):
        inv = np.float32(ROPE_THETA) ** (-np.arange(HEAD_DIM // 2, dtype=np.float32) * np.float32(2.0) / np.float32(HEAD_DIM))
        freq = jnp.asarray(np.concatenate([inv, inv])[None, :].astype(np.float32))
        flat = (SEQS, SLOTS * KV_HEADS, HEAD_DIM)
        operands = (positions, tokens, attn_norm, q_norm[None, :], k_norm[None, :], freq, w_q, w_k, w_v, w_o, k_cache.reshape(flat), v_cache.reshape(flat))
        row, new, k_loc, v_loc = step_call(*[pltpu.with_memory_space_constraint(a, pltpu.HBM) for a in operands])
        k_out, v_out, new_kv, block_out = store_call(k_loc.reshape(k_cache.shape), v_loc.reshape(v_cache.shape), new, row)
        return block_out, k_out, v_out, new_kv

    return jax.shard_map(device_step, mesh=mesh, in_specs=(P('dp', None), P('dp'), cache_spec, cache_spec, P(), P(), P(), P(), P(), P(), P()), out_specs=(P('dp', None), cache_spec, cache_spec, P('dp', None, None, None)), check_vma=False)
```

```python
import functools

import jax
import jax.numpy as jnp
import numpy as np
from jax import lax
from jax.experimental import pallas as pl
from jax.experimental.pallas import tpu as pltpu
from jax.sharding import PartitionSpec as P

NORM_EPS = 1e-6
ROPE_THETA = 1000000.0
NEG_FILL = -1e30
SEQS, DIM, HEADS, KV_HEADS, HEAD_DIM, SLOTS = 64, 2560, 32, 8, 128, 16
HALF = HEADS // 2
CHIPS = 64
SCALE = HEAD_DIM ** -0.5
F32, BF16 = jnp.float32, jnp.bfloat16
MESH = pl.DeviceIdType.MESH
DEPTH = 2
TILES = 6
HOPS = (0, 1, 2, 1)
OFFSETS = sorted(((a, b, c) for a in range(4) for b in range(4) for c in range(4)), key=lambda o: -sum(HOPS[d] for d in o))
LAG = 5


def rms(values, gain):
    return values * lax.rsqrt(jnp.mean(values * values, axis=-1, keepdims=True) + NORM_EPS) * gain


def iota(shape, axis):
    return lax.broadcasted_iota(jnp.int32, shape, axis)


def pick(row, lane):
    spread = jnp.broadcast_to(row, (HALF, HEAD_DIM))
    return jnp.sum(jnp.where(lane, spread, 0.0), axis=-1, keepdims=True)


def step_kernel(pos_hbm, tok_hbm, an_hbm, qn_hbm, kn_hbm, freq_hbm, wq_hbm, wk_hbm, wv_hbm, wo_hbm, kc_hbm, vc_hbm,
                out_ref, new_ref, kbuf, vbuf,
                pos_ref, tok_ref, an_ref, qn_ref, kn_ref, freq_ref, isem, facbuf, hid, cosr, sinr, wbuf, wobuf, gbuf, wts, obuf, oin, st, stin, fac, osend, stsend, rbuf, rst,
                lhs, ypart, yin, ysend, ybuf,
                wsem, wosem, csem, gsend, grecv, dsend, drecv, dssend, dsrecv,
                ssend, srecv, tsend, trecv, ysem, bsend, brecv, fsend, frecv):
    me = lax.axis_index("sp")
    chip, core = me // 2, me % 2
    place = (lax.div(chip, 16), lax.rem(lax.div(chip, 4), 4), lax.rem(chip, 4))
    zed = place[0]
    turn = [[lax.rem(p + d, 4) * w for d in range(4)] for p, w in zip(place, (16, 4, 1))]

    def chip_at(offset):
        return turn[0][offset[0]] + turn[1][offset[1]] + turn[2][offset[2]]
    mate = chip * 2 + (1 - core)
    start = me * SLOTS

    def dev(index):
        return (lax.axis_index("dp"), index)

    def tile_copy(t):
        src, col = ((wk_hbm, 0), (wv_hbm, 0))[t] if t < 2 else (wq_hbm, (t - 2) * 512)
        col = pl.multiple_of(core * (512 if t < 2 else 2048) + col, 512)
        return pltpu.make_async_copy(src.at[:, pl.ds(col, 512)], wbuf.at[t], wsem.at[t])

    def kvload(i):
        rows = pl.ds(i * 16, 16)
        return (pltpu.make_async_copy(kc_hbm.at[rows], kbuf.at[rows], csem.at[0, i]),
                pltpu.make_async_copy(vc_hbm.at[rows], vbuf.at[rows], csem.at[1, i]))

    def tile_ready(t):
        tile_copy(t).wait()
        if t + DEPTH < TILES:
            tile_copy(t + DEPTH).start()
        else:
            for i in (2 * (t + DEPTH - TILES), 2 * (t + DEPTH - TILES) + 1):
                for c in kvload(i):
                    c.start()

    inputs = [pltpu.make_async_copy(a, b, isem.at[i]) for i, (a, b) in enumerate(
        [(tok_hbm, tok_ref), (an_hbm, an_ref), (pos_hbm, pos_ref), (freq_hbm, freq_ref), (kn_hbm, kn_ref), (qn_hbm, qn_ref)])]
    for c in inputs:
        c.start()
    for t in range(DEPTH):
        tile_copy(t).start()
    def each_other(send):
        for o in OFFSETS[:-1]:
            send(chip_at(o), (4 - o[0]) % 4)

    barrier = pltpu.get_barrier_semaphore()
    pl.semaphore_signal(barrier, inc=1, device_id=dev(mate), device_id_type=MESH)

    @pl.loop(1, CHIPS)
    def _(off):
        pl.semaphore_signal(barrier, inc=1, device_id=dev(lax.rem(chip + off, CHIPS) * 2 + core), device_id_type=MESH)

    for c in inputs:
        c.wait()

    tok = tok_ref[...].astype(F32)
    hid[...] = rms(tok, an_ref[...].astype(F32).reshape(1, DIM)).astype(BF16)
    row8 = iota((SEQS, HEAD_DIM), 0)
    posv = jnp.zeros((SEQS, HEAD_DIM), jnp.int32)
    for s in range(SEQS):
        posv = jnp.where(row8 == s, pos_ref[s], posv)
    angle = posv.astype(F32) * freq_ref[...]
    cosr[...] = jnp.cos(angle)
    sinr[...] = jnp.where(iota((SEQS, HEAD_DIM), 1) < HEAD_DIM // 2, -1.0, 1.0) * jnp.sin(angle)

    def project(tile):
        return jnp.dot(hid[...], wbuf[tile], preferred_element_type=F32).astype(BF16).astype(F32)

    def rope(head, gain):
        normed = rms(head, gain)
        turned = normed * cosr[...] + pltpu.roll(normed, HEAD_DIM // 2, 1) * sinr[...]
        return turned.astype(BF16).astype(F32)

    for t in range(2):
        tile_ready(t)
        res = project(t)
        for h in range(4):
            head = res[:, h * 128:(h + 1) * 128]
            gbuf[4 + core, :, 4 * t + h, :] = head if t else rope(head, kn_ref[...].astype(F32))

    def gcopy(group, slot):
        return pltpu.make_async_remote_copy(src_ref=gbuf.at[group], dst_ref=gbuf.at[group], send_sem=gsend.at[slot],
                                            recv_sem=grecv.at[slot], device_id=dev(mate), device_id_type=MESH)

    for g in range(2):
        for t2 in range(2):
            t = 2 + g * 2 + t2
            tile_ready(t)
            res = project(t)
            for h in range(4):
                gbuf[2 * core + g, :, 4 * t2 + h, :] = rope(res[:, h * 128:(h + 1) * 128], qn_ref[...].astype(F32))
        if g == 0:
            pl.semaphore_wait(barrier, CHIPS)
            gcopy(4 + core, 2).start()
        gcopy(2 * core + g, g).start()

    wocopy = pltpu.make_async_copy(wo_hbm.at[pl.ds(pl.multiple_of(core * 2048, 2048), 2048)], wobuf, wosem.at[0])
    wocopy.start()
    for slot in range(3):
        gcopy(4 + core if slot == 2 else 2 * core + slot, slot).wait()
    for i in range(4):
        for c in kvload(i):
            c.wait()

    row32, col32 = iota((HEADS, HEAD_DIM), 0), iota((HEADS, HEAD_DIM), 1)
    same_head = (col32 % KV_HEADS) == (row32 // 4)
    slot_of = col32 // KV_HEADS + start
    row16, lane16 = iota((HALF, HEAD_DIM), 0), iota((HALF, HEAD_DIM), 1)

    def weigh(blk):
        acc = [[jnp.zeros((HALF, HEAD_DIM), F32) for _ in range(2)] for _ in range(2)]
        for s8 in range(8):
            s = blk * 8 + s8
            q = jnp.concatenate([gbuf[g, s] for g in range(4)], axis=0).astype(BF16)
            scores = lax.dot_general(q, kbuf[s], (((1,), (1,)), ((), ())), preferred_element_type=F32) * SCALE
            live = same_head & (slot_of < pos_ref[s])
            scores = jnp.where(live, scores, NEG_FILL)
            peak = jnp.max(scores, axis=-1, keepdims=True)
            weights = jnp.where(live, jnp.exp(scores - peak), 0.0)
            total = jnp.sum(weights, axis=-1, keepdims=True)
            wts[s] = weights.astype(BF16)
            here = lane16 == s8 * HALF + row16
            for half in range(2):
                cut = slice(half * HALF, (half + 1) * HALF)
                acc[half][0] += jnp.where(here, peak[cut], 0.0)
                acc[half][1] += jnp.where(here, total[cut], 0.0)
        for half in range(2):
            for k in range(2):
                st[half, blk, pl.ds(k, 1), :] = jnp.sum(acc[half][k], axis=0, keepdims=True)

    def mix(i):
        for n in range(8 * i, 8 * i + 8):
            s = chip_at(OFFSETS[n])
            mixed = jnp.dot(wts[s], vbuf[s], preferred_element_type=F32)
            for half in range(2):
                obuf[half, n] = mixed[half * HALF:(half + 1) * HALF]
        ocopy(i).start()

    def ocopy(i):
        rows = pl.ds(i * 8, 8)
        return pltpu.make_async_remote_copy(src_ref=obuf.at[1 - core, rows], dst_ref=oin.at[rows], send_sem=dsend.at[i],
                                            recv_sem=drecv.at[i], device_id=dev(mate), device_id_type=MESH)

    def merge(i):
        ocopy(i).wait()
        for n in range(8 * i, 8 * i + 8):
            s = chip_at(OFFSETS[n])
            here = lane16 == lax.rem(s, 8) * HALF + row16
            f0, f1 = fac[0, pl.ds(lax.div(s, 8), 1), :], fac[1, pl.ds(lax.div(s, 8), 1), :]
            osend[n] = obuf[core, n] * pick(f0, here) + oin[n] * pick(f1, here)
        for n in range(8 * i, min(8 * i + 8, CHIPS - 1)):
            pltpu.make_async_remote_copy(src_ref=osend.at[n], dst_ref=rbuf.at[chip], send_sem=ssend.at[0],
                                         recv_sem=srecv.at[(4 - OFFSETS[n][0]) % 4],
                                         device_id=dev(chip_at(OFFSETS[n]) * 2 + core), device_id_type=MESH).start()

    @pl.loop(0, 8)
    def _(blk):
        weigh(blk)

    stcopy = pltpu.make_async_remote_copy(src_ref=st.at[1 - core], dst_ref=stin, send_sem=dssend.at[0], recv_sem=dsrecv.at[0],
                                          device_id=dev(mate), device_id_type=MESH)
    stcopy.start()

    for i in range(LAG):
        mix(i)

    stcopy.wait()
    m0, l0, m1, l1 = st[core, :, 0, :], st[core, :, 1, :], stin[:, 0, :], stin[:, 1, :]
    top = jnp.maximum(m0, m1)
    f0, f1 = jnp.exp(m0 - top), jnp.exp(m1 - top)
    fac[0], fac[1] = f0, f1
    stsend[:, 0, :] = top
    stsend[:, 1, :] = l0 * f0 + l1 * f1

    def send_stats(s, _):
        pltpu.make_async_remote_copy(src_ref=stsend.at[lax.div(s, 8)], dst_ref=rst.at[chip], send_sem=tsend.at[0], recv_sem=trecv.at[0],
                                     device_id=dev(s * 2 + core), device_id_type=MESH).start()

    each_other(send_stats)

    for i in range(LAG, 8 + LAG):
        if i < 8:
            mix(i)
        merge(i - LAG)

    rst[chip] = stsend[chip // 8]
    rbuf[chip] = osend[CHIPS - 1]

    def all_of(src, dst, send, recv):
        return pltpu.make_async_remote_copy(src_ref=src, dst_ref=dst, send_sem=send, recv_sem=recv, device_id=dev(mate),
                                            device_id_type=MESH)

    upper = iota((SEQS, 8, HEAD_DIM), 1) < 4
    new_ref[:, 0] = jnp.where(upper, gbuf[4], pltpu.roll(gbuf[5], 4, 1)).astype(BF16)
    new_ref[:, 1] = jnp.where(upper, pltpu.roll(gbuf[4], 4, 1), gbuf[5]).astype(BF16)

    slot_row = iota((128, HEAD_DIM), 0) // KV_HEADS + start

    @pl.loop(0, 16)
    def _(i):
        for s4 in range(4):
            s = i * 4 + s4
            first, second = gbuf[4, s], gbuf[5, s]
            mine = slot_row == pos_ref[s]
            k_new = jnp.where(upper[0], first, pltpu.roll(second, 4, 0))
            v_new = jnp.where(upper[0], pltpu.roll(first, 4, 0), second)
            kbuf[s] = jnp.where(mine, jnp.concatenate([k_new] * SLOTS, axis=0).astype(BF16), kbuf[s])
            vbuf[s] = jnp.where(mine, jnp.concatenate([v_new] * SLOTS, axis=0).astype(BF16), vbuf[s])

    others = pl.ds(0, CHIPS - 1)
    all_of(rst.at[others], rst.at[others], tsend.at[0], trecv.at[0]).wait_recv()
    here = lane16 == lax.rem(chip, 8) * HALF + row16
    tops = rst[:, 0, :]
    top = jnp.max(tops, axis=0, keepdims=True)
    facs = jnp.exp(tops - top)
    facbuf[...] = facs
    total = pick(jnp.sum(rst[:, 1, :] * facs, axis=0, keepdims=True), here)
    q_own = jnp.concatenate([gbuf[2 * core, chip], gbuf[2 * core + 1, chip]], axis=0)
    kv_own = gbuf[4 + core, chip]
    k_own = jnp.concatenate([jnp.broadcast_to(kv_own[i:i + 1], (4, HEAD_DIM)) for i in range(4)], axis=0)
    v_own = jnp.concatenate([jnp.broadcast_to(kv_own[4 + i:5 + i], (4, HEAD_DIM)) for i in range(4)], axis=0)
    s_own = jnp.sum(q_own * k_own, axis=-1, keepdims=True) * SCALE
    top = pick(top, here)
    peak = jnp.maximum(top, s_own)
    f_old, f_new = jnp.exp(top - peak), jnp.exp(s_own - peak)
    acc = jnp.zeros((HALF, HEAD_DIM), F32)
    for group in (0, 1, 3, 2):
        part = rbuf.at[pl.ds(0, 15 if group == 0 else 16)]
        all_of(part, part, ssend.at[0], srecv.at[group]).wait_recv()
        base = lax.rem(zed + group, 4) * 16
        for c in range(16):
            acc += rbuf[base + c] * pick(facbuf[pl.ds(base + c, 1), :], here)
    attn = (acc * f_old + v_own * f_new) / (total * f_old + f_new)
    for h in range(HALF):
        lhs[:, h * 128:(h + 1) * 128] = jnp.where(row16 == h, attn, 0.0).astype(BF16)

    wocopy.wait()

    def out_cols(half, slot):
        cols = pl.ds(pl.multiple_of(half * 1280, 1280), 1280)
        res = jnp.sum(jnp.dot(lhs[...], wobuf[:, cols], preferred_element_type=F32), axis=0, keepdims=True)
        for k in range(10):
            ypart[slot, pl.ds(k, 1), :] = res[:, k * 128:(k + 1) * 128]

    out_cols(1 - core, 0)
    ycopy = pltpu.make_async_remote_copy(src_ref=ypart.at[0], dst_ref=yin, send_sem=ysem.at[0], recv_sem=ysem.at[1],
                                         device_id=dev(mate), device_id_type=MESH)
    ycopy.start()
    out_cols(core, 1)
    ycopy.wait()
    ysend[...] = ypart[1] + yin[...]

    def bcopy(s, group):
        return pltpu.make_async_remote_copy(src_ref=ysend, dst_ref=ybuf.at[core, chip], send_sem=bsend.at[0],
                                            recv_sem=brecv.at[group], device_id=dev(s * 2 + core), device_id_type=MESH)

    each_other(lambda s, group: bcopy(s, group).start())

    ybuf[core, chip] = ysend[...]

    def slab(half, group):
        return ybuf.at[half, pl.ds(lax.rem(zed + group, 4) * 16, 16)]

    def fcopy(half, group):
        ref = slab(half, group)
        return pltpu.make_async_remote_copy(src_ref=ref, dst_ref=ref, send_sem=fsend.at[group], recv_sem=frecv.at[group],
                                            device_id=dev(mate), device_id_type=MESH)

    def finish(half, group):
        rows = pl.ds(pl.multiple_of(lax.rem(zed + group, 4) * 16, 16), 16)
        for k in range(10):
            cols = pl.ds(pl.multiple_of(half * 1280 + k * 128, 128), 128)
            out_ref[rows, cols] = (tok_ref[rows, cols].astype(F32) + ybuf[half, rows, k, :]).astype(BF16)

    for group in (0, 1, 3, 2):
        ref = ybuf.at[core, pl.ds(0, 15 if group == 0 else 16)]
        all_of(ref, ref, bsend.at[0], brecv.at[group]).wait_recv()
        fcopy(core, group).start()
        finish(core, group)
    for group in (0, 1, 3, 2):
        fcopy(1 - core, group).wait_recv()
        finish(1 - core, group)

    for group in range(4):
        fcopy(core, group).wait_send()
    all_of(rst.at[others], rst.at[others], tsend.at[0], trecv.at[0]).wait_send()
    all_of(rbuf.at[others], rbuf.at[others], ssend.at[0], srecv.at[0]).wait_send()
    rest = ybuf.at[0, others]
    all_of(rest, rest, bsend.at[0], brecv.at[0]).wait_send()


def step_call(*args):
    dma = pltpu.SemaphoreType.DMA
    vmem = pltpu.VMEM
    vm = pl.BlockSpec(memory_space=pltpu.VMEM)
    return pl.pallas_call(
        step_kernel,
        name="decode_step",
        out_shape=(jax.ShapeDtypeStruct((SEQS, DIM), BF16), jax.ShapeDtypeStruct((SEQS, 2, KV_HEADS, HEAD_DIM), BF16),
                   jax.ShapeDtypeStruct((SEQS, 128, HEAD_DIM), BF16), jax.ShapeDtypeStruct((SEQS, 128, HEAD_DIM), BF16)),
        in_specs=[pl.BlockSpec(memory_space=pltpu.HBM)] * 12,
        out_specs=(vm,) * 4,
        scratch_shapes=[
            pltpu.SMEM((SEQS,), jnp.int32), vmem((SEQS, DIM), BF16), vmem((DIM,), BF16), vmem((1, HEAD_DIM), BF16), vmem((1, HEAD_DIM), BF16), vmem((1, HEAD_DIM), F32),
            dma((6,)), vmem((CHIPS, HEAD_DIM), F32),
            vmem((SEQS, DIM), BF16), vmem((SEQS, HEAD_DIM), F32), vmem((SEQS, HEAD_DIM), F32),
            vmem((TILES, DIM, 512), BF16), vmem((2048, DIM), BF16),
            vmem((6, SEQS, 8, HEAD_DIM), F32),
            vmem((SEQS, HEADS, HEAD_DIM), BF16), vmem((2, SEQS, HALF, HEAD_DIM), F32), vmem((SEQS, HALF, HEAD_DIM), F32),
            vmem((2, 8, 2, HEAD_DIM), F32), vmem((8, 2, HEAD_DIM), F32), vmem((2, 8, HEAD_DIM), F32),
            vmem((SEQS, HALF, HEAD_DIM), F32), vmem((8, 2, HEAD_DIM), F32),
            vmem((CHIPS, HALF, HEAD_DIM), F32), vmem((CHIPS, 2, HEAD_DIM), F32),
            vmem((HALF, 2048), BF16), vmem((2, 10, HEAD_DIM), F32), vmem((10, HEAD_DIM), F32), vmem((10, HEAD_DIM), F32),
            vmem((2, CHIPS, 10, HEAD_DIM), F32),
            dma((TILES,)), dma((1,)), dma((2, 4)), dma((3,)), dma((3,)), dma((8,)), dma((8,)), dma((1,)), dma((1,)),
            dma((1,)), dma((4,)), dma((1,)), dma((1,)), dma((2,)), dma((1,)), dma((4,)), dma((4,)), dma((4,)),
        ],
        compiler_params=pltpu.CompilerParams(collective_id=0, has_side_effects=True, vmem_limit_bytes=48 * 2 ** 20),
    )(*args)


def store_kernel(*refs):
    sem = refs[-1]
    count = (len(refs) - 1) // 2
    copies = [pltpu.make_async_copy(refs[i], refs[count + i], sem.at[i]) for i in range(count)]
    for c in copies:
        c.start()
    for c in copies:
        c.wait()


def store_call(*arrays):
    return pl.pallas_call(
        store_kernel,
        name="store",
        out_shape=tuple(jax.ShapeDtypeStruct(a.shape, a.dtype) for a in arrays),
        in_specs=[pl.BlockSpec(memory_space=pltpu.VMEM)] * len(arrays),
        out_specs=(pl.BlockSpec(memory_space=pl.ANY),) * len(arrays),
        scratch_shapes=[pltpu.SemaphoreType.DMA((len(arrays),))],
        compiler_params=pltpu.CompilerParams(vmem_limit_bytes=12 * 2 ** 20),
    )(*arrays)


def solution(mesh):
    cache_spec = P('dp', 'sp', None, None)

    def device_step(tokens, positions, k_cache, v_cache, w_q, w_k, w_v, w_o, attn_norm, q_norm, k_norm):
        inv = np.float32(ROPE_THETA) ** (-np.arange(HEAD_DIM // 2, dtype=np.float32) * np.float32(2.0) / np.float32(HEAD_DIM))
        freq = jnp.asarray(np.concatenate([inv, inv])[None, :].astype(np.float32))
        flat = (SEQS, SLOTS * KV_HEADS, HEAD_DIM)
        operands = (positions, tokens, attn_norm, q_norm[None, :], k_norm[None, :], freq, w_q, w_k, w_v, w_o, k_cache.reshape(flat), v_cache.reshape(flat))
        row, new, k_loc, v_loc = step_call(*[pltpu.with_memory_space_constraint(a, pltpu.HBM) for a in operands])
        k_out, v_out, new_kv, block_out = store_call(k_loc.reshape(k_cache.shape), v_loc.reshape(v_cache.shape), new, row)
        return block_out, k_out, v_out, new_kv

    return jax.shard_map(device_step, mesh=mesh, in_specs=(P('dp', None), P('dp'), cache_spec, cache_spec, P(), P(), P(), P(), P(), P(), P()), out_specs=(P('dp', None), cache_spec, cache_spec, P('dp', None, None, None)), check_vma=False)
```

```python
import functools

import jax
import jax.numpy as jnp
import numpy as np
from jax import lax
from jax.experimental import pallas as pl
from jax.experimental.pallas import tpu as pltpu
from jax.sharding import PartitionSpec as P

NORM_EPS = 1e-6
ROPE_THETA = 1000000.0
NEG_FILL = -1e30
SEQS, DIM, HEADS, KV_HEADS, HEAD_DIM, SLOTS = 64, 2560, 32, 8, 128, 16
HALF = HEADS // 2
CHIPS = 64
SCALE = HEAD_DIM ** -0.5
F32, BF16 = jnp.float32, jnp.bfloat16
MESH = pl.DeviceIdType.MESH
DEPTH = 2
TILES = 6
FAR_FIRST = sorted(range(16), key=lambda k: -(min(k // 4, 4 - k // 4) + min(k % 4, 4 - k % 4)))
LAG = 5


def rms(values, gain):
    return values * lax.rsqrt(jnp.mean(values * values, axis=-1, keepdims=True) + NORM_EPS) * gain


def iota(shape, axis):
    return lax.broadcasted_iota(jnp.int32, shape, axis)


def pick(row, lane):
    spread = jnp.broadcast_to(row, (HALF, HEAD_DIM))
    return jnp.sum(jnp.where(lane, spread, 0.0), axis=-1, keepdims=True)


def step_kernel(pos_hbm, tok_hbm, an_hbm, qn_hbm, kn_hbm, freq_hbm, wq_hbm, wk_hbm, wv_hbm, wo_hbm, kc_hbm, vc_hbm,
                out_ref, new_ref, kbuf, vbuf,
                pos_ref, tok_ref, an_ref, qn_ref, kn_ref, freq_ref, isem, facbuf, hid, cosr, sinr, wbuf, wobuf, gbuf, wts, obuf, oin, st, stin, fac, osend, stsend, rbuf, rst,
                lhs, ypart, yin, ysend, ybuf,
                wsem, wosem, csem, gsend, grecv, dsend, drecv, dssend, dsrecv,
                ssend, srecv, tsend, trecv, ysem, bsend, brecv, fsend, frecv):
    me = lax.axis_index("sp")
    chip, core = me // 2, me % 2
    zed, low = lax.div(chip, 16), lax.rem(chip, 16)
    mate = chip * 2 + (1 - core)
    start = me * SLOTS

    def dev(index):
        return (lax.axis_index("dp"), index)

    def tile_copy(t):
        src, col = ((wk_hbm, 0), (wv_hbm, 0))[t] if t < 2 else (wq_hbm, (t - 2) * 512)
        col = pl.multiple_of(core * (512 if t < 2 else 2048) + col, 512)
        return pltpu.make_async_copy(src.at[:, pl.ds(col, 512)], wbuf.at[t], wsem.at[t])

    def kvload(i):
        rows = pl.ds(i * 16, 16)
        return (pltpu.make_async_copy(kc_hbm.at[rows], kbuf.at[rows], csem.at[0, i]),
                pltpu.make_async_copy(vc_hbm.at[rows], vbuf.at[rows], csem.at[1, i]))

    def tile_ready(t):
        tile_copy(t).wait()
        if t + DEPTH < TILES:
            tile_copy(t + DEPTH).start()
        else:
            for i in (2 * (t + DEPTH - TILES), 2 * (t + DEPTH - TILES) + 1):
                for c in kvload(i):
                    c.start()

    inputs = [pltpu.make_async_copy(a, b, isem.at[i]) for i, (a, b) in enumerate(
        [(tok_hbm, tok_ref), (an_hbm, an_ref), (pos_hbm, pos_ref), (freq_hbm, freq_ref), (kn_hbm, kn_ref), (qn_hbm, qn_ref)])]
    for c in inputs:
        c.start()
    for t in range(DEPTH):
        tile_copy(t).start()
    def each_other(send):
        for dz in (2, 1, 3, 0):
            base = lax.rem(zed + dz, 4) * 16
            for k in FAR_FIRST:
                if dz or k:
                    send(base + lax.rem(low + k, 16), (4 - dz) % 4)

    barrier = pltpu.get_barrier_semaphore()
    pl.semaphore_signal(barrier, inc=1, device_id=dev(mate), device_id_type=MESH)

    @pl.loop(1, CHIPS)
    def _(off):
        pl.semaphore_signal(barrier, inc=1, device_id=dev(lax.rem(chip + off, CHIPS) * 2 + core), device_id_type=MESH)

    for n in range(2):
        wts[:, pl.ds(n * HEADS, HEADS), pl.ds((1 - n) * HEAD_DIM, HEAD_DIM)] = jnp.zeros((SEQS // 2, HEADS, HEAD_DIM), BF16)
    for c in inputs:
        c.wait()

    tok = tok_ref[...].astype(F32)
    hid[...] = rms(tok, an_ref[...].astype(F32).reshape(1, DIM)).astype(BF16)
    row8 = iota((SEQS, HEAD_DIM), 0)
    posv = jnp.zeros((SEQS, HEAD_DIM), jnp.int32)
    for s in range(SEQS):
        posv = jnp.where(row8 == s, pos_ref[s], posv)
    angle = posv.astype(F32) * freq_ref[...]
    cosr[...] = jnp.cos(angle)
    sinr[...] = jnp.where(iota((SEQS, HEAD_DIM), 1) < HEAD_DIM // 2, -1.0, 1.0) * jnp.sin(angle)

    def project(tile):
        return jnp.dot(hid[...], wbuf[tile], preferred_element_type=F32).astype(BF16).astype(F32)

    def rope(head, gain):
        normed = rms(head, gain)
        turned = normed * cosr[...] + pltpu.roll(normed, HEAD_DIM // 2, 1) * sinr[...]
        return turned.astype(BF16).astype(F32)

    for t in range(2):
        tile_ready(t)
        res = project(t)
        for h in range(4):
            head = res[:, h * 128:(h + 1) * 128]
            gbuf[4 + core, :, 4 * t + h, :] = head if t else rope(head, kn_ref[...].astype(F32))

    def gcopy(group, slot):
        return pltpu.make_async_remote_copy(src_ref=gbuf.at[group], dst_ref=gbuf.at[group], send_sem=gsend.at[slot],
                                            recv_sem=grecv.at[slot], device_id=dev(mate), device_id_type=MESH)

    for g in range(2):
        for t2 in range(2):
            t = 2 + g * 2 + t2
            tile_ready(t)
            res = project(t)
            for h in range(4):
                gbuf[2 * core + g, :, 4 * t2 + h, :] = rope(res[:, h * 128:(h + 1) * 128], qn_ref[...].astype(F32))
        if g == 0:
            pl.semaphore_wait(barrier, CHIPS)
            gcopy(4 + core, 2).start()
        gcopy(2 * core + g, g).start()

    wocopy = pltpu.make_async_copy(wo_hbm.at[pl.ds(pl.multiple_of(core * 2048, 2048), 2048)], wobuf, wosem.at[0])
    wocopy.start()
    for slot in range(3):
        gcopy(4 + core if slot == 2 else 2 * core + slot, slot).wait()
    for i in range(4):
        for c in kvload(i):
            c.wait()

    def block_of(i):
        return lax.rem(zed + 2 + i // 2 - (i // 4) * (2 * (i // 2) - 1), 4) * 2 + lax.rem(i, 2)

    row32, col32 = iota((HEADS, HEAD_DIM), 0), iota((HEADS, HEAD_DIM), 1)
    same_head = (col32 % KV_HEADS) == (row32 // 4)
    slot_of = col32 // KV_HEADS + start
    row16, lane16 = iota((HALF, HEAD_DIM), 0), iota((HALF, HEAD_DIM), 1)

    def weigh(blk):
        acc = [[jnp.zeros((HALF, HEAD_DIM), F32) for _ in range(2)] for _ in range(2)]
        for p4 in range(4):
            pair = blk * 4 + p4
            both = pl.ds(pair * 2, 2)
            q = jnp.concatenate([gbuf[g, pair * 2 + n] for n in range(2) for g in range(4)], axis=0).astype(BF16)
            keys = kbuf[both].reshape(2 * HEAD_DIM, HEAD_DIM)
            products = lax.dot_general(q, keys, (((1,), (1,)), ((), ())), preferred_element_type=F32)
            for n in range(2):
                rows, cols = pl.ds(n * HEADS, HEADS), pl.ds(n * HEAD_DIM, HEAD_DIM)
                scores = products[n * HEADS:(n + 1) * HEADS, n * HEAD_DIM:(n + 1) * HEAD_DIM] * SCALE
                live = same_head & (slot_of < pos_ref[pair * 2 + n])
                scores = jnp.where(live, scores, NEG_FILL)
                peak = jnp.max(scores, axis=-1, keepdims=True)
                weights = jnp.where(live, jnp.exp(scores - peak), 0.0)
                total = jnp.sum(weights, axis=-1, keepdims=True)
                wts[pair, rows, cols] = weights.astype(BF16)
                here = lane16 == (p4 * 2 + n) * HALF + row16
                for half in range(2):
                    cut = slice(half * HALF, (half + 1) * HALF)
                    acc[half][0] += jnp.where(here, peak[cut], 0.0)
                    acc[half][1] += jnp.where(here, total[cut], 0.0)
        for half in range(2):
            for k in range(2):
                st[half, blk, pl.ds(k, 1), :] = jnp.sum(acc[half][k], axis=0, keepdims=True)

    def mix(i):
        blk = block_of(i)
        for p4 in range(4):
            pair = blk * 4 + p4
            values = vbuf[pl.ds(pair * 2, 2)].reshape(2 * HEAD_DIM, HEAD_DIM)
            mixed = jnp.dot(wts[pair], values, preferred_element_type=F32)
            for n in range(2):
                for half in range(2):
                    top = n * HEADS + half * HALF
                    obuf[half, pair * 2 + n] = mixed[top:top + HALF]
        ocopy(i).start()

    def ocopy(i):
        rows = pl.ds(block_of(i) * 8, 8)
        return pltpu.make_async_remote_copy(src_ref=obuf.at[1 - core, rows], dst_ref=oin.at[rows], send_sem=dsend.at[i],
                                            recv_sem=drecv.at[i], device_id=dev(mate), device_id_type=MESH)

    def merge(i):
        blk = block_of(i)
        ocopy(i).wait()
        f0, f1 = fac[0, pl.ds(blk, 1), :], fac[1, pl.ds(blk, 1), :]
        for s8 in range(8):
            s = blk * 8 + s8
            here = lane16 == s8 * HALF + row16
            osend[s] = obuf[core, s] * pick(f0, here) + oin[s] * pick(f1, here)
        group = lax.rem(zed - lax.div(blk, 2) + 4, 4)
        for s8 in range(8):
            s = blk * 8 + s8

            @pl.when(s != chip)
            def _():
                pltpu.make_async_remote_copy(src_ref=osend.at[s], dst_ref=rbuf.at[chip], send_sem=ssend.at[0], recv_sem=srecv.at[group],
                                             device_id=dev(s * 2 + core), device_id_type=MESH).start()

    @pl.loop(0, 8)
    def _(blk):
        weigh(blk)

    stcopy = pltpu.make_async_remote_copy(src_ref=st.at[1 - core], dst_ref=stin, send_sem=dssend.at[0], recv_sem=dsrecv.at[0],
                                          device_id=dev(mate), device_id_type=MESH)
    stcopy.start()

    @pl.loop(0, LAG)
    def _(i):
        mix(i)

    stcopy.wait()
    m0, l0, m1, l1 = st[core, :, 0, :], st[core, :, 1, :], stin[:, 0, :], stin[:, 1, :]
    top = jnp.maximum(m0, m1)
    f0, f1 = jnp.exp(m0 - top), jnp.exp(m1 - top)
    fac[0], fac[1] = f0, f1
    stsend[:, 0, :] = top
    stsend[:, 1, :] = l0 * f0 + l1 * f1

    def send_stats(s, _):
        pltpu.make_async_remote_copy(src_ref=stsend.at[lax.div(s, 8)], dst_ref=rst.at[chip], send_sem=tsend.at[0], recv_sem=trecv.at[0],
                                     device_id=dev(s * 2 + core), device_id_type=MESH).start()

    each_other(send_stats)

    @pl.loop(LAG, 8 + LAG)
    def _(i):
        @pl.when(i < 8)
        def _():
            mix(i)

        merge(i - LAG)

    rst[chip] = stsend[chip // 8]
    rbuf[chip] = osend[chip]

    def all_of(src, dst, send, recv):
        return pltpu.make_async_remote_copy(src_ref=src, dst_ref=dst, send_sem=send, recv_sem=recv, device_id=dev(mate),
                                            device_id_type=MESH)

    upper = iota((SEQS, 8, HEAD_DIM), 1) < 4
    new_ref[:, 0] = jnp.where(upper, gbuf[4], pltpu.roll(gbuf[5], 4, 1)).astype(BF16)
    new_ref[:, 1] = jnp.where(upper, pltpu.roll(gbuf[4], 4, 1), gbuf[5]).astype(BF16)

    slot_row = iota((128, HEAD_DIM), 0) // KV_HEADS + start

    @pl.loop(0, 16)
    def _(i):
        for s4 in range(4):
            s = i * 4 + s4
            first, second = gbuf[4, s], gbuf[5, s]
            mine = slot_row == pos_ref[s]
            k_new = jnp.where(upper[0], first, pltpu.roll(second, 4, 0))
            v_new = jnp.where(upper[0], pltpu.roll(first, 4, 0), second)
            kbuf[s] = jnp.where(mine, jnp.concatenate([k_new] * SLOTS, axis=0).astype(BF16), kbuf[s])
            vbuf[s] = jnp.where(mine, jnp.concatenate([v_new] * SLOTS, axis=0).astype(BF16), vbuf[s])

    others = pl.ds(0, CHIPS - 1)
    all_of(rst.at[others], rst.at[others], tsend.at[0], trecv.at[0]).wait_recv()
    here = lane16 == lax.rem(chip, 8) * HALF + row16
    tops = rst[:, 0, :]
    top = jnp.max(tops, axis=0, keepdims=True)
    facs = jnp.exp(tops - top)
    facbuf[...] = facs
    total = pick(jnp.sum(rst[:, 1, :] * facs, axis=0, keepdims=True), here)
    q_own = jnp.concatenate([gbuf[2 * core, chip], gbuf[2 * core + 1, chip]], axis=0)
    kv_own = gbuf[4 + core, chip]
    k_own = jnp.concatenate([jnp.broadcast_to(kv_own[i:i + 1], (4, HEAD_DIM)) for i in range(4)], axis=0)
    v_own = jnp.concatenate([jnp.broadcast_to(kv_own[4 + i:5 + i], (4, HEAD_DIM)) for i in range(4)], axis=0)
    s_own = jnp.sum(q_own * k_own, axis=-1, keepdims=True) * SCALE
    top = pick(top, here)
    peak = jnp.maximum(top, s_own)
    f_old, f_new = jnp.exp(top - peak), jnp.exp(s_own - peak)
    acc = jnp.zeros((HALF, HEAD_DIM), F32)
    for group in (0, 1, 3, 2):
        part = rbuf.at[pl.ds(0, 15 if group == 0 else 16)]
        all_of(part, part, ssend.at[0], srecv.at[group]).wait_recv()
        base = lax.rem(zed + group, 4) * 16
        for c in range(16):
            acc += rbuf[base + c] * pick(facbuf[pl.ds(base + c, 1), :], here)
    attn = (acc * f_old + v_own * f_new) / (total * f_old + f_new)
    for h in range(HALF):
        lhs[:, h * 128:(h + 1) * 128] = jnp.where(row16 == h, attn, 0.0).astype(BF16)

    wocopy.wait()

    def out_cols(half, slot):
        cols = pl.ds(pl.multiple_of(half * 1280, 1280), 1280)
        res = jnp.sum(jnp.dot(lhs[...], wobuf[:, cols], preferred_element_type=F32), axis=0, keepdims=True)
        for k in range(10):
            ypart[slot, pl.ds(k, 1), :] = res[:, k * 128:(k + 1) * 128]

    out_cols(1 - core, 0)
    ycopy = pltpu.make_async_remote_copy(src_ref=ypart.at[0], dst_ref=yin, send_sem=ysem.at[0], recv_sem=ysem.at[1],
                                         device_id=dev(mate), device_id_type=MESH)
    ycopy.start()
    out_cols(core, 1)
    ycopy.wait()
    ysend[...] = ypart[1] + yin[...]

    def bcopy(s, group):
        return pltpu.make_async_remote_copy(src_ref=ysend, dst_ref=ybuf.at[core, chip], send_sem=bsend.at[0],
                                            recv_sem=brecv.at[group], device_id=dev(s * 2 + core), device_id_type=MESH)

    each_other(lambda s, group: bcopy(s, group).start())

    ybuf[core, chip] = ysend[...]

    def slab(half, group):
        return ybuf.at[half, pl.ds(lax.rem(zed + group, 4) * 16, 16)]

    def fcopy(half, group):
        ref = slab(half, group)
        return pltpu.make_async_remote_copy(src_ref=ref, dst_ref=ref, send_sem=fsend.at[group], recv_sem=frecv.at[group],
                                            device_id=dev(mate), device_id_type=MESH)

    def finish(half, group):
        rows = pl.ds(pl.multiple_of(lax.rem(zed + group, 4) * 16, 16), 16)
        for k in range(10):
            cols = pl.ds(pl.multiple_of(half * 1280 + k * 128, 128), 128)
            out_ref[rows, cols] = (tok_ref[rows, cols].astype(F32) + ybuf[half, rows, k, :]).astype(BF16)

    for group in (0, 1, 3, 2):
        ref = ybuf.at[core, pl.ds(0, 15 if group == 0 else 16)]
        all_of(ref, ref, bsend.at[0], brecv.at[group]).wait_recv()
        fcopy(core, group).start()
        finish(core, group)
    for group in (0, 1, 3, 2):
        fcopy(1 - core, group).wait_recv()
        finish(1 - core, group)

    for group in range(4):
        fcopy(core, group).wait_send()
    all_of(rst.at[others], rst.at[others], tsend.at[0], trecv.at[0]).wait_send()
    all_of(rbuf.at[others], rbuf.at[others], ssend.at[0], srecv.at[0]).wait_send()
    rest = ybuf.at[0, others]
    all_of(rest, rest, bsend.at[0], brecv.at[0]).wait_send()


def step_call(*args):
    dma = pltpu.SemaphoreType.DMA
    vmem = pltpu.VMEM
    vm = pl.BlockSpec(memory_space=pltpu.VMEM)
    return pl.pallas_call(
        step_kernel,
        name="decode_step",
        out_shape=(jax.ShapeDtypeStruct((SEQS, DIM), BF16), jax.ShapeDtypeStruct((SEQS, 2, KV_HEADS, HEAD_DIM), BF16),
                   jax.ShapeDtypeStruct((SEQS, 128, HEAD_DIM), BF16), jax.ShapeDtypeStruct((SEQS, 128, HEAD_DIM), BF16)),
        in_specs=[pl.BlockSpec(memory_space=pltpu.HBM)] * 12,
        out_specs=(vm,) * 4,
        scratch_shapes=[
            pltpu.SMEM((SEQS,), jnp.int32), vmem((SEQS, DIM), BF16), vmem((DIM,), BF16), vmem((1, HEAD_DIM), BF16), vmem((1, HEAD_DIM), BF16), vmem((1, HEAD_DIM), F32),
            dma((6,)), vmem((CHIPS, HEAD_DIM), F32),
            vmem((SEQS, DIM), BF16), vmem((SEQS, HEAD_DIM), F32), vmem((SEQS, HEAD_DIM), F32),
            vmem((TILES, DIM, 512), BF16), vmem((2048, DIM), BF16),
            vmem((6, SEQS, 8, HEAD_DIM), F32),
            vmem((SEQS // 2, 2 * HEADS, 2 * HEAD_DIM), BF16), vmem((2, SEQS, HALF, HEAD_DIM), F32), vmem((SEQS, HALF, HEAD_DIM), F32),
            vmem((2, 8, 2, HEAD_DIM), F32), vmem((8, 2, HEAD_DIM), F32), vmem((2, 8, HEAD_DIM), F32),
            vmem((SEQS, HALF, HEAD_DIM), F32), vmem((8, 2, HEAD_DIM), F32),
            vmem((CHIPS, HALF, HEAD_DIM), F32), vmem((CHIPS, 2, HEAD_DIM), F32),
            vmem((HALF, 2048), BF16), vmem((2, 10, HEAD_DIM), F32), vmem((10, HEAD_DIM), F32), vmem((10, HEAD_DIM), F32),
            vmem((2, CHIPS, 10, HEAD_DIM), F32),
            dma((TILES,)), dma((1,)), dma((2, 4)), dma((3,)), dma((3,)), dma((8,)), dma((8,)), dma((1,)), dma((1,)),
            dma((1,)), dma((4,)), dma((1,)), dma((1,)), dma((2,)), dma((1,)), dma((4,)), dma((4,)), dma((4,)),
        ],
        compiler_params=pltpu.CompilerParams(collective_id=0, has_side_effects=True, vmem_limit_bytes=48 * 2 ** 20),
    )(*args)


def store_kernel(*refs):
    sem = refs[-1]
    count = (len(refs) - 1) // 2
    copies = [pltpu.make_async_copy(refs[i], refs[count + i], sem.at[i]) for i in range(count)]
    for c in copies:
        c.start()
    for c in copies:
        c.wait()


def store_call(*arrays):
    return pl.pallas_call(
        store_kernel,
        name="store",
        out_shape=tuple(jax.ShapeDtypeStruct(a.shape, a.dtype) for a in arrays),
        in_specs=[pl.BlockSpec(memory_space=pltpu.VMEM)] * len(arrays),
        out_specs=(pl.BlockSpec(memory_space=pl.ANY),) * len(arrays),
        scratch_shapes=[pltpu.SemaphoreType.DMA((len(arrays),))],
        compiler_params=pltpu.CompilerParams(vmem_limit_bytes=12 * 2 ** 20),
    )(*arrays)


def solution(mesh):
    cache_spec = P('dp', 'sp', None, None)

    def device_step(tokens, positions, k_cache, v_cache, w_q, w_k, w_v, w_o, attn_norm, q_norm, k_norm):
        inv = np.float32(ROPE_THETA) ** (-np.arange(HEAD_DIM // 2, dtype=np.float32) * np.float32(2.0) / np.float32(HEAD_DIM))
        freq = jnp.asarray(np.concatenate([inv, inv])[None, :].astype(np.float32))
        flat = (SEQS, SLOTS * KV_HEADS, HEAD_DIM)
        operands = (positions, tokens, attn_norm, q_norm[None, :], k_norm[None, :], freq, w_q, w_k, w_v, w_o, k_cache.reshape(flat), v_cache.reshape(flat))
        row, new, k_loc, v_loc = step_call(*[pltpu.with_memory_space_constraint(a, pltpu.HBM) for a in operands])
        k_out, v_out, new_kv, block_out = store_call(k_loc.reshape(k_cache.shape), v_loc.reshape(v_cache.shape), new, row)
        return block_out, k_out, v_out, new_kv

    return jax.shard_map(device_step, mesh=mesh, in_specs=(P('dp', None), P('dp'), cache_spec, cache_spec, P(), P(), P(), P(), P(), P(), P()), out_specs=(P('dp', None), cache_spec, cache_spec, P('dp', None, None, None)), check_vma=False)
```

```python
import functools

import jax
import jax.numpy as jnp
import numpy as np
from jax import lax
from jax.experimental import pallas as pl
from jax.experimental.pallas import tpu as pltpu
from jax.sharding import PartitionSpec as P

NORM_EPS = 1e-6
ROPE_THETA = 1000000.0
NEG_FILL = -1e30
SEQS, DIM, HEADS, KV_HEADS, HEAD_DIM, SLOTS = 64, 2560, 32, 8, 128, 16
HALF = HEADS // 2
CHIPS = 64
SCALE = HEAD_DIM ** -0.5
F32, BF16 = jnp.float32, jnp.bfloat16
MESH = pl.DeviceIdType.MESH
DEPTH = 2
TILES = 6
FAR_FIRST = sorted(range(16), key=lambda k: -(min(k // 4, 4 - k // 4) + min(k % 4, 4 - k % 4)))
LAG = 5


def rms(values, gain):
    return values * lax.rsqrt(jnp.mean(values * values, axis=-1, keepdims=True) + NORM_EPS) * gain


def iota(shape, axis):
    return lax.broadcasted_iota(jnp.int32, shape, axis)


def pick(row, lane):
    spread = jnp.broadcast_to(row, (HALF, HEAD_DIM))
    return jnp.sum(jnp.where(lane, spread, 0.0), axis=-1, keepdims=True)


def step_kernel(pos_hbm, tok_hbm, an_hbm, qn_hbm, kn_hbm, freq_hbm, wq_hbm, wk_hbm, wv_hbm, wo_hbm, kc_hbm, vc_hbm,
                out_ref, new_ref, kbuf, vbuf,
                pos_ref, tok_ref, an_ref, qn_ref, kn_ref, freq_ref, isem, facbuf, hid, cosr, sinr, wbuf, wobuf, gbuf, wts, obuf, oin, st, stin, fac, osend, stsend, rbuf, rst,
                lhs, ypart, yin, ysend, ybuf,
                wsem, wosem, csem, gsend, grecv, dsend, drecv, dssend, dsrecv,
                ssend, srecv, tsend, trecv, ysem, bsend, brecv, fsend, frecv):
    me = lax.axis_index("sp")
    chip, core = me // 2, me % 2
    zed, low = lax.div(chip, 16), lax.rem(chip, 16)
    mate = chip * 2 + (1 - core)
    start = me * SLOTS

    def dev(index):
        return (lax.axis_index("dp"), index)

    def tile_copy(t):
        src, col = (wq_hbm, t * 512) if t < 4 else ((wk_hbm, 0), (wv_hbm, 0))[t - 4]
        col = pl.multiple_of(core * (2048 if t < 4 else 512) + col, 512)
        return pltpu.make_async_copy(src.at[:, pl.ds(col, 512)], wbuf.at[t], wsem.at[t])

    def kvload(i, which):
        rows = pl.ds(i * 16, 16)
        src, dst = ((kc_hbm, kbuf), (vc_hbm, vbuf))[which]
        return pltpu.make_async_copy(src.at[rows], dst.at[rows], csem.at[which, i])

    def tile_ready(t):
        tile_copy(t).wait()
        if t + DEPTH < TILES:
            tile_copy(t + DEPTH).start()
        else:
            for i in range(4):
                kvload(i, t + DEPTH - TILES).start()

    inputs = [pltpu.make_async_copy(a, b, isem.at[i]) for i, (a, b) in enumerate(
        [(tok_hbm, tok_ref), (an_hbm, an_ref), (pos_hbm, pos_ref), (freq_hbm, freq_ref), (kn_hbm, kn_ref), (qn_hbm, qn_ref)])]
    for c in inputs:
        c.start()
    for t in range(DEPTH):
        tile_copy(t).start()
    def each_other(send):
        for dz in (2, 1, 3, 0):
            base = lax.rem(zed + dz, 4) * 16
            for k in FAR_FIRST:
                if dz or k:
                    send(base + lax.rem(low + k, 16), (4 - dz) % 4)

    barrier = pltpu.get_barrier_semaphore()
    pl.semaphore_signal(barrier, inc=1, device_id=dev(mate), device_id_type=MESH)

    @pl.loop(1, CHIPS)
    def _(off):
        pl.semaphore_signal(barrier, inc=1, device_id=dev(lax.rem(chip + off, CHIPS) * 2 + core), device_id_type=MESH)

    for n in range(2):
        wts[:, pl.ds(n * HEADS, HEADS), pl.ds((1 - n) * HEAD_DIM, HEAD_DIM)] = jnp.zeros((SEQS // 2, HEADS, HEAD_DIM), BF16)
    for c in inputs:
        c.wait()

    tok = tok_ref[...].astype(F32)
    hid[...] = rms(tok, an_ref[...].astype(F32).reshape(1, DIM)).astype(BF16)
    row8 = iota((SEQS, HEAD_DIM), 0)
    posv = jnp.zeros((SEQS, HEAD_DIM), jnp.int32)
    for s in range(SEQS):
        posv = jnp.where(row8 == s, pos_ref[s], posv)
    angle = posv.astype(F32) * freq_ref[...]
    cosr[...] = jnp.cos(angle)
    sinr[...] = jnp.where(iota((SEQS, HEAD_DIM), 1) < HEAD_DIM // 2, -1.0, 1.0) * jnp.sin(angle)

    def project(tile):
        return jnp.dot(hid[...], wbuf[tile], preferred_element_type=F32).astype(BF16).astype(F32)

    def rope(head, gain):
        normed = rms(head, gain)
        turned = normed * cosr[...] + pltpu.roll(normed, HEAD_DIM // 2, 1) * sinr[...]
        return turned.astype(BF16).astype(F32)

    def gcopy(group, slot):
        return pltpu.make_async_remote_copy(src_ref=gbuf.at[group], dst_ref=gbuf.at[group], send_sem=gsend.at[slot],
                                            recv_sem=grecv.at[slot], device_id=dev(mate), device_id_type=MESH)

    for t in range(4):
        tile_ready(t)
        res = project(t)
        for h in range(4):
            gbuf[2 * core + t // 2, :, 4 * (t % 2) + h, :] = rope(res[:, h * 128:(h + 1) * 128], qn_ref[...].astype(F32))

    pl.semaphore_wait(barrier, CHIPS)
    for g in range(2):
        gcopy(2 * core + g, g).start()
    for t in range(2):
        tile_ready(4 + t)
        res = project(4 + t)
        for h in range(4):
            head = res[:, h * 128:(h + 1) * 128]
            gbuf[4 + core, :, 4 * t + h, :] = head if t else rope(head, kn_ref[...].astype(F32))
    gcopy(4 + core, 2).start()

    wocopy = pltpu.make_async_copy(wo_hbm.at[pl.ds(pl.multiple_of(core * 2048, 2048), 2048)], wobuf, wosem.at[0])
    wocopy.start()
    for g in range(2):
        gcopy(2 * core + g, g).wait()
    for i in range(4):
        kvload(i, 0).wait()

    def block_of(i):
        return lax.rem(zed + 2 + i // 2 - (i // 4) * (2 * (i // 2) - 1), 4) * 2 + lax.rem(i, 2)

    row32, col32 = iota((HEADS, HEAD_DIM), 0), iota((HEADS, HEAD_DIM), 1)
    same_head = (col32 % KV_HEADS) == (row32 // 4)
    slot_of = col32 // KV_HEADS + start
    row16, lane16 = iota((HALF, HEAD_DIM), 0), iota((HALF, HEAD_DIM), 1)

    def weigh(blk):
        acc = [[jnp.zeros((HALF, HEAD_DIM), F32) for _ in range(2)] for _ in range(2)]
        for p4 in range(4):
            pair = blk * 4 + p4
            both = pl.ds(pair * 2, 2)
            q = jnp.concatenate([gbuf[g, pair * 2 + n] for n in range(2) for g in range(4)], axis=0).astype(BF16)
            keys = kbuf[both].reshape(2 * HEAD_DIM, HEAD_DIM)
            products = lax.dot_general(q, keys, (((1,), (1,)), ((), ())), preferred_element_type=F32)
            for n in range(2):
                rows, cols = pl.ds(n * HEADS, HEADS), pl.ds(n * HEAD_DIM, HEAD_DIM)
                scores = products[n * HEADS:(n + 1) * HEADS, n * HEAD_DIM:(n + 1) * HEAD_DIM] * SCALE
                live = same_head & (slot_of < pos_ref[pair * 2 + n])
                scores = jnp.where(live, scores, NEG_FILL)
                peak = jnp.max(scores, axis=-1, keepdims=True)
                weights = jnp.where(live, jnp.exp(scores - peak), 0.0)
                total = jnp.sum(weights, axis=-1, keepdims=True)
                wts[pair, rows, cols] = weights.astype(BF16)
                here = lane16 == (p4 * 2 + n) * HALF + row16
                for half in range(2):
                    cut = slice(half * HALF, (half + 1) * HALF)
                    acc[half][0] += jnp.where(here, peak[cut], 0.0)
                    acc[half][1] += jnp.where(here, total[cut], 0.0)
        for half in range(2):
            for k in range(2):
                st[half, blk, pl.ds(k, 1), :] = jnp.sum(acc[half][k], axis=0, keepdims=True)

    def mix(i):
        blk = block_of(i)
        for p4 in range(4):
            pair = blk * 4 + p4
            values = vbuf[pl.ds(pair * 2, 2)].reshape(2 * HEAD_DIM, HEAD_DIM)
            mixed = jnp.dot(wts[pair], values, preferred_element_type=F32)
            for n in range(2):
                for half in range(2):
                    top = n * HEADS + half * HALF
                    obuf[half, pair * 2 + n] = mixed[top:top + HALF]
        ocopy(i).start()

    def ocopy(i):
        rows = pl.ds(block_of(i) * 8, 8)
        return pltpu.make_async_remote_copy(src_ref=obuf.at[1 - core, rows], dst_ref=oin.at[rows], send_sem=dsend.at[i],
                                            recv_sem=drecv.at[i], device_id=dev(mate), device_id_type=MESH)

    def merge(i):
        blk = block_of(i)
        ocopy(i).wait()
        f0, f1 = fac[0, pl.ds(blk, 1), :], fac[1, pl.ds(blk, 1), :]
        for s8 in range(8):
            s = blk * 8 + s8
            here = lane16 == s8 * HALF + row16
            osend[s] = obuf[core, s] * pick(f0, here) + oin[s] * pick(f1, here)
        group = lax.rem(zed - lax.div(blk, 2) + 4, 4)
        for s8 in range(8):
            s = blk * 8 + s8

            @pl.when(s != chip)
            def _():
                pltpu.make_async_remote_copy(src_ref=osend.at[s], dst_ref=rbuf.at[chip], send_sem=ssend.at[0], recv_sem=srecv.at[group],
                                             device_id=dev(s * 2 + core), device_id_type=MESH).start()

    @pl.loop(0, 8)
    def _(blk):
        weigh(blk)

    stcopy = pltpu.make_async_remote_copy(src_ref=st.at[1 - core], dst_ref=stin, send_sem=dssend.at[0], recv_sem=dsrecv.at[0],
                                          device_id=dev(mate), device_id_type=MESH)
    stcopy.start()

    for i in range(4):
        kvload(i, 1).wait()

    @pl.loop(0, LAG)
    def _(i):
        mix(i)

    stcopy.wait()
    m0, l0, m1, l1 = st[core, :, 0, :], st[core, :, 1, :], stin[:, 0, :], stin[:, 1, :]
    top = jnp.maximum(m0, m1)
    f0, f1 = jnp.exp(m0 - top), jnp.exp(m1 - top)
    fac[0], fac[1] = f0, f1
    stsend[:, 0, :] = top
    stsend[:, 1, :] = l0 * f0 + l1 * f1

    def send_stats(s, _):
        pltpu.make_async_remote_copy(src_ref=stsend.at[lax.div(s, 8)], dst_ref=rst.at[chip], send_sem=tsend.at[0], recv_sem=trecv.at[0],
                                     device_id=dev(s * 2 + core), device_id_type=MESH).start()

    each_other(send_stats)

    @pl.loop(LAG, 8 + LAG)
    def _(i):
        @pl.when(i < 8)
        def _():
            mix(i)

        merge(i - LAG)

    rst[chip] = stsend[chip // 8]
    rbuf[chip] = osend[chip]

    def all_of(src, dst, send, recv):
        return pltpu.make_async_remote_copy(src_ref=src, dst_ref=dst, send_sem=send, recv_sem=recv, device_id=dev(mate),
                                            device_id_type=MESH)

    gcopy(4 + core, 2).wait()
    upper = iota((SEQS, 8, HEAD_DIM), 1) < 4
    new_ref[:, 0] = jnp.where(upper, gbuf[4], pltpu.roll(gbuf[5], 4, 1)).astype(BF16)
    new_ref[:, 1] = jnp.where(upper, pltpu.roll(gbuf[4], 4, 1), gbuf[5]).astype(BF16)

    slot_row = iota((128, HEAD_DIM), 0) // KV_HEADS + start

    @pl.loop(0, 16)
    def _(i):
        for s4 in range(4):
            s = i * 4 + s4
            first, second = gbuf[4, s], gbuf[5, s]
            mine = slot_row == pos_ref[s]
            k_new = jnp.where(upper[0], first, pltpu.roll(second, 4, 0))
            v_new = jnp.where(upper[0], pltpu.roll(first, 4, 0), second)
            kbuf[s] = jnp.where(mine, jnp.concatenate([k_new] * SLOTS, axis=0).astype(BF16), kbuf[s])
            vbuf[s] = jnp.where(mine, jnp.concatenate([v_new] * SLOTS, axis=0).astype(BF16), vbuf[s])

    others = pl.ds(0, CHIPS - 1)
    all_of(rst.at[others], rst.at[others], tsend.at[0], trecv.at[0]).wait_recv()
    here = lane16 == lax.rem(chip, 8) * HALF + row16
    tops = rst[:, 0, :]
    top = jnp.max(tops, axis=0, keepdims=True)
    facs = jnp.exp(tops - top)
    facbuf[...] = facs
    total = pick(jnp.sum(rst[:, 1, :] * facs, axis=0, keepdims=True), here)
    q_own = jnp.concatenate([gbuf[2 * core, chip], gbuf[2 * core + 1, chip]], axis=0)
    kv_own = gbuf[4 + core, chip]
    k_own = jnp.concatenate([jnp.broadcast_to(kv_own[i:i + 1], (4, HEAD_DIM)) for i in range(4)], axis=0)
    v_own = jnp.concatenate([jnp.broadcast_to(kv_own[4 + i:5 + i], (4, HEAD_DIM)) for i in range(4)], axis=0)
    s_own = jnp.sum(q_own * k_own, axis=-1, keepdims=True) * SCALE
    top = pick(top, here)
    peak = jnp.maximum(top, s_own)
    f_old, f_new = jnp.exp(top - peak), jnp.exp(s_own - peak)
    acc = jnp.zeros((HALF, HEAD_DIM), F32)
    for group in (0, 1, 3, 2):
        part = rbuf.at[pl.ds(0, 15 if group == 0 else 16)]
        all_of(part, part, ssend.at[0], srecv.at[group]).wait_recv()
        base = lax.rem(zed + group, 4) * 16
        for c in range(16):
            acc += rbuf[base + c] * pick(facbuf[pl.ds(base + c, 1), :], here)
    attn = (acc * f_old + v_own * f_new) / (total * f_old + f_new)
    for h in range(HALF):
        lhs[:, h * 128:(h + 1) * 128] = jnp.where(row16 == h, attn, 0.0).astype(BF16)

    wocopy.wait()

    def out_cols(half, slot):
        cols = pl.ds(pl.multiple_of(half * 1280, 1280), 1280)
        res = jnp.sum(jnp.dot(lhs[...], wobuf[:, cols], preferred_element_type=F32), axis=0, keepdims=True)
        for k in range(10):
            ypart[slot, pl.ds(k, 1), :] = res[:, k * 128:(k + 1) * 128]

    out_cols(1 - core, 0)
    ycopy = pltpu.make_async_remote_copy(src_ref=ypart.at[0], dst_ref=yin, send_sem=ysem.at[0], recv_sem=ysem.at[1],
                                         device_id=dev(mate), device_id_type=MESH)
    ycopy.start()
    out_cols(core, 1)
    ycopy.wait()
    ysend[...] = ypart[1] + yin[...]

    def bcopy(s, group):
        return pltpu.make_async_remote_copy(src_ref=ysend, dst_ref=ybuf.at[core, chip], send_sem=bsend.at[0],
                                            recv_sem=brecv.at[group], device_id=dev(s * 2 + core), device_id_type=MESH)

    each_other(lambda s, group: bcopy(s, group).start())

    ybuf[core, chip] = ysend[...]

    def slab(half, group):
        return ybuf.at[half, pl.ds(lax.rem(zed + group, 4) * 16, 16)]

    def fcopy(half, group):
        ref = slab(half, group)
        return pltpu.make_async_remote_copy(src_ref=ref, dst_ref=ref, send_sem=fsend.at[group], recv_sem=frecv.at[group],
                                            device_id=dev(mate), device_id_type=MESH)

    def finish(half, group):
        rows = pl.ds(pl.multiple_of(lax.rem(zed + group, 4) * 16, 16), 16)
        for k in range(10):
            cols = pl.ds(pl.multiple_of(half * 1280 + k * 128, 128), 128)
            out_ref[rows, cols] = (tok_ref[rows, cols].astype(F32) + ybuf[half, rows, k, :]).astype(BF16)

    for group in (0, 1, 3, 2):
        ref = ybuf.at[core, pl.ds(0, 15 if group == 0 else 16)]
        all_of(ref, ref, bsend.at[0], brecv.at[group]).wait_recv()
        fcopy(core, group).start()
        finish(core, group)
    for group in (0, 1, 3, 2):
        fcopy(1 - core, group).wait_recv()
        finish(1 - core, group)

    for group in range(4):
        fcopy(core, group).wait_send()
    all_of(rst.at[others], rst.at[others], tsend.at[0], trecv.at[0]).wait_send()
    all_of(rbuf.at[others], rbuf.at[others], ssend.at[0], srecv.at[0]).wait_send()
    rest = ybuf.at[0, others]
    all_of(rest, rest, bsend.at[0], brecv.at[0]).wait_send()


def step_call(*args):
    dma = pltpu.SemaphoreType.DMA
    vmem = pltpu.VMEM
    vm = pl.BlockSpec(memory_space=pltpu.VMEM)
    return pl.pallas_call(
        step_kernel,
        name="decode_step",
        out_shape=(jax.ShapeDtypeStruct((SEQS, DIM), BF16), jax.ShapeDtypeStruct((SEQS, 2, KV_HEADS, HEAD_DIM), BF16),
                   jax.ShapeDtypeStruct((SEQS, 128, HEAD_DIM), BF16), jax.ShapeDtypeStruct((SEQS, 128, HEAD_DIM), BF16)),
        in_specs=[pl.BlockSpec(memory_space=pltpu.HBM)] * 12,
        out_specs=(vm,) * 4,
        scratch_shapes=[
            pltpu.SMEM((SEQS,), jnp.int32), vmem((SEQS, DIM), BF16), vmem((DIM,), BF16), vmem((1, HEAD_DIM), BF16), vmem((1, HEAD_DIM), BF16), vmem((1, HEAD_DIM), F32),
            dma((6,)), vmem((CHIPS, HEAD_DIM), F32),
            vmem((SEQS, DIM), BF16), vmem((SEQS, HEAD_DIM), F32), vmem((SEQS, HEAD_DIM), F32),
            vmem((TILES, DIM, 512), BF16), vmem((2048, DIM), BF16),
            vmem((6, SEQS, 8, HEAD_DIM), F32),
            vmem((SEQS // 2, 2 * HEADS, 2 * HEAD_DIM), BF16), vmem((2, SEQS, HALF, HEAD_DIM), F32), vmem((SEQS, HALF, HEAD_DIM), F32),
            vmem((2, 8, 2, HEAD_DIM), F32), vmem((8, 2, HEAD_DIM), F32), vmem((2, 8, HEAD_DIM), F32),
            vmem((SEQS, HALF, HEAD_DIM), F32), vmem((8, 2, HEAD_DIM), F32),
            vmem((CHIPS, HALF, HEAD_DIM), F32), vmem((CHIPS, 2, HEAD_DIM), F32),
            vmem((HALF, 2048), BF16), vmem((2, 10, HEAD_DIM), F32), vmem((10, HEAD_DIM), F32), vmem((10, HEAD_DIM), F32),
            vmem((2, CHIPS, 10, HEAD_DIM), F32),
            dma((TILES,)), dma((1,)), dma((2, 4)), dma((3,)), dma((3,)), dma((8,)), dma((8,)), dma((1,)), dma((1,)),
            dma((1,)), dma((4,)), dma((1,)), dma((1,)), dma((2,)), dma((1,)), dma((4,)), dma((4,)), dma((4,)),
        ],
        compiler_params=pltpu.CompilerParams(collective_id=0, has_side_effects=True, vmem_limit_bytes=48 * 2 ** 20),
    )(*args)


def store_kernel(*refs):
    sem = refs[-1]
    count = (len(refs) - 1) // 2
    copies = [pltpu.make_async_copy(refs[i], refs[count + i], sem.at[i]) for i in range(count)]
    for c in copies:
        c.start()
    for c in copies:
        c.wait()


def store_call(*arrays):
    return pl.pallas_call(
        store_kernel,
        name="store",
        out_shape=tuple(jax.ShapeDtypeStruct(a.shape, a.dtype) for a in arrays),
        in_specs=[pl.BlockSpec(memory_space=pltpu.VMEM)] * len(arrays),
        out_specs=(pl.BlockSpec(memory_space=pl.ANY),) * len(arrays),
        scratch_shapes=[pltpu.SemaphoreType.DMA((len(arrays),))],
        compiler_params=pltpu.CompilerParams(vmem_limit_bytes=12 * 2 ** 20),
    )(*arrays)


def solution(mesh):
    cache_spec = P('dp', 'sp', None, None)

    def device_step(tokens, positions, k_cache, v_cache, w_q, w_k, w_v, w_o, attn_norm, q_norm, k_norm):
        inv = np.float32(ROPE_THETA) ** (-np.arange(HEAD_DIM // 2, dtype=np.float32) * np.float32(2.0) / np.float32(HEAD_DIM))
        freq = jnp.asarray(np.concatenate([inv, inv])[None, :].astype(np.float32))
        flat = (SEQS, SLOTS * KV_HEADS, HEAD_DIM)
        operands = (positions, tokens, attn_norm, q_norm[None, :], k_norm[None, :], freq, w_q, w_k, w_v, w_o, k_cache.reshape(flat), v_cache.reshape(flat))
        row, new, k_loc, v_loc = step_call(*[pltpu.with_memory_space_constraint(a, pltpu.HBM) for a in operands])
        k_out, v_out, new_kv, block_out = store_call(k_loc.reshape(k_cache.shape), v_loc.reshape(v_cache.shape), new, row)
        return block_out, k_out, v_out, new_kv

    return jax.shard_map(device_step, mesh=mesh, in_specs=(P('dp', None), P('dp'), cache_spec, cache_spec, P(), P(), P(), P(), P(), P(), P()), out_specs=(P('dp', None), cache_spec, cache_spec, P('dp', None, None, None)), check_vma=False)
```

```python
import functools

import jax
import jax.numpy as jnp
import numpy as np
from jax import lax
from jax.experimental import pallas as pl
from jax.experimental.pallas import tpu as pltpu
from jax.sharding import PartitionSpec as P

NORM_EPS = 1e-6
ROPE_THETA = 1000000.0
NEG_FILL = -1e30
SEQS, DIM, HEADS, KV_HEADS, HEAD_DIM, SLOTS = 64, 2560, 32, 8, 128, 16
HALF = HEADS // 2
CHIPS = 64
SCALE = HEAD_DIM ** -0.5
F32, BF16 = jnp.float32, jnp.bfloat16
MESH = pl.DeviceIdType.MESH
DEPTH = 2
TILES = 6
FAR_FIRST = sorted(range(16), key=lambda k: -(min(k // 4, 4 - k // 4) + min(k % 4, 4 - k % 4)))
LAG = 5


def rms(values, gain):
    return values * lax.rsqrt(jnp.mean(values * values, axis=-1, keepdims=True) + NORM_EPS) * gain


def iota(shape, axis):
    return lax.broadcasted_iota(jnp.int32, shape, axis)


def pick(row, lane):
    spread = jnp.broadcast_to(row, (HALF, HEAD_DIM))
    return jnp.sum(jnp.where(lane, spread, 0.0), axis=-1, keepdims=True)


def step_kernel(pos_hbm, tok_hbm, an_hbm, qn_hbm, kn_hbm, freq_hbm, wq_hbm, wk_hbm, wv_hbm, wo_hbm, kc_hbm, vc_hbm,
                out_ref, new_ref, kbuf, vbuf,
                pos_ref, tok_ref, an_ref, qn_ref, kn_ref, freq_ref, isem, facbuf, hid, cosr, sinr, wbuf, wobuf, gbuf, wts, obuf, oin, st, stin, fac, osend, stsend, rbuf, rst,
                lhs, ypart, yin, ysend, ybuf,
                wsem, wosem, csem, gsend, grecv, dsend, drecv, dssend, dsrecv,
                ssend, srecv, tsend, trecv, ysem, bsend, brecv, fsend, frecv):
    me = lax.axis_index("sp")
    chip, core = me // 2, me % 2
    zed, low = lax.div(chip, 16), lax.rem(chip, 16)
    mate = chip * 2 + (1 - core)
    start = me * SLOTS

    def dev(index):
        return (lax.axis_index("dp"), index)

    def tile_copy(t):
        src, col = (wq_hbm, t * 512) if t < 4 else ((wk_hbm, 0), (wv_hbm, 0))[t - 4]
        col = pl.multiple_of(core * (2048 if t < 4 else 512) + col, 512)
        return pltpu.make_async_copy(src.at[:, pl.ds(col, 512)], wbuf.at[t], wsem.at[t])

    def kvload(i, which):
        rows = pl.ds(i * 16, 16)
        src, dst = ((kc_hbm, kbuf), (vc_hbm, vbuf))[which]
        return pltpu.make_async_copy(src.at[rows], dst.at[rows], csem.at[which, i])

    def tile_ready(t):
        tile_copy(t).wait()
        if t + DEPTH < TILES:
            tile_copy(t + DEPTH).start()
        else:
            for i in range(4):
                kvload(i, t + DEPTH - TILES).start()

    inputs = [pltpu.make_async_copy(a, b, isem.at[i]) for i, (a, b) in enumerate(
        [(tok_hbm, tok_ref), (an_hbm, an_ref), (pos_hbm, pos_ref), (freq_hbm, freq_ref), (kn_hbm, kn_ref), (qn_hbm, qn_ref)])]
    for c in inputs:
        c.start()
    for t in range(DEPTH):
        tile_copy(t).start()
    def each_other(send):
        for dz in (2, 1, 3, 0):
            base = lax.rem(zed + dz, 4) * 16
            for k in FAR_FIRST:
                if dz or k:
                    send(base + lax.rem(low + k, 16), (4 - dz) % 4)

    barrier = pltpu.get_barrier_semaphore()
    pl.semaphore_signal(barrier, inc=1, device_id=dev(mate), device_id_type=MESH)

    @pl.loop(1, CHIPS)
    def _(off):
        pl.semaphore_signal(barrier, inc=1, device_id=dev(lax.rem(chip + off, CHIPS) * 2 + core), device_id_type=MESH)

    for n in range(2):
        wts[:, pl.ds(n * HEADS, HEADS), pl.ds((1 - n) * HEAD_DIM, HEAD_DIM)] = jnp.zeros((SEQS // 2, HEADS, HEAD_DIM), BF16)
    for c in inputs:
        c.wait()

    tok = tok_ref[...].astype(F32)
    hid[...] = rms(tok, an_ref[...].astype(F32).reshape(1, DIM)).astype(BF16)
    row8 = iota((SEQS, HEAD_DIM), 0)
    posv = jnp.zeros((SEQS, HEAD_DIM), jnp.int32)
    for s in range(SEQS):
        posv = jnp.where(row8 == s, pos_ref[s], posv)
    angle = posv.astype(F32) * freq_ref[...]
    cosr[...] = jnp.cos(angle)
    sinr[...] = jnp.where(iota((SEQS, HEAD_DIM), 1) < HEAD_DIM // 2, -1.0, 1.0) * jnp.sin(angle)

    def project(tile):
        return jnp.dot(hid[...], wbuf[tile], preferred_element_type=F32).astype(BF16).astype(F32)

    def rope(head, gain):
        normed = rms(head, gain)
        turned = normed * cosr[...] + pltpu.roll(normed, HEAD_DIM // 2, 1) * sinr[...]
        return turned.astype(BF16).astype(F32)

    def gcopy(group, slot):
        return pltpu.make_async_remote_copy(src_ref=gbuf.at[group], dst_ref=gbuf.at[group], send_sem=gsend.at[slot],
                                            recv_sem=grecv.at[slot], device_id=dev(mate), device_id_type=MESH)

    for t in range(4):
        tile_ready(t)
        res = project(t)
        for h in range(4):
            gbuf[2 * core + t // 2, :, 4 * (t % 2) + h, :] = rope(res[:, h * 128:(h + 1) * 128], qn_ref[...].astype(F32))

    pl.semaphore_wait(barrier, CHIPS)
    for g in range(2):
        gcopy(2 * core + g, g).start()
    for t in range(2):
        tile_ready(4 + t)
        res = project(4 + t)
        for h in range(4):
            head = res[:, h * 128:(h + 1) * 128]
            gbuf[4 + core, :, 4 * t + h, :] = head if t else rope(head, kn_ref[...].astype(F32))
    gcopy(4 + core, 2).start()

    wocopy = pltpu.make_async_copy(wo_hbm.at[pl.ds(pl.multiple_of(core * 2048, 2048), 2048)], wobuf, wosem.at[0])
    wocopy.start()
    for g in range(2):
        gcopy(2 * core + g, g).wait()
    for i in range(4):
        kvload(i, 0).wait()

    def block_of(i):
        return lax.rem(zed + 2 + i // 2 - (i // 4) * (2 * (i // 2) - 1), 4) * 2 + lax.rem(i, 2)

    row32, col32 = iota((HEADS, HEAD_DIM), 0), iota((HEADS, HEAD_DIM), 1)
    same_head = (col32 % KV_HEADS) == (row32 // 4)
    slot_of = col32 // KV_HEADS + start
    row16, lane16 = iota((HALF, HEAD_DIM), 0), iota((HALF, HEAD_DIM), 1)

    def weigh(blk):
        acc = [[jnp.zeros((HALF, HEAD_DIM), F32) for _ in range(2)] for _ in range(2)]
        for p4 in range(4):
            pair = blk * 4 + p4
            both = pl.ds(pair * 2, 2)
            q = jnp.concatenate([gbuf[g, pair * 2 + n] for n in range(2) for g in range(4)], axis=0).astype(BF16)
            keys = kbuf[both].reshape(2 * HEAD_DIM, HEAD_DIM)
            products = lax.dot_general(q, keys, (((1,), (1,)), ((), ())), preferred_element_type=F32)
            for n in range(2):
                rows, cols = pl.ds(n * HEADS, HEADS), pl.ds(n * HEAD_DIM, HEAD_DIM)
                scores = products[n * HEADS:(n + 1) * HEADS, n * HEAD_DIM:(n + 1) * HEAD_DIM] * SCALE
                live = same_head & (slot_of < pos_ref[pair * 2 + n])
                scores = jnp.where(live, scores, NEG_FILL)
                peak = jnp.max(scores, axis=-1, keepdims=True)
                weights = jnp.where(live, jnp.exp(scores - peak), 0.0)
                total = jnp.sum(weights, axis=-1, keepdims=True)
                wts[pair, rows, cols] = weights.astype(BF16)
                here = lane16 == (p4 * 2 + n) * HALF + row16
                for half in range(2):
                    cut = slice(half * HALF, (half + 1) * HALF)
                    acc[half][0] += jnp.where(here, peak[cut], 0.0)
                    acc[half][1] += jnp.where(here, total[cut], 0.0)
        for half in range(2):
            for k in range(2):
                st[half, blk, pl.ds(k, 1), :] = jnp.sum(acc[half][k], axis=0, keepdims=True)

    def mix(i):
        blk = block_of(i)
        for p4 in range(4):
            pair = blk * 4 + p4
            values = vbuf[pl.ds(pair * 2, 2)].reshape(2 * HEAD_DIM, HEAD_DIM)
            mixed = jnp.dot(wts[pair], values, preferred_element_type=F32)
            for n in range(2):
                for half in range(2):
                    top = n * HEADS + half * HALF
                    obuf[half, pair * 2 + n] = mixed[top:top + HALF]
        ocopy(i).start()

    def ocopy(i):
        rows = pl.ds(block_of(i) * 8, 8)
        return pltpu.make_async_remote_copy(src_ref=obuf.at[1 - core, rows], dst_ref=oin.at[rows], send_sem=dsend.at[i],
                                            recv_sem=drecv.at[i], device_id=dev(mate), device_id_type=MESH)

    def merge(i):
        blk = block_of(i)
        ocopy(i).wait()
        f0, f1 = fac[0, pl.ds(blk, 1), :], fac[1, pl.ds(blk, 1), :]
        for s8 in range(8):
            s = blk * 8 + s8
            here = lane16 == s8 * HALF + row16
            osend[s] = obuf[core, s] * pick(f0, here) + oin[s] * pick(f1, here)
        group = lax.rem(zed - lax.div(blk, 2) + 4, 4)
        for s8 in range(8):
            s = blk * 8 + s8

            @pl.when(s != chip)
            def _():
                pltpu.make_async_remote_copy(src_ref=osend.at[s], dst_ref=rbuf.at[chip], send_sem=ssend.at[0], recv_sem=srecv.at[group],
                                             device_id=dev(s * 2 + core), device_id_type=MESH).start()

    @pl.loop(0, 8)
    def _(blk):
        weigh(blk)

    stcopy = pltpu.make_async_remote_copy(src_ref=st.at[1 - core], dst_ref=stin, send_sem=dssend.at[0], recv_sem=dsrecv.at[0],
                                          device_id=dev(mate), device_id_type=MESH)
    stcopy.start()

    for i in range(4):
        kvload(i, 1).wait()

    @pl.loop(0, LAG)
    def _(i):
        mix(i)

    stcopy.wait()
    m0, l0, m1, l1 = st[core, :, 0, :], st[core, :, 1, :], stin[:, 0, :], stin[:, 1, :]
    top = jnp.maximum(m0, m1)
    f0, f1 = jnp.exp(m0 - top), jnp.exp(m1 - top)
    fac[0], fac[1] = f0, f1
    stsend[:, 0, :] = top
    stsend[:, 1, :] = l0 * f0 + l1 * f1

    def send_stats(s, _):
        pltpu.make_async_remote_copy(src_ref=stsend.at[lax.div(s, 8)], dst_ref=rst.at[chip], send_sem=tsend.at[0], recv_sem=trecv.at[0],
                                     device_id=dev(s * 2 + core), device_id_type=MESH).start()

    def mix_and_merge(first, last):
        @pl.loop(first, last)
        def _(i):
            @pl.when(i < 8)
            def _():
                mix(i)

            merge(i - LAG)

    mix_and_merge(LAG, LAG + 2)
    each_other(send_stats)
    mix_and_merge(LAG + 2, LAG + 8)
    rst[chip] = stsend[chip // 8]
    rbuf[chip] = osend[chip]

    def all_of(src, dst, send, recv):
        return pltpu.make_async_remote_copy(src_ref=src, dst_ref=dst, send_sem=send, recv_sem=recv, device_id=dev(mate),
                                            device_id_type=MESH)

    gcopy(4 + core, 2).wait()
    upper = iota((SEQS, 8, HEAD_DIM), 1) < 4
    new_ref[:, 0] = jnp.where(upper, gbuf[4], pltpu.roll(gbuf[5], 4, 1)).astype(BF16)
    new_ref[:, 1] = jnp.where(upper, pltpu.roll(gbuf[4], 4, 1), gbuf[5]).astype(BF16)

    slot_row = iota((128, HEAD_DIM), 0) // KV_HEADS + start

    @pl.loop(0, 16)
    def _(i):
        for s4 in range(4):
            s = i * 4 + s4
            first, second = gbuf[4, s], gbuf[5, s]
            mine = slot_row == pos_ref[s]
            k_new = jnp.where(upper[0], first, pltpu.roll(second, 4, 0))
            v_new = jnp.where(upper[0], pltpu.roll(first, 4, 0), second)
            kbuf[s] = jnp.where(mine, jnp.concatenate([k_new] * SLOTS, axis=0).astype(BF16), kbuf[s])
            vbuf[s] = jnp.where(mine, jnp.concatenate([v_new] * SLOTS, axis=0).astype(BF16), vbuf[s])

    others = pl.ds(0, CHIPS - 1)
    all_of(rst.at[others], rst.at[others], tsend.at[0], trecv.at[0]).wait_recv()
    here = lane16 == lax.rem(chip, 8) * HALF + row16
    tops = rst[:, 0, :]
    top = jnp.max(tops, axis=0, keepdims=True)
    facs = jnp.exp(tops - top)
    facbuf[...] = facs
    total = pick(jnp.sum(rst[:, 1, :] * facs, axis=0, keepdims=True), here)
    q_own = jnp.concatenate([gbuf[2 * core, chip], gbuf[2 * core + 1, chip]], axis=0)
    kv_own = gbuf[4 + core, chip]
    k_own = jnp.concatenate([jnp.broadcast_to(kv_own[i:i + 1], (4, HEAD_DIM)) for i in range(4)], axis=0)
    v_own = jnp.concatenate([jnp.broadcast_to(kv_own[4 + i:5 + i], (4, HEAD_DIM)) for i in range(4)], axis=0)
    s_own = jnp.sum(q_own * k_own, axis=-1, keepdims=True) * SCALE
    top = pick(top, here)
    peak = jnp.maximum(top, s_own)
    f_old, f_new = jnp.exp(top - peak), jnp.exp(s_own - peak)
    acc = jnp.zeros((HALF, HEAD_DIM), F32)
    for group in (0, 1, 3, 2):
        part = rbuf.at[pl.ds(0, 15 if group == 0 else 16)]
        all_of(part, part, ssend.at[0], srecv.at[group]).wait_recv()
        base = lax.rem(zed + group, 4) * 16
        for c in range(16):
            acc += rbuf[base + c] * pick(facbuf[pl.ds(base + c, 1), :], here)
    attn = (acc * f_old + v_own * f_new) / (total * f_old + f_new)
    for h in range(HALF):
        lhs[:, h * 128:(h + 1) * 128] = jnp.where(row16 == h, attn, 0.0).astype(BF16)

    wocopy.wait()

    def out_cols(half, slot):
        cols = pl.ds(pl.multiple_of(half * 1280, 1280), 1280)
        res = jnp.sum(jnp.dot(lhs[...], wobuf[:, cols], preferred_element_type=F32), axis=0, keepdims=True)
        for k in range(10):
            ypart[slot, pl.ds(k, 1), :] = res[:, k * 128:(k + 1) * 128]

    out_cols(1 - core, 0)
    ycopy = pltpu.make_async_remote_copy(src_ref=ypart.at[0], dst_ref=yin, send_sem=ysem.at[0], recv_sem=ysem.at[1],
                                         device_id=dev(mate), device_id_type=MESH)
    ycopy.start()
    out_cols(core, 1)
    ycopy.wait()
    ysend[...] = ypart[1] + yin[...]

    def bcopy(s, group):
        return pltpu.make_async_remote_copy(src_ref=ysend, dst_ref=ybuf.at[core, chip], send_sem=bsend.at[0],
                                            recv_sem=brecv.at[group], device_id=dev(s * 2 + core), device_id_type=MESH)

    each_other(lambda s, group: bcopy(s, group).start())

    ybuf[core, chip] = ysend[...]

    def slab(half, group):
        return ybuf.at[half, pl.ds(lax.rem(zed + group, 4) * 16, 16)]

    def fcopy(half, group):
        ref = slab(half, group)
        return pltpu.make_async_remote_copy(src_ref=ref, dst_ref=ref, send_sem=fsend.at[group], recv_sem=frecv.at[group],
                                            device_id=dev(mate), device_id_type=MESH)

    def finish(half, group):
        rows = pl.ds(pl.multiple_of(lax.rem(zed + group, 4) * 16, 16), 16)
        for k in range(10):
            cols = pl.ds(pl.multiple_of(half * 1280 + k * 128, 128), 128)
            out_ref[rows, cols] = (tok_ref[rows, cols].astype(F32) + ybuf[half, rows, k, :]).astype(BF16)

    for group in (0, 1, 3, 2):
        ref = ybuf.at[core, pl.ds(0, 15 if group == 0 else 16)]
        all_of(ref, ref, bsend.at[0], brecv.at[group]).wait_recv()
        fcopy(core, group).start()
        finish(core, group)
    for group in (0, 1, 3, 2):
        fcopy(1 - core, group).wait_recv()
        finish(1 - core, group)

    for group in range(4):
        fcopy(core, group).wait_send()
    all_of(rst.at[others], rst.at[others], tsend.at[0], trecv.at[0]).wait_send()
    all_of(rbuf.at[others], rbuf.at[others], ssend.at[0], srecv.at[0]).wait_send()
    rest = ybuf.at[0, others]
    all_of(rest, rest, bsend.at[0], brecv.at[0]).wait_send()


def step_call(*args):
    dma = pltpu.SemaphoreType.DMA
    vmem = pltpu.VMEM
    vm = pl.BlockSpec(memory_space=pltpu.VMEM)
    return pl.pallas_call(
        step_kernel,
        name="decode_step",
        out_shape=(jax.ShapeDtypeStruct((SEQS, DIM), BF16), jax.ShapeDtypeStruct((SEQS, 2, KV_HEADS, HEAD_DIM), BF16),
                   jax.ShapeDtypeStruct((SEQS, 128, HEAD_DIM), BF16), jax.ShapeDtypeStruct((SEQS, 128, HEAD_DIM), BF16)),
        in_specs=[pl.BlockSpec(memory_space=pltpu.HBM)] * 12,
        out_specs=(vm,) * 4,
        scratch_shapes=[
            pltpu.SMEM((SEQS,), jnp.int32), vmem((SEQS, DIM), BF16), vmem((DIM,), BF16), vmem((1, HEAD_DIM), BF16), vmem((1, HEAD_DIM), BF16), vmem((1, HEAD_DIM), F32),
            dma((6,)), vmem((CHIPS, HEAD_DIM), F32),
            vmem((SEQS, DIM), BF16), vmem((SEQS, HEAD_DIM), F32), vmem((SEQS, HEAD_DIM), F32),
            vmem((TILES, DIM, 512), BF16), vmem((2048, DIM), BF16),
            vmem((6, SEQS, 8, HEAD_DIM), F32),
            vmem((SEQS // 2, 2 * HEADS, 2 * HEAD_DIM), BF16), vmem((2, SEQS, HALF, HEAD_DIM), F32), vmem((SEQS, HALF, HEAD_DIM), F32),
            vmem((2, 8, 2, HEAD_DIM), F32), vmem((8, 2, HEAD_DIM), F32), vmem((2, 8, HEAD_DIM), F32),
            vmem((SEQS, HALF, HEAD_DIM), F32), vmem((8, 2, HEAD_DIM), F32),
            vmem((CHIPS, HALF, HEAD_DIM), F32), vmem((CHIPS, 2, HEAD_DIM), F32),
            vmem((HALF, 2048), BF16), vmem((2, 10, HEAD_DIM), F32), vmem((10, HEAD_DIM), F32), vmem((10, HEAD_DIM), F32),
            vmem((2, CHIPS, 10, HEAD_DIM), F32),
            dma((TILES,)), dma((1,)), dma((2, 4)), dma((3,)), dma((3,)), dma((8,)), dma((8,)), dma((1,)), dma((1,)),
            dma((1,)), dma((4,)), dma((1,)), dma((1,)), dma((2,)), dma((1,)), dma((4,)), dma((4,)), dma((4,)),
        ],
        compiler_params=pltpu.CompilerParams(collective_id=0, has_side_effects=True, vmem_limit_bytes=48 * 2 ** 20),
    )(*args)


def store_kernel(*refs):
    sem = refs[-1]
    count = (len(refs) - 1) // 2
    copies = [pltpu.make_async_copy(refs[i], refs[count + i], sem.at[i]) for i in range(count)]
    for c in copies:
        c.start()
    for c in copies:
        c.wait()


def store_call(*arrays):
    return pl.pallas_call(
        store_kernel,
        name="store",
        out_shape=tuple(jax.ShapeDtypeStruct(a.shape, a.dtype) for a in arrays),
        in_specs=[pl.BlockSpec(memory_space=pltpu.VMEM)] * len(arrays),
        out_specs=(pl.BlockSpec(memory_space=pl.ANY),) * len(arrays),
        scratch_shapes=[pltpu.SemaphoreType.DMA((len(arrays),))],
        compiler_params=pltpu.CompilerParams(vmem_limit_bytes=12 * 2 ** 20),
    )(*arrays)


def solution(mesh):
    cache_spec = P('dp', 'sp', None, None)

    def device_step(tokens, positions, k_cache, v_cache, w_q, w_k, w_v, w_o, attn_norm, q_norm, k_norm):
        inv = np.float32(ROPE_THETA) ** (-np.arange(HEAD_DIM // 2, dtype=np.float32) * np.float32(2.0) / np.float32(HEAD_DIM))
        freq = jnp.asarray(np.concatenate([inv, inv])[None, :].astype(np.float32))
        flat = (SEQS, SLOTS * KV_HEADS, HEAD_DIM)
        operands = (positions, tokens, attn_norm, q_norm[None, :], k_norm[None, :], freq, w_q, w_k, w_v, w_o, k_cache.reshape(flat), v_cache.reshape(flat))
        row, new, k_loc, v_loc = step_call(*[pltpu.with_memory_space_constraint(a, pltpu.HBM) for a in operands])
        k_out, v_out, new_kv, block_out = store_call(k_loc.reshape(k_cache.shape), v_loc.reshape(v_cache.shape), new, row)
        return block_out, k_out, v_out, new_kv

    return jax.shard_map(device_step, mesh=mesh, in_specs=(P('dp', None), P('dp'), cache_spec, cache_spec, P(), P(), P(), P(), P(), P(), P()), out_specs=(P('dp', None), cache_spec, cache_spec, P('dp', None, None, None)), check_vma=False)
```
